128 devices in a mesh: depth: 4 (over z), col: 4 (over y), row: 8 (over x, core).
Axes of the slice: x: 4, y: 4, z: 4, core: 2. Of those that a mesh axis runs over, the one named last changes fastest.
Arguments:
- a_mat: bfloat16 [8192, 8192], P(('row', 'depth'), 'col')
- b_mat: bfloat16 [8192, 8192], P(('row', 'depth'), 'col')
Outputs:
- output: bfloat16 [8192, 8192], P(('row', 'depth'), 'col')
All inputs are finite; a program needn't handle non-finite values.
Results may differ from the reference program's by a relative error of at most 0.001.
Values are sent between devices in bfloat16 or wider.
A program may use at most 1 GiB of HBM per device.

```python
import jax
import jax.numpy as jnp

N = 8192


def setup_inputs(seed: int = 0) -> dict:
    key_a, key_b = jax.random.split(jax.random.key(seed))
    unit_scale = N ** -0.25
    a_vals = jax.random.normal(key_a, (N, N), jnp.float32) + unit_scale
    b_vals = jax.random.normal(key_b, (N, N), jnp.float32) + unit_scale
    a_mat = (a_vals * unit_scale).astype(jnp.bfloat16)
    b_mat = (b_vals * unit_scale).astype(jnp.bfloat16)
    return {"a_mat": a_mat, "b_mat": b_mat}


def reference(a_mat, b_mat):
    return jnp.dot(a_mat, b_mat, preferred_element_type=jnp.float32).astype(jnp.bfloat16)
```

```python
import functools

import jax
import jax.numpy as jnp
from jax import lax
from jax.experimental import pallas as pl
from jax.experimental.pallas import tpu as pltpu
from jax.sharding import PartitionSpec as P

MESH = pl.DeviceIdType.MESH
GROUPS = 4


def kernel(a_ref, b_ref, out_ref, a_buf, b_buf, acc, stage, load_sem, y_recv, y_fwd, pair_recv, x_recv, x_fwd, z_recv, sib_recv, c_recv, send_sem):
    z, y, r = lax.axis_index("depth"), lax.axis_index("col"), lax.axis_index("row")
    x, c = r // 2, r % 2
    rows, width = a_ref.shape
    half = width // 2

    pair = z + 1 - 2 * (z % 2)
    mirror = 3 - z
    side = ((z + 1) // 2) % 2
    z_of = (z, mirror, pair, 3 - pair)

    y_peer = ({"col": (y + 1) % 4}, {"col": (y + 3) % 4})
    x_peer = ({"row": ((x + 1) % 4) * 2 + c}, {"row": ((x + 3) % 4) * 2 + c})
    to_pair, to_mirror, to_sibling = {"depth": pair}, {"depth": mirror}, {"row": x * 2 + 1 - c}
    peers = y_peer + x_peer + (to_pair, to_mirror, to_sibling)

    def remote(src, dst, kind, recv, where):
        return pltpu.make_async_remote_copy(src_ref=src, dst_ref=dst, send_sem=send_sem.at[kind], recv_sem=recv, device_id=where, device_id_type=MESH)

    def arrived(ref, recv):
        remote(ref, ref, 0, recv, to_sibling).wait_recv()

    def sent(ref, kind):
        remote(ref, ref, kind, z_recv.at[0], to_sibling).wait_send()

    own_rows, pair_rows = pl.ds(0, rows), pl.ds(rows, rows)
    part_rows = (own_rows, pair_rows)

    def a_load(g, cc):
        which = c + cc - 2 * c * cc
        start = pl.multiple_of(which * half + z_of[g] * rows, rows)
        return pltpu.make_async_copy(a_ref.at[:, pl.ds(start, rows)], a_buf.at[0, g, cc, own_rows], load_sem.at[g * 2 + cc])

    my_cols = pl.ds(pl.multiple_of(side * half, half), half)
    other_cols = pl.ds(pl.multiple_of((1 - side) * half, half), half)
    b_load = pltpu.make_async_copy(b_ref.at[:, my_cols], b_buf.at[0, 0, 0], load_sem.at[8])

    b_load.start()
    for g in (0, 2, 3, 1):
        for cc in range(2):
            a_load(g, cc).start()

    barrier = pltpu.get_barrier_semaphore()
    for where in peers:
        pl.semaphore_signal(barrier, inc=1, device_id=where, device_id_type=MESH)
    pl.semaphore_wait(barrier, len(peers))

    slot_of = (3, 1)
    k_half = (pl.ds(0, rows // 2), pl.ds(rows // 2, rows // 2))

    def send_x(g):
        for d in range(2):
            for h in (d, 1 - d):
                remote(b_buf.at[0, g, 0, k_half[h]], b_buf.at[slot_of[d], g, 0, k_half[h]], 0, x_recv.at[d, g, h], x_peer[d]).start()

    def forward_x(g, d):
        arrived(b_buf.at[slot_of[d], g, 0, k_half[d]], x_recv.at[d, g, d])
        remote(b_buf.at[slot_of[d], g, 0, k_half[d]], b_buf.at[2, g, 0, k_half[d]], 0, x_fwd.at[d, g], x_peer[d]).start()

    def send_y(g, part):
        for d in range(2):
            for cc in (d, 1 - d):
                remote(a_buf.at[0, g, cc, part_rows[part]], a_buf.at[slot_of[d], g, cc, part_rows[part]], 1, y_recv.at[d, g, part, cc], y_peer[d]).start()

    def forward_y(g, part, d):
        arrived(a_buf.at[slot_of[d], g, d, part_rows[part]], y_recv.at[d, g, part, d])
        remote(a_buf.at[slot_of[d], g, d, part_rows[part]], a_buf.at[2, g, d, part_rows[part]], 1, y_fwd.at[d, g, part], y_peer[d]).start()

    def send_pair(g):
        for cc in range(2):
            remote(a_buf.at[0, (g + 2) % 4, cc, own_rows], a_buf.at[0, g, cc, pair_rows], 2, pair_recv.at[g, cc], to_pair).start()

    def pair_arrived(g):
        for cc in range(2):
            arrived(a_buf.at[0, g, cc, pair_rows], pair_recv.at[g, cc])

    def send_sibling(j, g):
        remote(b_buf.at[j, g, 0], b_buf.at[j, g, 1], 4, sib_recv.at[j, g], to_sibling).start()

    b_load.wait()
    send_x(0)
    remote(b_buf.at[0, 0, 0], b_buf.at[0, 1, 0], 3, z_recv.at[1], to_mirror).start()
    for cc in range(2):
        a_load(0, cc).wait()
    send_y(0, 0)
    for cc in range(2):
        a_load(2, cc).wait()
    send_pair(0)
    for cc in range(2):
        a_load(3, cc).wait()
    send_pair(1)
    remote(b_ref.at[:, other_cols], b_buf.at[0, 2, 0], 3, z_recv.at[2], to_pair).start()
    send_pair(2)
    for cc in range(2):
        a_load(1, cc).wait()
    send_pair(3)
    send_sibling(0, 0)
    pair_arrived(0)
    send_y(0, 1)

    tile = half // 4

    def compute(g):
        slots = [(x + j - y + 4) % 4 for j in range(4)]

        def product(part, n):
            cols = pl.ds(pl.multiple_of(n * tile, tile), tile)
            total = None
            for j in range(4):
                for cc in range(2):
                    term = jnp.dot(a_buf[slots[j], g, cc, part_rows[part], :], b_buf[j, g, cc, :, cols], preferred_element_type=jnp.float32)
                    total = term if total is None else total + term
            return cols, total

        for part in (1, 0):
            def body(n, carry, part=part):
                cols, total = product(part, n)
                if g == 0:
                    acc[part_rows[part], cols] = total
                elif g < GROUPS - 1:
                    acc[part_rows[part], cols] += total
                else:
                    stage[part, :, cols] = (acc[part_rows[part], cols] + total).astype(stage.dtype)
                return carry

            lax.fori_loop(0, 4, body, 0)
            if g == GROUPS - 1 and part == 1:
                remote(stage.at[1], out_ref.at[:, my_cols], 5, c_recv, to_pair).start()

    def finish_group(g):
        for part in range(2):
            for d in range(2):
                arrived(a_buf.at[slot_of[d], g, 1 - d, part_rows[part]], y_recv.at[d, g, part, 1 - d])
                arrived(a_buf.at[2, g, d, part_rows[part]], y_fwd.at[d, g, part])
        for j in range(4):
            arrived(b_buf.at[j, g, 1], sib_recv.at[j, g])

    def opposite_arrived(g):
        for d in range(2):
            arrived(b_buf.at[2, g, 0, k_half[d]], x_fwd.at[d, g])
        send_sibling(2, g)

    for g in range(GROUPS):
        for d in range(2):
            forward_y(g, 0, d)
        if g > 0:
            opposite_arrived(g - 1)
        for d in range(2):
            forward_x(g, d)
        for d in range(2):
            forward_y(g, 1, d)
        if g + 1 < GROUPS:
            arrived(b_buf.at[0, g + 1, 0], z_recv.at[g + 1])
            send_x(g + 1)
            send_y(g + 1, 0)
            pair_arrived(g + 1)
            send_y(g + 1, 1)
            if g + 1 == 2:
                remote(b_buf.at[0, 2, 0], b_buf.at[0, 3, 0], 3, z_recv.at[3], to_mirror).start()
            send_sibling(0, g + 1)
        for d in range(2):
            arrived(b_buf.at[slot_of[d], g, 0, k_half[1 - d]], x_recv.at[d, g, 1 - d])
            send_sibling(slot_of[d], g)
        if g > 0:
            finish_group(g - 1)
            compute(g - 1)

    opposite_arrived(GROUPS - 1)
    finish_group(GROUPS - 1)
    compute(GROUPS - 1)
    own_out = pltpu.make_async_copy(stage.at[0], out_ref.at[:, my_cols], load_sem.at[9])
    own_out.start()

    sent(b_buf.at[pl.ds(0, 3), :, 0], 0)
    sent(a_buf.at[pl.ds(0, 3)], 1)
    sent(a_buf.at[0, :, :, own_rows], 2)
    sent(b_buf.at[0, pl.ds(0, 3), 0], 3)
    sent(b_buf.at[:, :, 0], 4)
    sent(stage.at[1], 5)
    arrived(out_ref.at[:, other_cols], c_recv)
    own_out.wait()


def solution(mesh):
    def product(a_blk, b_blk):
        rows, width = a_blk.shape
        half = width // 2
        dma = pltpu.SemaphoreType.DMA
        return pl.pallas_call(
            kernel,
            out_shape=jax.ShapeDtypeStruct((rows, width), jnp.bfloat16),
            in_specs=[pl.BlockSpec(memory_space=pl.ANY)] * 2,
            out_specs=pl.BlockSpec(memory_space=pl.ANY),
            scratch_shapes=[
                pltpu.VMEM((4, GROUPS, 2, 2 * rows, rows), jnp.bfloat16),
                pltpu.VMEM((4, GROUPS, 2, rows, half), jnp.bfloat16),
                pltpu.VMEM((2 * rows, half), jnp.float32),
                pltpu.VMEM((2, rows, half), jnp.bfloat16),
                dma((10,)),
                dma((2, GROUPS, 2, 2)),
                dma((2, GROUPS, 2)),
                dma((GROUPS, 2)),
                dma((2, GROUPS, 2)),
                dma((2, GROUPS)),
                dma((GROUPS,)),
                dma((4, GROUPS)),
                dma(()),
                dma((6,)),
            ],
            compiler_params=pltpu.CompilerParams(collective_id=0, has_side_effects=True, vmem_limit_bytes=48 * 1024 * 1024),
        )(a_blk, b_blk)

    block_spec = P(("row", "depth"), "col")
    return jax.shard_map(product, mesh=mesh, in_specs=(block_spec, block_spec), out_specs=block_spec, check_vma=False)
```

```python
import jax
import jax.numpy as jnp
from jax import lax
from jax.experimental import pallas as pl
from jax.experimental.pallas import tpu as pltpu
from jax.sharding import PartitionSpec as P

MESH = pl.DeviceIdType.MESH
GROUPS = 4
X_STEPS = ((0, 0, 2), (1, 0, 2), (2, 0, 2), (3, 0, 1), (3, 1, 1))
X_KIND, Y_KIND, PAIR_A, Z_KIND, SIBLING, C_KIND, Z_LATE, SIBLING_LATE, X_MINE, X_OTHER = range(10)


def kernel(a_ref, b_ref, out_ref, a_buf, b_buf, other_buf, acc, stage, load_sem, y_recv, y_fwd, pair_recv, x_recv, x_fwd, late_recv, late_fwd, z_recv, z_late, sib_recv, sib_late, c_recv, send_sem):
    z, y, r = lax.axis_index("depth"), lax.axis_index("col"), lax.axis_index("row")
    x, c = r // 2, r % 2
    rows, width = a_ref.shape
    half = width // 2
    late = rows // 4
    early = rows - late

    pair = z + 1 - 2 * (z % 2)
    mirror = 3 - z
    side = ((z + 1) // 2) % 2
    z_of = (z, mirror, pair, 3 - pair)

    y_peer = ({"col": (y + 1) % 4}, {"col": (y + 3) % 4})
    x_peer = ({"row": ((x + 1) % 4) * 2 + c}, {"row": ((x + 3) % 4) * 2 + c})
    to_pair, to_mirror, to_sibling = {"depth": pair}, {"depth": mirror}, {"row": x * 2 + 1 - c}
    peers = y_peer + x_peer + (to_pair, to_mirror, to_sibling)

    def remote(src, dst, kind, recv, where):
        return pltpu.make_async_remote_copy(src_ref=src, dst_ref=dst, send_sem=send_sem.at[kind], recv_sem=recv, device_id=where, device_id_type=MESH)

    def arrived(ref, recv):
        remote(ref, ref, 0, recv, to_sibling).wait_recv()

    def sent(ref, kind):
        remote(ref, ref, kind, z_recv.at[0], to_sibling).wait_send()

    part_rows = (pl.ds(0, rows), pl.ds(rows, rows))
    early_rows, late_rows = pl.ds(0, early), pl.ds(early, late)
    early_half = (pl.ds(0, early // 2), pl.ds(early // 2, early // 2))
    late_half = (pl.ds(early, late // 2), pl.ds(early + late // 2, late // 2))
    other_half = (pl.ds(0, late // 2), pl.ds(late // 2, late // 2))
    my_cols = pl.ds(pl.multiple_of(side * half, half), half)
    other_cols = pl.ds(pl.multiple_of((1 - side) * half, half), half)

    def step_cols(s):
        _, first, count = X_STEPS[s]
        return pl.ds(first * (half // 2), count * (half // 2))

    def a_load(g, cc):
        which = c + cc - 2 * c * cc
        start = pl.multiple_of(which * half + z_of[g] * rows, rows)
        return pltpu.make_async_copy(a_ref.at[:, pl.ds(start, rows)], a_buf.at[0, g, cc, part_rows[0]], load_sem.at[g * 2 + cc])

    def a_loaded(g):
        for cc in range(2):
            a_load(g, cc).wait()

    b_load = pltpu.make_async_copy(b_ref.at[:, my_cols], b_buf.at[0, 0, 0], load_sem.at[8])
    other_load = pltpu.make_async_copy(b_ref.at[late_rows, other_cols], other_buf.at[0], load_sem.at[9])
    b_load.start()
    other_load.start()
    for g in (0, 2, 3, 1):
        for cc in range(2):
            a_load(g, cc).start()

    barrier = pltpu.get_barrier_semaphore()
    for where in peers:
        pl.semaphore_signal(barrier, inc=1, device_id=where, device_id_type=MESH)
    pl.semaphore_wait(barrier, len(peers))

    slot_of = (3, 1)

    def send_x(s):
        g, cols = X_STEPS[s][0], step_cols(s)
        for d in range(2):
            for h in (d, 1 - d):
                remote(b_buf.at[0, g, 0, early_half[h], cols], b_buf.at[slot_of[d], g, 0, early_half[h], cols], X_KIND, x_recv.at[d, s, h], x_peer[d]).start()

    def forward_x(s):
        g, cols = X_STEPS[s][0], step_cols(s)
        for d in range(2):
            got = b_buf.at[slot_of[d], g, 0, early_half[d], cols]
            arrived(got, x_recv.at[d, s, d])
            remote(got, b_buf.at[2, g, 0, early_half[d], cols], X_KIND, x_fwd.at[d, s], x_peer[d]).start()

    def send_sibling(j, s):
        g, cols = X_STEPS[s][0], step_cols(s)
        remote(b_buf.at[j, g, 0, early_rows, cols], b_buf.at[j, g, 1, early_rows, cols], SIBLING, sib_recv.at[j, s], to_sibling).start()

    def sibling_arrived(s):
        g, cols = X_STEPS[s][0], step_cols(s)
        for j in range(4):
            arrived(b_buf.at[j, g, 1, early_rows, cols], sib_recv.at[j, s])

    def finish_x(s):
        g, cols = X_STEPS[s][0], step_cols(s)
        for d in range(2):
            arrived(b_buf.at[slot_of[d], g, 0, early_half[1 - d], cols], x_recv.at[d, s, 1 - d])
            send_sibling(slot_of[d], s)
        for d in range(2):
            arrived(b_buf.at[2, g, 0, early_half[d], cols], x_fwd.at[d, s])
        send_sibling(2, s)

    def send_sibling_late(g):
        remote(b_buf.at[:, g, 0, late_rows], b_buf.at[:, g, 1, late_rows], SIBLING_LATE, sib_late.at[g], to_sibling).start()

    def sibling_late_arrived(g):
        arrived(b_buf.at[:, g, 1, late_rows], sib_late.at[g])

    def late_refs(slot, h):
        return b_buf.at[slot, 0, 0, late_half[h]], other_buf.at[slot, other_half[h]]

    def send_late_x():
        for k in range(2):
            for d in range(2):
                for h in (d, 1 - d):
                    remote(late_refs(0, h)[k], late_refs(slot_of[d], h)[k], X_MINE + k, late_recv.at[d, k, h], x_peer[d]).start()

    def forward_late_x(k):
        for d in range(2):
            got = late_refs(slot_of[d], d)[k]
            arrived(got, late_recv.at[d, k, d])
            remote(got, late_refs(2, d)[k], X_MINE + k, late_fwd.at[d, k], x_peer[d]).start()

    def late_x_arrived(k):
        for d in range(2):
            arrived(late_refs(slot_of[d], 1 - d)[k], late_recv.at[d, k, 1 - d])
            arrived(late_refs(2, d)[k], late_fwd.at[d, k])

    def late_slots(g, u):
        return b_buf.at[pl.ds(2 * u, 2), g, 0, late_rows]

    def send_z_late(src, g, u, where):
        remote(src, late_slots(g, u), Z_LATE, z_late.at[g, u], where).start()

    def send_y(g, part):
        for d in range(2):
            for cc in (d, 1 - d):
                remote(a_buf.at[0, g, cc, part_rows[part]], a_buf.at[slot_of[d], g, cc, part_rows[part]], Y_KIND, y_recv.at[d, g, part, cc], y_peer[d]).start()

    def forward_y(g, part):
        for d in range(2):
            got = a_buf.at[slot_of[d], g, d, part_rows[part]]
            arrived(got, y_recv.at[d, g, part, d])
            remote(got, a_buf.at[2, g, d, part_rows[part]], Y_KIND, y_fwd.at[d, g, part], y_peer[d]).start()

    def near_y_arrived(g, part):
        for d in range(2):
            arrived(a_buf.at[slot_of[d], g, 1 - d, part_rows[part]], y_recv.at[d, g, part, 1 - d])

    def far_y_arrived(g, part):
        for d in range(2):
            arrived(a_buf.at[2, g, d, part_rows[part]], y_fwd.at[d, g, part])

    def finish_y(g, part):
        near_y_arrived(g, part)
        far_y_arrived(g, part)

    def send_pair(g):
        for cc in range(2):
            remote(a_buf.at[0, (g + 2) % 4, cc, part_rows[0]], a_buf.at[0, g, cc, part_rows[1]], PAIR_A, pair_recv.at[g, cc], to_pair).start()

    def pair_arrived(g):
        for cc in range(2):
            arrived(a_buf.at[0, g, cc, part_rows[1]], pair_recv.at[g, cc])

    tile = half // 4

    def compute(g, part, first, count, slots=(0, 1, 2, 3), last=False):
        def body(n, carry):
            cols = pl.ds(pl.multiple_of(n * tile, tile), tile)
            total = None
            for i in slots:
                j = (y + i - x + 4) % 4
                for cc in range(2):
                    term = jnp.dot(a_buf[i, g, cc, part_rows[part], :], b_buf[j, g, cc, :, cols], preferred_element_type=jnp.float32)
                    total = term if total is None else total + term
            if g > 0 or len(slots) < 4:
                total = total + acc[part_rows[part], cols]
            if last:
                stage[part, :, cols] = total.astype(stage.dtype)
            else:
                acc[part_rows[part], cols] = total
            return carry

        lax.fori_loop(first, first + count, body, 0)

    def out_cols(of_side, k):
        return pl.ds(pl.multiple_of(of_side * half + k * (half // 2), half // 2), half // 2)

    def send_c(k):
        remote(stage.at[1, :, pl.ds(k * (half // 2), half // 2)], out_ref.at[:, out_cols(side, k)], C_KIND, c_recv.at[k], to_pair).start()

    b_load.wait()
    other_load.wait()
    send_late_x()
    remote(b_buf.at[0, 0, 0, early_rows], b_buf.at[0, 1, 0, early_rows], Z_KIND, z_recv.at[1], to_mirror).start()
    a_loaded(0)
    send_y(0, 0)
    a_loaded(2)
    send_pair(0)
    send_x(0)
    a_loaded(3)
    send_pair(1)
    remote(b_ref.at[early_rows, other_cols], b_buf.at[0, 2, 0, early_rows], Z_KIND, z_recv.at[2], to_pair).start()
    send_pair(2)
    a_loaded(1)
    send_pair(3)
    send_sibling(0, 0)

    forward_late_x(0)
    forward_y(0, 0)
    forward_late_x(1)
    pair_arrived(0)
    send_y(0, 1)
    late_x_arrived(0)
    for u in range(2):
        send_z_late(late_slots(0, u), 1, u, to_mirror)
    send_sibling_late(0)
    late_x_arrived(1)
    for u in range(2):
        send_z_late(other_buf.at[pl.ds(2 * u, 2)], 2, u, to_pair)

    forward_y(0, 1)
    send_y(1, 0)
    pair_arrived(1)
    send_y(1, 1)
    forward_x(0)
    arrived(b_buf.at[0, 1, 0, early_rows], z_recv.at[1])
    send_x(1)
    send_sibling(0, 1)

    finish_x(0)
    arrived(b_buf.at[0, 2, 0, early_rows], z_recv.at[2])
    remote(b_buf.at[0, 2, 0, early_rows], b_buf.at[0, 3, 0, early_rows], Z_KIND, z_recv.at[3], to_mirror).start()
    send_sibling(0, 2)
    forward_y(1, 0)
    for u in range(2):
        arrived(late_slots(1, u), z_late.at[1, u])
    send_sibling_late(1)
    forward_x(1)
    send_x(2)
    forward_y(1, 1)
    pair_arrived(2)
    send_y(2, 1)
    pair_arrived(3)
    send_y(3, 1)

    for part in range(2):
        finish_y(0, part)
    sibling_arrived(0)
    sibling_late_arrived(0)
    compute(0, 1, 0, 4)
    compute(0, 0, 0, 4)

    finish_x(1)
    forward_y(2, 1)
    arrived(b_buf.at[0, 3, 0, early_rows], z_recv.at[3])
    forward_x(2)
    send_x(3)
    send_x(4)
    send_sibling(0, 3)
    send_sibling(0, 4)
    for u in range(2):
        arrived(late_slots(2, u), z_late.at[2, u])
        send_z_late(late_slots(2, u), 3, u, to_mirror)
    send_sibling_late(2)

    for part in range(2):
        finish_y(1, part)
    sibling_arrived(1)
    sibling_late_arrived(1)
    compute(1, 1, 0, 4)
    forward_y(3, 1)
    send_y(2, 0)
    send_y(3, 0)
    compute(1, 0, 0, 4)

    finish_x(2)
    forward_x(3)
    for u in range(2):
        arrived(late_slots(3, u), z_late.at[3, u])
    send_sibling_late(3)
    finish_y(2, 1)
    sibling_arrived(2)
    sibling_late_arrived(2)
    compute(2, 1, 0, 4)

    finish_x(3)
    forward_y(2, 0)
    forward_x(4)
    finish_y(3, 1)
    sibling_arrived(3)
    sibling_late_arrived(3)
    compute(3, 1, 0, 2, last=True)
    send_c(0)

    finish_x(4)
    sibling_arrived(4)
    compute(3, 1, 2, 2, last=True)
    send_c(1)
    forward_y(3, 0)
    finish_y(2, 0)
    compute(2, 0, 0, 4)
    near_y_arrived(3, 0)
    compute(3, 0, 0, 4, slots=(0, 1, 3))
    far_y_arrived(3, 0)
    own_out = []
    for k in range(2):
        compute(3, 0, 2 * k, 2, slots=(2,), last=True)
        own_out.append(pltpu.make_async_copy(stage.at[0, :, pl.ds(k * (half // 2), half // 2)], out_ref.at[:, out_cols(side, k)], load_sem.at[10 + k]))
        own_out[k].start()

    sent(b_buf.at[pl.ds(0, 3), :, 0, early_rows], X_KIND)
    sent(a_buf.at[pl.ds(0, 3)], Y_KIND)
    sent(a_buf.at[0, :, :, part_rows[0]], PAIR_A)
    sent(b_buf.at[0, pl.ds(0, 3), 0, early_rows], Z_KIND)
    sent(b_buf.at[:, :, 0, early_rows], SIBLING)
    sent(b_buf.at[:, pl.ds(0, 3), 0, late_rows], Z_LATE)
    sent(b_buf.at[:, :, 0, late_rows], SIBLING_LATE)
    sent(b_buf.at[pl.ds(0, 3), 0, 0, late_rows], X_MINE)
    sent(other_buf.at[pl.ds(0, 3)], X_OTHER)
    sent(stage.at[1], C_KIND)
    for k in range(2):
        arrived(out_ref.at[:, out_cols(1 - side, k)], c_recv.at[k])
    for copy in own_out:
        copy.wait()


def solution(mesh):
    def product(a_blk, b_blk):
        rows, width = a_blk.shape
        half = width // 2
        dma = pltpu.SemaphoreType.DMA
        return pl.pallas_call(
            kernel,
            out_shape=jax.ShapeDtypeStruct((rows, width), jnp.bfloat16),
            in_specs=[pl.BlockSpec(memory_space=pltpu.HBM)] * 2,
            out_specs=pl.BlockSpec(memory_space=pltpu.HBM),
            scratch_shapes=[
                pltpu.VMEM((4, GROUPS, 2, 2 * rows, rows), jnp.bfloat16),
                pltpu.VMEM((4, GROUPS, 2, rows, half), jnp.bfloat16),
                pltpu.VMEM((4, rows // 4, half), jnp.bfloat16),
                pltpu.VMEM((2 * rows, half), jnp.float32),
                pltpu.VMEM((2, rows, half), jnp.bfloat16),
                dma((12,)),
                dma((2, GROUPS, 2, 2)),
                dma((2, GROUPS, 2)),
                dma((GROUPS, 2)),
                dma((2, len(X_STEPS), 2)),
                dma((2, len(X_STEPS))),
                dma((2, 2, 2)),
                dma((2, 2)),
                dma((GROUPS,)),
                dma((GROUPS, 2)),
                dma((4, len(X_STEPS))),
                dma((GROUPS,)),
                dma((2,)),
                dma((10,)),
            ],
            compiler_params=pltpu.CompilerParams(collective_id=0, has_side_effects=True, vmem_limit_bytes=60 * 1024 * 1024),
        )(a_blk, b_blk)

    block_spec = P(("row", "depth"), "col")
    return jax.shard_map(product, mesh=mesh, in_specs=(block_spec, block_spec), out_specs=block_spec, check_vma=False)
```

```python
import jax
import jax.numpy as jnp
from jax import lax
from jax.experimental import pallas as pl
from jax.experimental.pallas import tpu as pltpu
from jax.sharding import PartitionSpec as P

MESH = pl.DeviceIdType.MESH
GROUPS = 4
X_STEPS = ((0, False, 0, 4), (1, True, 0, 4), (2, False, 0, 4), (3, False, 0, 2), (3, False, 2, 1), (3, False, 3, 1))
C_PIECES = ((0, 2), (2, 1), (3, 1))
X_KIND, X_EARLY, Y_OWN, Y_PAIR, PAIR_A, PAIR_FULL, Z_KIND, Z_EARLY, Z_LATE, SIBLING, C_KIND = range(11)


def kernel(a_ref, b_ref, out_ref, a_buf, b_buf, acc, stage, load_sem, y_recv, y_fwd, pair_recv, pair_full, x_recv, x_fwd, z_recv, z_late, sib_recv, sib_late, c_recv, send_sem):
    z, y, r = lax.axis_index("depth"), lax.axis_index("col"), lax.axis_index("row")
    x, c = r // 2, r % 2
    rows, width = a_ref.shape
    half = width // 2
    tile = half // 4
    early = rows // 4

    pair = z + 1 - 2 * (z % 2)
    mirror = 3 - z
    side = ((z + 1) // 2) % 2
    z_of = (z, mirror, pair, 3 - pair)

    y_peer = ({"col": (y + 1) % 4}, {"col": (y + 3) % 4})
    x_peer = ({"row": ((x + 1) % 4) * 2 + c}, {"row": ((x + 3) % 4) * 2 + c})
    to_pair, to_mirror, to_sibling = {"depth": pair}, {"depth": mirror}, {"row": x * 2 + 1 - c}
    peers = y_peer + x_peer + (to_pair, to_mirror, to_sibling)

    def remote(src, dst, kind, recv, where):
        return pltpu.make_async_remote_copy(src_ref=src, dst_ref=dst, send_sem=send_sem.at[kind], recv_sem=recv, device_id=where, device_id_type=MESH)

    def arrived(ref, recv):
        remote(ref, ref, 0, recv, to_sibling).wait_recv()

    def sent(ref, kind):
        remote(ref, ref, kind, z_recv.at[0], to_sibling).wait_send()

    part_rows = (pl.ds(0, rows), pl.ds(rows, rows))
    early_rows, late_rows = pl.ds(0, early), pl.ds(early, rows - early)
    my_cols = pl.ds(pl.multiple_of(side * half, half), half)
    other_cols = pl.ds(pl.multiple_of((1 - side) * half, half), half)

    def a_load(g, cc):
        which = c + cc - 2 * c * cc
        start = pl.multiple_of(which * half + z_of[g] * rows, rows)
        return pltpu.make_async_copy(a_ref.at[:, pl.ds(start, rows)], a_buf.at[0, g, cc, part_rows[0]], load_sem.at[g * 2 + cc])

    def a_loaded(g):
        for cc in range(2):
            a_load(g, cc).wait()

    b_load = pltpu.make_async_copy(b_ref.at[:, my_cols], b_buf.at[0, 0, 0], load_sem.at[8])
    b_load.start()
    for g in (0, 2, 3, 1):
        for cc in range(2):
            a_load(g, cc).start()

    barrier = pltpu.get_barrier_semaphore()
    for where in peers:
        pl.semaphore_signal(barrier, inc=1, device_id=where, device_id_type=MESH)
    pl.semaphore_wait(barrier, len(peers))

    slot_of = (3, 1)

    def step_refs(s, slot, piece=None, core=0):
        g, early_only, first, count = X_STEPS[s]
        size = early if early_only else rows
        at = pl.ds(0, size) if piece is None else pl.ds(piece * (size // 2), size // 2)
        return b_buf.at[slot, g, core, at, pl.ds(first * tile, count * tile)]

    def x_kind(s):
        return X_EARLY if X_STEPS[s][1] else X_KIND

    def send_x(s):
        for d in range(2):
            for h in (d, 1 - d):
                remote(step_refs(s, 0, h), step_refs(s, slot_of[d], h), x_kind(s), x_recv.at[d, s, h], x_peer[d]).start()

    def forward_x(s):
        for d in range(2):
            arrived(step_refs(s, slot_of[d], d), x_recv.at[d, s, d])
            remote(step_refs(s, slot_of[d], d), step_refs(s, 2, d), x_kind(s), x_fwd.at[d, s], x_peer[d]).start()

    def send_sibling(j, s):
        remote(step_refs(s, j), step_refs(s, j, core=1), SIBLING, sib_recv.at[j, s], to_sibling).start()

    def near_x(s):
        for d in range(2):
            arrived(step_refs(s, slot_of[d], 1 - d), x_recv.at[d, s, 1 - d])
            send_sibling(slot_of[d], s)

    def far_x(s):
        for d in range(2):
            arrived(step_refs(s, 2, d), x_fwd.at[d, s])
        send_sibling(2, s)

    def sibling_arrived(s):
        for j in range(4):
            arrived(step_refs(s, j, core=1), sib_recv.at[j, s])

    def send_late(j):
        remote(b_buf.at[j, 0, 0, late_rows], b_buf.at[j, 1, 0, late_rows], Z_LATE, z_late.at[j], to_mirror).start()

    def late_arrived(j):
        arrived(b_buf.at[j, 1, 0, late_rows], z_late.at[j])
        remote(b_buf.at[j, 1, 0, late_rows], b_buf.at[j, 1, 1, late_rows], SIBLING, sib_late.at[j], to_sibling).start()

    def sibling_late_arrived(j):
        arrived(b_buf.at[j, 1, 1, late_rows], sib_late.at[j])

    def send_y(g, part):
        for d in range(2):
            for cc in (d, 1 - d):
                remote(a_buf.at[0, g, cc, part_rows[part]], a_buf.at[slot_of[d], g, cc, part_rows[part]], Y_OWN + part, y_recv.at[d, g, part, cc], y_peer[d]).start()

    def forward_y(g, part):
        for d in range(2):
            got = a_buf.at[slot_of[d], g, d, part_rows[part]]
            arrived(got, y_recv.at[d, g, part, d])
            remote(got, a_buf.at[2, g, d, part_rows[part]], Y_OWN + part, y_fwd.at[d, g, part], y_peer[d]).start()

    def near_y(g, part):
        for d in range(2):
            arrived(a_buf.at[slot_of[d], g, 1 - d, part_rows[part]], y_recv.at[d, g, part, 1 - d])

    def far_y(g, part):
        for d in range(2):
            arrived(a_buf.at[2, g, d, part_rows[part]], y_fwd.at[d, g, part])

    def send_pair(g):
        for cc in range(2):
            remote(a_buf.at[0, (g + 2) % 4, cc, part_rows[0]], a_buf.at[0, g, cc, part_rows[1]], PAIR_A, pair_recv.at[g, cc], to_pair).start()

    def pair_arrived(g):
        for cc in range(2):
            arrived(a_buf.at[0, g, cc, part_rows[1]], pair_recv.at[g, cc])

    def send_pair_full(i):
        remote(a_buf.at[i, 1, :, part_rows[0]], a_buf.at[i, 3, :, part_rows[1]], PAIR_FULL, pair_full.at[i], to_pair).start()

    def pair_full_arrived():
        for i in range(4):
            arrived(a_buf.at[i, 3, :, part_rows[1]], pair_full.at[i])

    def compute(g, part, tiles=(0, 4), slots=(0, 1, 2, 3), by_a=False, add=True, last=False):
        def body(n, carry):
            at = pl.multiple_of(n * tile, tile)
            cols = pl.ds(at, tile)
            total = None
            for slot in slots:
                i, j = (slot, (y + slot - x + 4) % 4) if by_a else ((x + slot - y + 4) % 4, slot)
                for cc in range(2):
                    term = jnp.dot(a_buf[i, g, cc, part_rows[part], :], b_buf[j, g, cc, :, cols], preferred_element_type=jnp.float32)
                    total = term if total is None else total + term
            if add:
                total = total + acc[part_rows[part], cols]
            if not last:
                acc[part_rows[part], cols] = total
            elif part == 1:
                stage[:, cols] = total.astype(stage.dtype)
            else:
                out_ref[:, pl.ds(pl.multiple_of(side * half + at, tile), tile)] = total.astype(out_ref.dtype)
            return carry

        lax.fori_loop(tiles[0], tiles[0] + tiles[1], body, 0)

    def out_cols(of_side, k):
        first, count = C_PIECES[k]
        return pl.ds(pl.multiple_of(of_side * half + first * tile, tile), count * tile)

    def send_c(k):
        first, count = C_PIECES[k]
        remote(stage.at[:, pl.ds(first * tile, count * tile)], out_ref.at[:, out_cols(side, k)], C_KIND, c_recv.at[k], to_pair).start()

    b_load.wait()
    send_x(0)
    remote(b_buf.at[0, 0, 0, early_rows], b_buf.at[0, 1, 0, early_rows], Z_EARLY, z_recv.at[1], to_mirror).start()
    send_late(0)
    a_loaded(0)
    send_y(0, 0)
    a_loaded(2)
    send_pair(0)
    remote(b_ref.at[:, other_cols], b_buf.at[0, 2, 0], Z_KIND, z_recv.at[2], to_pair).start()
    a_loaded(3)
    send_pair(1)
    send_pair(2)
    a_loaded(1)
    send_sibling(0, 0)

    forward_y(0, 0)
    send_y(1, 0)
    send_pair_full(0)
    forward_x(0)
    arrived(step_refs(1, 0), z_recv.at[1])
    send_x(1)
    send_sibling(0, 1)
    near_x(0)
    send_late(3)
    forward_y(1, 0)
    pair_arrived(0)
    send_y(0, 1)
    arrived(b_buf.at[0, 2, 0], z_recv.at[2])
    remote(b_buf.at[0, 2, 0], b_buf.at[0, 3, 0], Z_KIND, z_recv.at[3], to_mirror).start()
    send_x(2)
    send_late(1)
    far_x(0)
    send_late(2)
    send_sibling(0, 2)
    near_y(1, 0)
    send_pair_full(1)
    send_pair_full(3)
    far_y(1, 0)
    send_pair_full(2)
    forward_x(1)
    forward_y(0, 1)
    pair_arrived(1)
    send_y(1, 1)
    near_x(1)
    far_x(1)

    near_y(0, 0)
    far_y(0, 0)
    sibling_arrived(0)
    compute(0, 0, add=False)

    forward_x(2)
    forward_y(1, 1)
    pair_arrived(2)
    send_y(2, 1)
    near_y(0, 1)
    far_y(0, 1)
    compute(0, 1, add=False)

    arrived(b_buf.at[0, 3, 0], z_recv.at[3])
    send_x(3)
    send_x(4)
    for s in (3, 4, 5):
        send_sibling(0, s)
    near_x(2)
    late_arrived(0)
    late_arrived(3)
    forward_y(2, 1)
    send_y(2, 0)
    send_y(3, 0)
    far_x(2)

    forward_x(3)
    send_x(5)
    near_y(1, 1)
    far_y(1, 1)
    late_arrived(1)
    sibling_arrived(1)
    for j in (0, 3, 1):
        sibling_late_arrived(j)
    compute(1, 1, slots=(0, 3, 1))
    forward_y(2, 0)
    near_x(3)
    near_y(2, 1)
    far_y(2, 1)
    sibling_arrived(2)
    compute(2, 1)
    forward_x(4)
    far_x(3)
    late_arrived(2)
    forward_y(3, 0)
    sibling_late_arrived(2)
    compute(1, 1, slots=(2,))
    forward_x(5)
    near_x(4)

    pair_full_arrived()
    sibling_arrived(3)
    compute(3, 1, tiles=(0, 2), last=True)
    send_c(0)
    far_x(4)
    near_x(5)
    sibling_arrived(4)
    compute(3, 1, tiles=(2, 1), last=True)
    send_c(1)
    far_x(5)
    compute(1, 0)
    sibling_arrived(5)
    compute(3, 1, tiles=(3, 1), last=True)
    send_c(2)
    near_y(2, 0)
    far_y(2, 0)
    compute(2, 0)
    near_y(3, 0)
    compute(3, 0, slots=(0, 1, 3), by_a=True)
    far_y(3, 0)
    compute(3, 0, slots=(2,), by_a=True, last=True)

    sent(b_buf.at[pl.ds(0, 3), pl.ds(0, 3), 0], X_KIND)
    sent(b_buf.at[pl.ds(0, 3), 0, 0, early_rows], X_EARLY)
    sent(a_buf.at[pl.ds(0, 3), :, :, part_rows[0]], Y_OWN)
    sent(a_buf.at[pl.ds(0, 3), pl.ds(0, 3), :, part_rows[1]], Y_PAIR)
    sent(a_buf.at[0, pl.ds(0, 3), :, part_rows[0]], PAIR_A)
    sent(a_buf.at[:, 0, :, part_rows[0]], PAIR_FULL)
    sent(b_buf.at[0, pl.ds(0, 2), 0], Z_KIND)
    sent(b_buf.at[0, 0, 0, early_rows], Z_EARLY)
    sent(b_buf.at[:, 0, 0, late_rows], Z_LATE)
    sent(b_buf.at[:, :, 0], SIBLING)
    sent(stage, C_KIND)
    for k in range(len(C_PIECES)):
        arrived(out_ref.at[:, out_cols(1 - side, k)], c_recv.at[k])


def solution(mesh):
    def product(a_blk, b_blk):
        rows, width = a_blk.shape
        half = width // 2
        dma = pltpu.SemaphoreType.DMA
        return pl.pallas_call(
            kernel,
            out_shape=jax.ShapeDtypeStruct((rows, width), jnp.bfloat16),
            in_specs=[pl.BlockSpec(memory_space=pltpu.HBM)] * 2,
            out_specs=pl.BlockSpec(memory_space=pltpu.VMEM),
            scratch_shapes=[
                pltpu.VMEM((4, GROUPS, 2, 2 * rows, rows), jnp.bfloat16),
                pltpu.VMEM((4, GROUPS, 2, rows, half), jnp.bfloat16),
                pltpu.VMEM((2 * rows, half), jnp.float32),
                pltpu.VMEM((rows, half), jnp.bfloat16),
                dma((9,)),
                dma((2, GROUPS, 2, 2)),
                dma((2, GROUPS, 2)),
                dma((GROUPS, 2)),
                dma((4,)),
                dma((2, len(X_STEPS), 2)),
                dma((2, len(X_STEPS))),
                dma((GROUPS,)),
                dma((4,)),
                dma((4, len(X_STEPS))),
                dma((4,)),
                dma((len(C_PIECES),)),
                dma((11,)),
            ],
            compiler_params=pltpu.CompilerParams(collective_id=0, has_side_effects=True, vmem_limit_bytes=56 * 1024 * 1024),
        )(a_blk, b_blk)

    block_spec = P(("row", "depth"), "col")
    return jax.shard_map(product, mesh=mesh, in_specs=(block_spec, block_spec), out_specs=block_spec, check_vma=False)
```

```python
import jax
import jax.numpy as jnp
from jax import lax
from jax.experimental import pallas as pl
from jax.experimental.pallas import tpu as pltpu
from jax.sharding import PartitionSpec as P

MESH = pl.DeviceIdType.MESH
GROUPS = 4
X_STEPS = ((0, False, 0, 4), (1, True, 0, 4), (2, False, 0, 4), (3, False, 0, 2), (3, False, 2, 1), (3, False, 3, 1))
C_PIECES = ((0, 2), (2, 1), (3, 1))
X_KIND, X_EARLY, Y_OWN, Y_PAIR, PAIR_A, PAIR_FULL, Z_KIND, Z_EARLY, Z_LATE, SIBLING, C_KIND = range(11)


def kernel(a_ref, b_ref, out_ref, a_buf, b_buf, acc, stage, load_sem, y_recv, y_fwd, pair_recv, pair_full, x_recv, x_fwd, z_recv, z_late, sib_recv, sib_late, c_recv, send_sem):
    z, y, r = lax.axis_index("depth"), lax.axis_index("col"), lax.axis_index("row")
    x, c = r // 2, r % 2
    rows, width = a_ref.shape
    half = width // 2
    tile = half // 4
    early = rows // 4

    pair = z + 1 - 2 * (z % 2)
    mirror = 3 - z
    side = ((z + 1) // 2) % 2
    z_of = (z, mirror, pair, 3 - pair)

    y_peer = ({"col": (y + 1) % 4}, {"col": (y + 3) % 4})
    x_peer = ({"row": ((x + 1) % 4) * 2 + c}, {"row": ((x + 3) % 4) * 2 + c})
    to_pair, to_mirror, to_sibling = {"depth": pair}, {"depth": mirror}, {"row": x * 2 + 1 - c}
    peers = y_peer + x_peer + (to_pair, to_mirror, to_sibling)

    def remote(src, dst, kind, recv, where):
        return pltpu.make_async_remote_copy(src_ref=src, dst_ref=dst, send_sem=send_sem.at[kind], recv_sem=recv, device_id=where, device_id_type=MESH)

    def arrived(ref, recv):
        remote(ref, ref, 0, recv, to_sibling).wait_recv()

    def sent(ref, kind):
        remote(ref, ref, kind, z_recv.at[0], to_sibling).wait_send()

    part_rows = (pl.ds(0, rows), pl.ds(rows, rows))
    early_rows, late_rows = pl.ds(0, early), pl.ds(early, rows - early)
    my_cols = pl.ds(pl.multiple_of(side * half, half), half)
    other_cols = pl.ds(pl.multiple_of((1 - side) * half, half), half)

    def a_load(g, cc):
        which = c + cc - 2 * c * cc
        start = pl.multiple_of(which * half + z_of[g] * rows, rows)
        return pltpu.make_async_copy(a_ref.at[:, pl.ds(start, rows)], a_buf.at[0, g, cc, part_rows[0]], load_sem.at[g * 2 + cc])

    def a_loaded(g):
        for cc in range(2):
            a_load(g, cc).wait()

    b_load = pltpu.make_async_copy(b_ref.at[:, my_cols], b_buf.at[0, 0, 0], load_sem.at[8])
    b_load.start()
    for g in (0, 2, 3, 1):
        for cc in range(2):
            a_load(g, cc).start()

    barrier = pltpu.get_barrier_semaphore()
    for where in peers:
        pl.semaphore_signal(barrier, inc=1, device_id=where, device_id_type=MESH)
    pl.semaphore_wait(barrier, len(peers))

    slot_of = (3, 1)

    def step_refs(s, slot, piece=None, core=0):
        g, early_only, first, count = X_STEPS[s]
        size = early if early_only else rows
        at = pl.ds(0, size) if piece is None else pl.ds(piece * (size // 2), size // 2)
        return b_buf.at[slot, g, core, at, pl.ds(first * tile, count * tile)]

    def x_kind(s):
        return X_EARLY if X_STEPS[s][1] else X_KIND

    def send_x(s):
        for d in range(2):
            for h in (d, 1 - d):
                remote(step_refs(s, 0, h), step_refs(s, slot_of[d], h), x_kind(s), x_recv.at[d, s, h], x_peer[d]).start()

    def forward_x(s):
        for d in range(2):
            arrived(step_refs(s, slot_of[d], d), x_recv.at[d, s, d])
            remote(step_refs(s, slot_of[d], d), step_refs(s, 2, d), x_kind(s), x_fwd.at[d, s], x_peer[d]).start()

    def send_sibling(j, s):
        remote(step_refs(s, j), step_refs(s, j, core=1), SIBLING, sib_recv.at[j, s], to_sibling).start()

    def near_x(s):
        for d in range(2):
            arrived(step_refs(s, slot_of[d], 1 - d), x_recv.at[d, s, 1 - d])
            send_sibling(slot_of[d], s)

    def far_x(s):
        for d in range(2):
            arrived(step_refs(s, 2, d), x_fwd.at[d, s])
        send_sibling(2, s)

    def sibling_arrived(s):
        for j in range(4):
            arrived(step_refs(s, j, core=1), sib_recv.at[j, s])

    def send_late(j):
        remote(b_buf.at[j, 0, 0, late_rows], b_buf.at[j, 1, 0, late_rows], Z_LATE, z_late.at[j], to_mirror).start()

    def late_arrived(j):
        arrived(b_buf.at[j, 1, 0, late_rows], z_late.at[j])
        remote(b_buf.at[j, 1, 0, late_rows], b_buf.at[j, 1, 1, late_rows], SIBLING, sib_late.at[j], to_sibling).start()

    def sibling_late_arrived(j):
        arrived(b_buf.at[j, 1, 1, late_rows], sib_late.at[j])

    def send_y(g, part):
        for d in range(2):
            for cc in (d, 1 - d):
                remote(a_buf.at[0, g, cc, part_rows[part]], a_buf.at[slot_of[d], g, cc, part_rows[part]], Y_OWN + part, y_recv.at[d, g, part, cc], y_peer[d]).start()

    def forward_y(g, part):
        for d in range(2):
            got = a_buf.at[slot_of[d], g, d, part_rows[part]]
            arrived(got, y_recv.at[d, g, part, d])
            remote(got, a_buf.at[2, g, d, part_rows[part]], Y_OWN + part, y_fwd.at[d, g, part], y_peer[d]).start()

    def near_y(g, part):
        for d in range(2):
            arrived(a_buf.at[slot_of[d], g, 1 - d, part_rows[part]], y_recv.at[d, g, part, 1 - d])

    def far_y(g, part):
        for d in range(2):
            arrived(a_buf.at[2, g, d, part_rows[part]], y_fwd.at[d, g, part])

    def send_pair(g):
        for cc in range(2):
            remote(a_buf.at[0, (g + 2) % 4, cc, part_rows[0]], a_buf.at[0, g, cc, part_rows[1]], PAIR_A, pair_recv.at[g, cc], to_pair).start()

    def pair_arrived(g):
        for cc in range(2):
            arrived(a_buf.at[0, g, cc, part_rows[1]], pair_recv.at[g, cc])

    def send_pair_full(i):
        remote(a_buf.at[i, 1, :, part_rows[0]], a_buf.at[i, 3, :, part_rows[1]], PAIR_FULL, pair_full.at[i], to_pair).start()

    def pair_full_arrived():
        for i in range(4):
            arrived(a_buf.at[i, 3, :, part_rows[1]], pair_full.at[i])

    def compute(g, part, tiles=(0, 4), slots=(0, 1, 2, 3), by_a=False, add=True, last=False):
        def body(n, carry):
            cols = pl.ds(pl.multiple_of(n * tile, tile), tile)
            total = None
            for slot in slots:
                i, j = (slot, (y + slot - x + 4) % 4) if by_a else ((x + slot - y + 4) % 4, slot)
                for cc in range(2):
                    term = jnp.dot(a_buf[i, g, cc, part_rows[part], :], b_buf[j, g, cc, :, cols], preferred_element_type=jnp.float32)
                    total = term if total is None else total + term
            if add:
                total = total + acc[part_rows[part], cols]
            if not last:
                acc[part_rows[part], cols] = total
            else:
                stage[part, :, cols] = total.astype(stage.dtype)
            return carry

        lax.fori_loop(tiles[0], tiles[0] + tiles[1], body, 0)

    def out_cols(of_side, k):
        first, count = C_PIECES[k]
        return pl.ds(pl.multiple_of(of_side * half + first * tile, tile), count * tile)

    def send_c(k):
        first, count = C_PIECES[k]
        remote(stage.at[1, :, pl.ds(first * tile, count * tile)], out_ref.at[:, out_cols(side, k)], C_KIND, c_recv.at[k], to_pair).start()

    b_load.wait()
    send_x(0)
    remote(b_buf.at[0, 0, 0, early_rows], b_buf.at[0, 1, 0, early_rows], Z_EARLY, z_recv.at[1], to_mirror).start()
    send_late(0)
    a_loaded(0)
    send_y(0, 0)
    a_loaded(2)
    send_pair(0)
    remote(b_ref.at[:, other_cols], b_buf.at[0, 2, 0], Z_KIND, z_recv.at[2], to_pair).start()
    a_loaded(3)
    send_pair(1)
    send_pair(2)
    a_loaded(1)
    send_sibling(0, 0)

    forward_y(0, 0)
    send_y(1, 0)
    send_pair_full(0)
    forward_x(0)
    arrived(step_refs(1, 0), z_recv.at[1])
    send_x(1)
    send_sibling(0, 1)
    near_x(0)
    send_late(3)
    forward_y(1, 0)
    pair_arrived(0)
    send_y(0, 1)
    arrived(b_buf.at[0, 2, 0], z_recv.at[2])
    remote(b_buf.at[0, 2, 0], b_buf.at[0, 3, 0], Z_KIND, z_recv.at[3], to_mirror).start()
    send_x(2)
    send_late(1)
    far_x(0)
    send_late(2)
    send_sibling(0, 2)
    near_y(1, 0)
    send_pair_full(1)
    send_pair_full(3)
    far_y(1, 0)
    send_pair_full(2)
    forward_x(1)
    forward_y(0, 1)
    pair_arrived(1)
    send_y(1, 1)
    near_x(1)
    far_x(1)

    near_y(0, 0)
    far_y(0, 0)
    sibling_arrived(0)
    compute(0, 0, add=False)

    forward_x(2)
    forward_y(1, 1)
    pair_arrived(2)
    send_y(2, 1)
    near_y(0, 1)
    far_y(0, 1)
    compute(0, 1, add=False)

    arrived(b_buf.at[0, 3, 0], z_recv.at[3])
    send_x(3)
    send_x(4)
    for s in (3, 4, 5):
        send_sibling(0, s)
    near_x(2)
    late_arrived(0)
    late_arrived(3)
    forward_y(2, 1)
    send_y(2, 0)
    send_y(3, 0)
    far_x(2)

    forward_x(3)
    send_x(5)
    near_y(1, 1)
    far_y(1, 1)
    late_arrived(1)
    sibling_arrived(1)
    for j in (0, 3, 1):
        sibling_late_arrived(j)
    compute(1, 1, slots=(0, 3, 1))
    forward_y(2, 0)
    near_x(3)
    near_y(2, 1)
    far_y(2, 1)
    sibling_arrived(2)
    compute(2, 1)
    forward_x(4)
    far_x(3)
    late_arrived(2)
    forward_y(3, 0)
    sibling_late_arrived(2)
    compute(1, 1, slots=(2,))
    forward_x(5)
    near_x(4)

    pair_full_arrived()
    sibling_arrived(3)
    compute(3, 1, tiles=(0, 2), last=True)
    send_c(0)
    far_x(4)
    near_x(5)
    sibling_arrived(4)
    compute(3, 1, tiles=(2, 1), last=True)
    send_c(1)
    far_x(5)
    compute(1, 0)
    sibling_arrived(5)
    compute(3, 1, tiles=(3, 1), last=True)
    send_c(2)
    near_y(2, 0)
    far_y(2, 0)
    compute(2, 0)
    near_y(3, 0)
    compute(3, 0, slots=(0, 1, 3), by_a=True)
    far_y(3, 0)
    compute(3, 0, slots=(2,), by_a=True, last=True)
    own_out = pltpu.make_async_copy(stage.at[0], out_ref.at[:, my_cols], load_sem.at[9])
    own_out.start()

    sent(b_buf.at[pl.ds(0, 3), pl.ds(0, 3), 0], X_KIND)
    sent(b_buf.at[pl.ds(0, 3), 0, 0, early_rows], X_EARLY)
    sent(a_buf.at[pl.ds(0, 3), :, :, part_rows[0]], Y_OWN)
    sent(a_buf.at[pl.ds(0, 3), pl.ds(0, 3), :, part_rows[1]], Y_PAIR)
    sent(a_buf.at[0, pl.ds(0, 3), :, part_rows[0]], PAIR_A)
    sent(a_buf.at[:, 0, :, part_rows[0]], PAIR_FULL)
    sent(b_buf.at[0, pl.ds(0, 2), 0], Z_KIND)
    sent(b_buf.at[0, 0, 0, early_rows], Z_EARLY)
    sent(b_buf.at[:, 0, 0, late_rows], Z_LATE)
    sent(b_buf.at[:, :, 0], SIBLING)
    sent(stage.at[1], C_KIND)
    for k in range(len(C_PIECES)):
        arrived(out_ref.at[:, out_cols(1 - side, k)], c_recv.at[k])
    own_out.wait()


def solution(mesh):
    def product(a_blk, b_blk):
        rows, width = a_blk.shape
        half = width // 2
        dma = pltpu.SemaphoreType.DMA
        return pl.pallas_call(
            kernel,
            out_shape=jax.ShapeDtypeStruct((rows, width), jnp.bfloat16),
            in_specs=[pl.BlockSpec(memory_space=pltpu.HBM)] * 2,
            out_specs=pl.BlockSpec(memory_space=pl.ANY),
            scratch_shapes=[
                pltpu.VMEM((4, GROUPS, 2, 2 * rows, rows), jnp.bfloat16),
                pltpu.VMEM((4, GROUPS, 2, rows, half), jnp.bfloat16),
                pltpu.VMEM((2 * rows, half), jnp.float32),
                pltpu.VMEM((2, rows, half), jnp.bfloat16),
                dma((10,)),
                dma((2, GROUPS, 2, 2)),
                dma((2, GROUPS, 2)),
                dma((GROUPS, 2)),
                dma((4,)),
                dma((2, len(X_STEPS), 2)),
                dma((2, len(X_STEPS))),
                dma((GROUPS,)),
                dma((4,)),
                dma((4, len(X_STEPS))),
                dma((4,)),
                dma((len(C_PIECES),)),
                dma((11,)),
            ],
            compiler_params=pltpu.CompilerParams(collective_id=0, has_side_effects=True, vmem_limit_bytes=48 * 1024 * 1024),
        )(a_blk, b_blk)

    block_spec = P(("row", "depth"), "col")
    return jax.shard_map(product, mesh=mesh, in_specs=(block_spec, block_spec), out_specs=block_spec, check_vma=False)
```

```python
import jax
import jax.numpy as jnp
from jax import lax
from jax.experimental import pallas as pl
from jax.experimental.pallas import tpu as pltpu
from jax.sharding import PartitionSpec as P

MESH = pl.DeviceIdType.MESH
GROUPS = 4
X_STEPS = ((0, False, 0, 4), (1, True, 0, 4), (2, False, 0, 4), (3, False, 0, 2), (3, False, 2, 1), (3, False, 3, 1))
C_PIECES = ((0, 2), (2, 1), (3, 1))
X_KIND, X_EARLY, Y_OWN, Y_PAIR, PAIR_A, PAIR_FULL, Z_KIND, Z_EARLY, Z_LATE, SIBLING, C_KIND = range(11)


def kernel(a_ref, b_ref, out_ref, a_buf, b_buf, acc, stage, load_sem, y_recv, y_fwd, pair_recv, pair_full, x_recv, x_fwd, z_recv, z_late, sib_recv, sib_late, c_recv, send_sem):
    z, y, r = lax.axis_index("depth"), lax.axis_index("col"), lax.axis_index("row")
    x, c = r // 2, r % 2
    rows, width = a_ref.shape
    half = width // 2
    tile = half // 4
    early = rows // 4

    pair = z + 1 - 2 * (z % 2)
    mirror = 3 - z
    side = ((z + 1) // 2) % 2
    z_of = (z, mirror, pair, 3 - pair)

    y_peer = ({"col": (y + 1) % 4}, {"col": (y + 3) % 4})
    x_peer = ({"row": ((x + 1) % 4) * 2 + c}, {"row": ((x + 3) % 4) * 2 + c})
    to_pair, to_mirror, to_sibling = {"depth": pair}, {"depth": mirror}, {"row": x * 2 + 1 - c}
    peers = y_peer + x_peer + (to_pair, to_mirror, to_sibling)

    def remote(src, dst, kind, recv, where):
        return pltpu.make_async_remote_copy(src_ref=src, dst_ref=dst, send_sem=send_sem.at[kind], recv_sem=recv, device_id=where, device_id_type=MESH)

    def arrived(ref, recv):
        remote(ref, ref, 0, recv, to_sibling).wait_recv()

    def sent(ref, kind):
        remote(ref, ref, kind, z_recv.at[0], to_sibling).wait_send()

    part_rows = (pl.ds(0, rows), pl.ds(rows, rows))
    early_rows, late_rows = pl.ds(0, early), pl.ds(early, rows - early)
    my_cols = pl.ds(pl.multiple_of(side * half, half), half)
    other_cols = pl.ds(pl.multiple_of((1 - side) * half, half), half)

    def a_load(g, cc):
        which = c + cc - 2 * c * cc
        start = pl.multiple_of(which * half + z_of[g] * rows, rows)
        return pltpu.make_async_copy(a_ref.at[:, pl.ds(start, rows)], a_buf.at[0, g, cc, part_rows[0]], load_sem.at[g * 2 + cc])

    def a_loaded(g):
        for cc in range(2):
            a_load(g, cc).wait()

    b_load = pltpu.make_async_copy(b_ref.at[:, my_cols], b_buf.at[0, 0, 0], load_sem.at[8])
    b_load.start()
    for g in (0, 2, 3, 1):
        for cc in range(2):
            a_load(g, cc).start()

    barrier = pltpu.get_barrier_semaphore()
    for where in peers:
        pl.semaphore_signal(barrier, inc=1, device_id=where, device_id_type=MESH)
    pl.semaphore_wait(barrier, len(peers))

    slot_of = (3, 1)

    def step_refs(s, slot, piece=None, core=0):
        g, early_only, first, count = X_STEPS[s]
        size = early if early_only else rows
        at = pl.ds(0, size) if piece is None else pl.ds(piece * (size // 2), size // 2)
        return b_buf.at[slot, g, core, at, pl.ds(first * tile, count * tile)]

    def x_kind(s):
        return X_EARLY if X_STEPS[s][1] else X_KIND

    def send_x(s):
        for d in range(2):
            for h in (d, 1 - d):
                remote(step_refs(s, 0, h), step_refs(s, slot_of[d], h), x_kind(s), x_recv.at[d, s, h], x_peer[d]).start()

    def forward_x(s):
        for d in range(2):
            arrived(step_refs(s, slot_of[d], d), x_recv.at[d, s, d])
            remote(step_refs(s, slot_of[d], d), step_refs(s, 2, d), x_kind(s), x_fwd.at[d, s], x_peer[d]).start()

    def send_sibling(j, s):
        remote(step_refs(s, j), step_refs(s, j, core=1), SIBLING, sib_recv.at[j, s], to_sibling).start()

    def near_x(s):
        for d in range(2):
            arrived(step_refs(s, slot_of[d], 1 - d), x_recv.at[d, s, 1 - d])
            send_sibling(slot_of[d], s)

    def far_x(s):
        for d in range(2):
            arrived(step_refs(s, 2, d), x_fwd.at[d, s])
        send_sibling(2, s)

    def sibling_arrived(s):
        for j in range(4):
            arrived(step_refs(s, j, core=1), sib_recv.at[j, s])

    def send_late(j):
        remote(b_buf.at[j, 0, 0, late_rows], b_buf.at[j, 1, 0, late_rows], Z_LATE, z_late.at[j], to_mirror).start()

    def late_arrived(j):
        arrived(b_buf.at[j, 1, 0, late_rows], z_late.at[j])
        remote(b_buf.at[j, 1, 0, late_rows], b_buf.at[j, 1, 1, late_rows], SIBLING, sib_late.at[j], to_sibling).start()

    def sibling_late_arrived(j):
        arrived(b_buf.at[j, 1, 1, late_rows], sib_late.at[j])

    def send_y(g, part):
        for d in range(2):
            for cc in (d, 1 - d):
                remote(a_buf.at[0, g, cc, part_rows[part]], a_buf.at[slot_of[d], g, cc, part_rows[part]], Y_OWN + part, y_recv.at[d, g, part, cc], y_peer[d]).start()

    def forward_y(g, part):
        for d in range(2):
            got = a_buf.at[slot_of[d], g, d, part_rows[part]]
            arrived(got, y_recv.at[d, g, part, d])
            remote(got, a_buf.at[2, g, d, part_rows[part]], Y_OWN + part, y_fwd.at[d, g, part], y_peer[d]).start()

    def near_y(g, part):
        for d in range(2):
            arrived(a_buf.at[slot_of[d], g, 1 - d, part_rows[part]], y_recv.at[d, g, part, 1 - d])

    def far_y(g, part):
        for d in range(2):
            arrived(a_buf.at[2, g, d, part_rows[part]], y_fwd.at[d, g, part])

    def send_pair(g):
        for cc in range(2):
            remote(a_buf.at[0, (g + 2) % 4, cc, part_rows[0]], a_buf.at[0, g, cc, part_rows[1]], PAIR_A, pair_recv.at[g, cc], to_pair).start()

    def pair_arrived(g):
        for cc in range(2):
            arrived(a_buf.at[0, g, cc, part_rows[1]], pair_recv.at[g, cc])

    def send_pair_full(i):
        remote(a_buf.at[i, 1, :, part_rows[0]], a_buf.at[i, 3, :, part_rows[1]], PAIR_FULL, pair_full.at[i], to_pair).start()

    def pair_full_arrived():
        for i in range(4):
            arrived(a_buf.at[i, 3, :, part_rows[1]], pair_full.at[i])

    def compute(g, part, tiles=(0, 4), slots=(0, 1, 2, 3), by_a=False, add=True, last=False):
        def body(n, carry):
            at = pl.multiple_of(n * tile, tile)
            cols = pl.ds(at, tile)
            total = None
            for slot in slots:
                i, j = (slot, (y + slot - x + 4) % 4) if by_a else ((x + slot - y + 4) % 4, slot)
                for cc in range(2):
                    term = jnp.dot(a_buf[i, g, cc, part_rows[part], :], b_buf[j, g, cc, :, cols], preferred_element_type=jnp.float32)
                    total = term if total is None else total + term
            if add:
                total = total + acc[part_rows[part], cols]
            if not last:
                acc[part_rows[part], cols] = total
            elif part == 1:
                stage[:, cols] = total.astype(stage.dtype)
            else:
                out_ref[:, pl.ds(pl.multiple_of(side * half + at, tile), tile)] = total.astype(out_ref.dtype)
            return carry

        lax.fori_loop(tiles[0], tiles[0] + tiles[1], body, 0)

    def out_cols(of_side, k):
        first, count = C_PIECES[k]
        return pl.ds(pl.multiple_of(of_side * half + first * tile, tile), count * tile)

    def send_c(k):
        first, count = C_PIECES[k]
        remote(stage.at[:, pl.ds(first * tile, count * tile)], out_ref.at[:, out_cols(side, k)], C_KIND, c_recv.at[k], to_pair).start()

    b_load.wait()
    send_x(0)
    remote(b_buf.at[0, 0, 0, early_rows], b_buf.at[0, 1, 0, early_rows], Z_EARLY, z_recv.at[1], to_mirror).start()
    send_late(0)
    a_loaded(0)
    send_y(0, 0)
    a_loaded(2)
    send_pair(0)
    remote(b_ref.at[:, other_cols], b_buf.at[0, 2, 0], Z_KIND, z_recv.at[2], to_pair).start()
    a_loaded(3)
    send_pair(1)
    send_pair(2)
    a_loaded(1)
    send_sibling(0, 0)

    forward_y(0, 0)
    send_y(1, 0)
    send_pair_full(0)
    forward_x(0)
    arrived(step_refs(1, 0), z_recv.at[1])
    send_x(1)
    send_sibling(0, 1)
    near_x(0)
    send_late(3)
    forward_y(1, 0)
    pair_arrived(0)
    send_y(0, 1)
    arrived(b_buf.at[0, 2, 0], z_recv.at[2])
    remote(b_buf.at[0, 2, 0], b_buf.at[0, 3, 0], Z_KIND, z_recv.at[3], to_mirror).start()
    send_x(2)
    send_late(1)
    far_x(0)
    send_late(2)
    send_sibling(0, 2)
    near_y(1, 0)
    send_pair_full(1)
    send_pair_full(3)
    far_y(1, 0)
    send_pair_full(2)
    forward_x(1)
    forward_y(0, 1)
    pair_arrived(1)
    send_y(1, 1)
    near_x(1)
    far_x(1)

    near_y(0, 0)
    far_y(0, 0)
    sibling_arrived(0)
    compute(0, 0, add=False)

    forward_x(2)
    forward_y(1, 1)
    pair_arrived(2)
    send_y(2, 1)
    near_y(0, 1)
    far_y(0, 1)
    compute(0, 1, add=False)

    arrived(b_buf.at[0, 3, 0], z_recv.at[3])
    send_x(3)
    send_x(4)
    for s in (3, 4, 5):
        send_sibling(0, s)
    near_x(2)
    late_arrived(0)
    late_arrived(3)
    forward_y(2, 1)
    send_y(2, 0)
    send_y(3, 0)
    far_x(2)

    forward_x(3)
    send_x(5)
    near_y(1, 1)
    far_y(1, 1)
    late_arrived(1)
    sibling_arrived(1)
    for j in (0, 3, 1):
        sibling_late_arrived(j)
    compute(1, 1, slots=(0, 3, 1))
    forward_y(2, 0)
    near_x(3)
    near_y(2, 1)
    far_y(2, 1)
    sibling_arrived(2)
    compute(2, 1)
    forward_x(4)
    far_x(3)
    late_arrived(2)
    forward_y(3, 0)
    sibling_late_arrived(2)
    compute(1, 1, slots=(2,))
    forward_x(5)
    near_x(4)

    pair_full_arrived()
    sibling_arrived(3)
    compute(3, 1, tiles=(0, 2), last=True)
    send_c(0)
    far_x(4)
    near_x(5)
    sibling_arrived(4)
    compute(3, 1, tiles=(2, 1), last=True)
    send_c(1)
    far_x(5)
    compute(1, 0)
    sibling_arrived(5)
    compute(3, 1, tiles=(3, 1), last=True)
    send_c(2)
    near_y(2, 0)
    far_y(2, 0)
    compute(2, 0)
    near_y(3, 0)
    compute(3, 0, slots=(0, 1, 3), by_a=True)
    far_y(3, 0)
    compute(3, 0, slots=(2,), by_a=True, last=True)

    sent(b_buf.at[pl.ds(0, 3), pl.ds(0, 3), 0], X_KIND)
    sent(b_buf.at[pl.ds(0, 3), 0, 0, early_rows], X_EARLY)
    sent(a_buf.at[pl.ds(0, 3), :, :, part_rows[0]], Y_OWN)
    sent(a_buf.at[pl.ds(0, 3), pl.ds(0, 3), :, part_rows[1]], Y_PAIR)
    sent(a_buf.at[0, pl.ds(0, 3), :, part_rows[0]], PAIR_A)
    sent(a_buf.at[:, 0, :, part_rows[0]], PAIR_FULL)
    sent(b_buf.at[0, pl.ds(0, 2), 0], Z_KIND)
    sent(b_buf.at[0, 0, 0, early_rows], Z_EARLY)
    sent(b_buf.at[:, 0, 0, late_rows], Z_LATE)
    sent(b_buf.at[:, :, 0], SIBLING)
    sent(stage, C_KIND)
    for k in range(len(C_PIECES)):
        arrived(out_ref.at[:, out_cols(1 - side, k)], c_recv.at[k])


def solution(mesh):
    def product(a_blk, b_blk):
        rows, width = a_blk.shape
        half = width // 2
        dma = pltpu.SemaphoreType.DMA
        return pl.pallas_call(
            kernel,
            out_shape=pltpu.VMEM((rows, width), jnp.bfloat16),
            in_specs=[pl.BlockSpec(memory_space=pltpu.HBM)] * 2,
            out_specs=pl.BlockSpec(memory_space=pltpu.VMEM),
            scratch_shapes=[
                pltpu.VMEM((4, GROUPS, 2, 2 * rows, rows), jnp.bfloat16),
                pltpu.VMEM((4, GROUPS, 2, rows, half), jnp.bfloat16),
                pltpu.VMEM((2 * rows, half), jnp.float32),
                pltpu.VMEM((rows, half), jnp.bfloat16),
                dma((9,)),
                dma((2, GROUPS, 2, 2)),
                dma((2, GROUPS, 2)),
                dma((GROUPS, 2)),
                dma((4,)),
                dma((2, len(X_STEPS), 2)),
                dma((2, len(X_STEPS))),
                dma((GROUPS,)),
                dma((4,)),
                dma((4, len(X_STEPS))),
                dma((4,)),
                dma((len(C_PIECES),)),
                dma((11,)),
            ],
            compiler_params=pltpu.CompilerParams(collective_id=0, has_side_effects=True, vmem_limit_bytes=56 * 1024 * 1024),
        )(a_blk, b_blk)

    block_spec = P(("row", "depth"), "col")
    return jax.shard_map(product, mesh=mesh, in_specs=(block_spec, block_spec), out_specs=block_spec, check_vma=False)
```

```python
import jax
import jax.numpy as jnp
from jax import lax
from jax.experimental import pallas as pl
from jax.experimental.pallas import tpu as pltpu
from jax.sharding import PartitionSpec as P

MESH = pl.DeviceIdType.MESH
GROUPS = 4
X_STEPS = ((0, False, 0, 4), (1, True, 0, 4), (2, False, 0, 4), (3, False, 0, 2), (3, False, 2, 1), (3, False, 3, 1))
C_PIECES = ((0, 2), (2, 1), (3, 1))
X_KIND, X_EARLY, Y_OWN, Y_PAIR, PAIR_A, PAIR_FULL, Z_KIND, Z_EARLY, Z_LATE, SIBLING, C_KIND = range(11)


def kernel(a_ref, b_ref, out_ref, a_buf, b_buf, acc, stage, load_sem, y_recv, y_fwd, pair_recv, pair_full, x_recv, x_fwd, z_recv, z_late, sib_recv, sib_late, c_recv, send_sem):
    z, y, r = lax.axis_index("depth"), lax.axis_index("col"), lax.axis_index("row")
    x, c = r // 2, r % 2
    rows, width = a_ref.shape
    half = width // 2
    tile = half // 4
    early = rows // 4

    pair = z + 1 - 2 * (z % 2)
    mirror = 3 - z
    side = ((z + 1) // 2) % 2
    z_of = (z, mirror, pair, 3 - pair)

    y_peer = ({"col": (y + 1) % 4}, {"col": (y + 3) % 4})
    x_peer = ({"row": ((x + 1) % 4) * 2 + c}, {"row": ((x + 3) % 4) * 2 + c})
    to_pair, to_mirror, to_sibling = {"depth": pair}, {"depth": mirror}, {"row": x * 2 + 1 - c}
    peers = y_peer + x_peer + (to_pair, to_mirror, to_sibling)

    def remote(src, dst, kind, recv, where):
        return pltpu.make_async_remote_copy(src_ref=src, dst_ref=dst, send_sem=send_sem.at[kind], recv_sem=recv, device_id=where, device_id_type=MESH)

    def arrived(ref, recv):
        remote(ref, ref, 0, recv, to_sibling).wait_recv()

    def sent(ref, kind):
        remote(ref, ref, kind, z_recv.at[0], to_sibling).wait_send()

    part_rows = (pl.ds(0, rows), pl.ds(rows, rows))
    early_rows, late_rows = pl.ds(0, early), pl.ds(early, rows - early)
    my_cols = pl.ds(pl.multiple_of(side * half, half), half)
    other_cols = pl.ds(pl.multiple_of((1 - side) * half, half), half)

    def a_load(g, cc):
        which = c + cc - 2 * c * cc
        start = pl.multiple_of(which * half + z_of[g] * rows, rows)
        return pltpu.make_async_copy(a_ref.at[:, pl.ds(start, rows)], a_buf.at[0, g, cc, part_rows[0]], load_sem.at[g * 2 + cc])

    def b_loaded():
        b_load.wait()

    def a_loaded(g):
        for cc in range(2):
            a_load(g, cc).wait()

    b_load = pltpu.make_async_copy(b_ref.at[:, my_cols], b_buf.at[0, 0, 0], load_sem.at[8])
    b_load.start()
    for g in (0, 2, 3, 1):
        for cc in range(2):
            a_load(g, cc).start()

    barrier = pltpu.get_barrier_semaphore()
    for where in peers:
        pl.semaphore_signal(barrier, inc=1, device_id=where, device_id_type=MESH)
    pl.semaphore_wait(barrier, len(peers))

    slot_of = (3, 1)

    def step_refs(s, slot, piece=None, core=0):
        g, early_only, first, count = X_STEPS[s]
        size = early if early_only else rows
        at = pl.ds(0, size) if piece is None else pl.ds(piece * (size // 2), size // 2)
        return b_buf.at[slot, g, core, at, pl.ds(first * tile, count * tile)]

    def x_kind(s):
        return X_EARLY if X_STEPS[s][1] else X_KIND

    def send_x(s):
        for d in range(2):
            for h in (d, 1 - d):
                remote(step_refs(s, 0, h), step_refs(s, slot_of[d], h), x_kind(s), x_recv.at[d, s, h], x_peer[d]).start()

    def forward_x(s):
        for d in range(2):
            arrived(step_refs(s, slot_of[d], d), x_recv.at[d, s, d])
            remote(step_refs(s, slot_of[d], d), step_refs(s, 2, d), x_kind(s), x_fwd.at[d, s], x_peer[d]).start()

    def send_sibling(j, s):
        remote(step_refs(s, j), step_refs(s, j, core=1), SIBLING, sib_recv.at[j, s], to_sibling).start()

    def near_x(s):
        for d in range(2):
            arrived(step_refs(s, slot_of[d], 1 - d), x_recv.at[d, s, 1 - d])
            send_sibling(slot_of[d], s)

    def far_x(s):
        for d in range(2):
            arrived(step_refs(s, 2, d), x_fwd.at[d, s])
        send_sibling(2, s)

    def sibling_arrived(s):
        for j in range(4):
            arrived(step_refs(s, j, core=1), sib_recv.at[j, s])

    def send_late(j):
        remote(b_buf.at[j, 0, 0, late_rows], b_buf.at[j, 1, 0, late_rows], Z_LATE, z_late.at[j], to_mirror).start()

    def late_arrived(j):
        arrived(b_buf.at[j, 1, 0, late_rows], z_late.at[j])
        remote(b_buf.at[j, 1, 0, late_rows], b_buf.at[j, 1, 1, late_rows], SIBLING, sib_late.at[j], to_sibling).start()

    def sibling_late_arrived(j):
        arrived(b_buf.at[j, 1, 1, late_rows], sib_late.at[j])

    def send_y(g, part):
        for d in range(2):
            for cc in (d, 1 - d):
                remote(a_buf.at[0, g, cc, part_rows[part]], a_buf.at[slot_of[d], g, cc, part_rows[part]], Y_OWN + part, y_recv.at[d, g, part, cc], y_peer[d]).start()

    def forward_y(g, part):
        for d in range(2):
            got = a_buf.at[slot_of[d], g, d, part_rows[part]]
            arrived(got, y_recv.at[d, g, part, d])
            remote(got, a_buf.at[2, g, d, part_rows[part]], Y_OWN + part, y_fwd.at[d, g, part], y_peer[d]).start()

    def near_y(g, part):
        for d in range(2):
            arrived(a_buf.at[slot_of[d], g, 1 - d, part_rows[part]], y_recv.at[d, g, part, 1 - d])

    def far_y(g, part):
        for d in range(2):
            arrived(a_buf.at[2, g, d, part_rows[part]], y_fwd.at[d, g, part])

    def send_pair(g):
        for cc in range(2):
            remote(a_buf.at[0, (g + 2) % 4, cc, part_rows[0]], a_buf.at[0, g, cc, part_rows[1]], PAIR_A, pair_recv.at[g, cc], to_pair).start()

    def pair_arrived(g):
        for cc in range(2):
            arrived(a_buf.at[0, g, cc, part_rows[1]], pair_recv.at[g, cc])

    def send_pair_full(i):
        remote(a_buf.at[i, 1, :, part_rows[0]], a_buf.at[i, 3, :, part_rows[1]], PAIR_FULL, pair_full.at[i], to_pair).start()

    def pair_full_arrived():
        for i in range(4):
            arrived(a_buf.at[i, 3, :, part_rows[1]], pair_full.at[i])

    def send_z_early():
        remote(b_buf.at[0, 0, 0, early_rows], b_buf.at[0, 1, 0, early_rows], Z_EARLY, z_recv.at[1], to_mirror).start()

    def send_z_pair():
        remote(b_ref.at[:, other_cols], b_buf.at[0, 2, 0], Z_KIND, z_recv.at[2], to_pair).start()

    def send_z_mirror():
        remote(b_buf.at[0, 2, 0], b_buf.at[0, 3, 0], Z_KIND, z_recv.at[3], to_mirror).start()

    def z_arrived(g):
        arrived(b_buf.at[0, g, 0, early_rows] if g == 1 else b_buf.at[0, g, 0], z_recv.at[g])

    def compute(g, part, tiles=(0, 4), slots=(0, 1, 2, 3), by_a=False, add=True, last=False):
        def body(n, carry):
            at = pl.multiple_of(n * tile, tile)
            cols = pl.ds(at, tile)
            total = None
            for slot in slots:
                i, j = (slot, (y + slot - x + 4) % 4) if by_a else ((x + slot - y + 4) % 4, slot)
                for cc in range(2):
                    term = jnp.dot(a_buf[i, g, cc, part_rows[part], :], b_buf[j, g, cc, :, cols], preferred_element_type=jnp.float32)
                    total = term if total is None else total + term
            if add:
                total = total + acc[part_rows[part], cols]
            if not last:
                acc[part_rows[part], cols] = total
            elif part == 1:
                stage[:, cols] = total.astype(stage.dtype)
            else:
                out_ref[:, pl.ds(pl.multiple_of(side * half + at, tile), tile)] = total.astype(out_ref.dtype)
            return carry

        lax.fori_loop(tiles[0], tiles[0] + tiles[1], body, 0)

    def out_cols(of_side, k):
        first, count = C_PIECES[k]
        return pl.ds(pl.multiple_of(of_side * half + first * tile, tile), count * tile)

    def send_c(k):
        first, count = C_PIECES[k]
        remote(stage.at[:, pl.ds(first * tile, count * tile)], out_ref.at[:, out_cols(side, k)], C_KIND, c_recv.at[k], to_pair).start()

    b_loaded()
    send_x(0)
    send_z_early()
    send_late(0)
    a_loaded(0)
    send_y(0, 0)
    a_loaded(2)
    send_pair(0)
    send_z_pair()
    a_loaded(3)
    send_pair(1)
    send_pair(2)
    a_loaded(1)
    send_pair_full(0)
    send_sibling(0, 0)

    forward_y(0, 0)
    send_y(1, 0)
    z_arrived(1)
    send_x(1)
    send_sibling(0, 1)
    forward_x(0)
    near_x(0)
    send_late(3)
    forward_y(1, 0)
    pair_arrived(0)
    send_y(0, 1)
    forward_x(1)
    near_y(1, 0)
    send_pair_full(1)
    send_pair_full(3)
    z_arrived(2)
    send_z_mirror()
    send_x(2)
    send_late(1)
    send_sibling(0, 2)
    far_x(0)
    send_late(2)
    far_y(1, 0)
    send_pair_full(2)
    near_x(1)
    near_y(0, 0)
    far_y(0, 0)
    forward_y(0, 1)
    sibling_arrived(0)
    compute(0, 0, add=False)
    pair_arrived(1)
    send_y(1, 1)
    far_x(1)
    near_y(0, 1)
    far_y(0, 1)
    compute(0, 1, add=False)
    forward_x(2)
    forward_y(1, 1)
    pair_arrived(2)
    send_y(2, 1)
    late_arrived(0)
    late_arrived(3)
    sibling_arrived(1)
    for j in (0, 3):
        sibling_late_arrived(j)
    compute(1, 0, slots=(0, 3))
    near_x(2)
    z_arrived(3)
    send_x(3)
    send_x(4)
    for s in (3, 4, 5):
        send_sibling(0, s)
    near_y(1, 1)
    far_y(1, 1)
    compute(1, 1, slots=(0, 3))
    forward_y(2, 1)
    send_y(2, 0)
    send_y(3, 0)
    far_x(2)
    forward_x(3)
    send_x(5)
    near_y(2, 1)
    far_y(2, 1)
    sibling_arrived(2)
    compute(2, 1)
    near_x(3)
    late_arrived(1)
    forward_y(2, 0)
    forward_x(4)
    near_x(4)
    sibling_late_arrived(1)
    compute(1, 1, slots=(1,))
    far_x(3)
    late_arrived(2)
    forward_x(5)
    forward_y(3, 0)
    pair_full_arrived()
    sibling_late_arrived(2)
    compute(1, 1, slots=(2,))
    sibling_arrived(3)
    compute(3, 1, tiles=(0, 2), last=True)
    send_c(0)
    near_x(5)
    far_x(4)
    sibling_arrived(4)
    compute(3, 1, tiles=(2, 1), last=True)
    send_c(1)
    far_x(5)
    sibling_arrived(5)
    compute(3, 1, tiles=(3, 1), last=True)
    send_c(2)
    compute(1, 0, slots=(1, 2))
    near_y(2, 0)
    far_y(2, 0)
    compute(2, 0)
    near_y(3, 0)
    compute(3, 0, slots=(0, 1, 3), by_a=True)
    far_y(3, 0)
    compute(3, 0, slots=(2,), by_a=True, last=True)

    sent(b_buf.at[pl.ds(0, 3), pl.ds(0, 3), 0], X_KIND)
    sent(b_buf.at[pl.ds(0, 3), 0, 0, early_rows], X_EARLY)
    sent(a_buf.at[pl.ds(0, 3), :, :, part_rows[0]], Y_OWN)
    sent(a_buf.at[pl.ds(0, 3), pl.ds(0, 3), :, part_rows[1]], Y_PAIR)
    sent(a_buf.at[0, pl.ds(0, 3), :, part_rows[0]], PAIR_A)
    sent(a_buf.at[:, 0, :, part_rows[0]], PAIR_FULL)
    sent(b_buf.at[0, pl.ds(0, 2), 0], Z_KIND)
    sent(b_buf.at[0, 0, 0, early_rows], Z_EARLY)
    sent(b_buf.at[:, 0, 0, late_rows], Z_LATE)
    sent(b_buf.at[:, :, 0], SIBLING)
    sent(stage, C_KIND)
    for k in range(len(C_PIECES)):
        arrived(out_ref.at[:, out_cols(1 - side, k)], c_recv.at[k])


def solution(mesh):
    def product(a_blk, b_blk):
        rows, width = a_blk.shape
        half = width // 2
        dma = pltpu.SemaphoreType.DMA
        return pl.pallas_call(
            kernel,
            out_shape=pltpu.VMEM((rows, width), jnp.bfloat16),
            in_specs=[pl.BlockSpec(memory_space=pltpu.HBM)] * 2,
            out_specs=pl.BlockSpec(memory_space=pltpu.VMEM),
            scratch_shapes=[
                pltpu.VMEM((4, GROUPS, 2, 2 * rows, rows), jnp.bfloat16),
                pltpu.VMEM((4, GROUPS, 2, rows, half), jnp.bfloat16),
                pltpu.VMEM((2 * rows, half), jnp.float32),
                pltpu.VMEM((rows, half), jnp.bfloat16),
                dma((9,)),
                dma((2, GROUPS, 2, 2)),
                dma((2, GROUPS, 2)),
                dma((GROUPS, 2)),
                dma((4,)),
                dma((2, len(X_STEPS), 2)),
                dma((2, len(X_STEPS))),
                dma((GROUPS,)),
                dma((4,)),
                dma((4, len(X_STEPS))),
                dma((4,)),
                dma((len(C_PIECES),)),
                dma((11,)),
            ],
            compiler_params=pltpu.CompilerParams(collective_id=0, has_side_effects=True, vmem_limit_bytes=56 * 1024 * 1024),
        )(a_blk, b_blk)

    block_spec = P(("row", "depth"), "col")
    return jax.shard_map(product, mesh=mesh, in_specs=(block_spec, block_spec), out_specs=block_spec, check_vma=False)
```

```python
import jax
import jax.numpy as jnp
from jax import lax
from jax.experimental import pallas as pl
from jax.experimental.pallas import tpu as pltpu
from jax.sharding import PartitionSpec as P

MESH = pl.DeviceIdType.MESH
GROUPS = 4
UNITS = 8
ALL, OUTER, INNER, NEAR, FAR = (0, 1, 2, 3), (0, 3), (1, 2), (0, 1, 3), (2,)
X_STEPS = ((0, False, 0, 8), (1, True, 0, 8), (2, False, 0, 8), (3, False, 0, 2), (3, False, 2, 2), (3, False, 4, 2), (3, False, 6, 1), (3, False, 7, 1))
STEPS = range(len(X_STEPS))
LAST_STEPS = [s for s in STEPS if X_STEPS[s][0] == 3]
Y_STEPS = ((0, 0), (1, 0), (0, 1), (1, 1), (2, 1), (3, 1), (2, 0), (3, 0))
LATE = ((0, 0), (0, 1), (3, 0), (3, 1), (1, 0), (2, 0), (1, 1), (2, 1))
PRODUCTS = (
    (0, 0, 4, 4, ALL),
    (0, 1, 4, 4, ALL),
    (0, 0, 0, 4, ALL),
    (0, 1, 0, 4, ALL),
    (1, 0, 0, 4, OUTER),
    (1, 0, 4, 4, OUTER),
    (1, 1, 4, 4, OUTER),
    (2, 1, 0, 4, ALL),
    (1, 1, 0, 4, OUTER),
    (1, 1, 0, 4, INNER),
    (1, 0, 0, 4, INNER),
    (3, 1, 0, 2, ALL),
    (2, 1, 4, 4, ALL),
    (3, 1, 2, 2, ALL),
    (1, 1, 4, 4, INNER),
    (3, 1, 4, 2, ALL),
    (1, 0, 4, 4, INNER),
    (3, 1, 6, 1, ALL),
    (2, 0, 4, 4, ALL),
    (3, 1, 7, 1, ALL),
    (2, 0, 0, 4, ALL),
    (3, 0, 0, 8, NEAR),
    (3, 0, 0, 8, FAR),
)
X_KIND, X_EARLY, Y_OWN, Y_PAIR, Y_LAST, PAIR_A, PAIR_LAST, FULL, FULL_LAST, Z_KIND, Z_EARLY, Z_LATE, SIBLING, C_KIND = range(14)


def stepper(function, order):
    entries = iter(order)

    def step():
        entry = next(entries)
        function(*(entry if isinstance(entry, tuple) else (entry,)))

    return step


def kernel(a_ref, b_ref, out_ref, a_buf, b_buf, acc, stage, load_sem, y_recv, y_fwd, pair_recv, pair_full, x_recv, x_fwd, z_recv, z_late, sib_recv, sib_late, c_recv, send_sem):
    z, y, r = lax.axis_index("depth"), lax.axis_index("col"), lax.axis_index("row")
    x, c = r // 2, r % 2
    rows, width = a_ref.shape
    half = width // 2
    unit = half // UNITS
    early = rows // 4
    over_y = rows * 3 // 8

    pair = z + 1 - 2 * (z % 2)
    mirror = 3 - z
    side = ((z + 1) // 2) % 2
    z_of = (z, mirror, pair, 3 - pair)

    y_peer = ({"col": (y + 1) % 4}, {"col": (y + 3) % 4})
    x_peer = ({"row": ((x + 1) % 4) * 2 + c}, {"row": ((x + 3) % 4) * 2 + c})
    to_pair, to_mirror, to_sibling = {"depth": pair}, {"depth": mirror}, {"row": x * 2 + 1 - c}
    peers = y_peer + x_peer + (to_pair, to_mirror, to_sibling)
    both = range(2)

    def remote(src, dst, kind, recv, where):
        return pltpu.make_async_remote_copy(src_ref=src, dst_ref=dst, send_sem=send_sem.at[kind], recv_sem=recv, device_id=where, device_id_type=MESH)

    waited = set()

    def arrived(ref, recv, *key):
        if key not in waited:
            waited.add(key)
            remote(ref, ref, X_KIND, recv, to_sibling).wait_recv()

    def sent(ref, kind):
        remote(ref, ref, kind, c_recv, to_sibling).wait_send()

    own_rows, pair_rows = part_rows = (pl.ds(0, rows), pl.ds(rows, rows))
    early_rows, late_rows = pl.ds(0, early), pl.ds(early, rows - early)
    col_half = (pl.ds(0, half // 2), pl.ds(half // 2, half // 2))
    my_cols = pl.ds(pl.multiple_of(side * half, half), half)
    other_cols = pl.ds(pl.multiple_of((1 - side) * half, half), half)
    slot_of = (3, 1)

    b_load = pltpu.make_async_copy(b_ref.at[:, my_cols], b_buf.at[0, 0, 0], load_sem.at[GROUPS])
    b_load.start()
    for g in (0, 2, 3, 1):
        for cc in both:
            start = pl.multiple_of((c + cc - 2 * c * cc) * half + z_of[g] * rows, rows)
            pltpu.make_async_copy(a_ref.at[:, pl.ds(start, rows)], a_buf.at[0, g, cc, own_rows], load_sem.at[g]).start()

    barrier = pltpu.get_barrier_semaphore()
    for where in peers:
        pl.semaphore_signal(barrier, inc=1, device_id=where, device_id_type=MESH)
    pl.semaphore_wait(barrier, len(peers))

    def loaded(g):
        arrived(a_buf.at[0, g, :, own_rows], load_sem.at[g], "load", g)

    def x_ref(s, slot, piece=None, core=0):
        g, early_only, first, count = X_STEPS[s]
        size = early if early_only else rows
        at = pl.ds(0, size) if piece is None else pl.ds(piece * (size // 2), size // 2)
        return b_buf.at[slot, g, core, at, pl.ds(first * unit, count * unit)]

    def x_kind(s):
        return X_EARLY if X_STEPS[s][1] else X_KIND

    def x_got(s, n):
        arrived(x_ref(s, 1), x_recv.at[s, n], "x", s, n)

    def far_x_got(s):
        arrived(x_ref(s, 2), x_fwd.at[s], "fx", s)

    def z_got(g):
        if g > 0:
            arrived(b_buf.at[0, g, 0, early_rows] if g == 1 else b_buf.at[0, g, 0], z_recv.at[g - 1], "z", g)

    @lambda f: stepper(f, [(s, n) for s in STEPS for n in both])
    def send_x(s, n):
        z_got(X_STEPS[s][0])
        for d in both:
            h = (d + n) % 2
            remote(x_ref(s, 0, h), x_ref(s, slot_of[d], h), x_kind(s), x_recv.at[s, n], x_peer[d]).start()

    @lambda f: stepper(f, STEPS)
    def forward_x(s):
        x_got(s, 0)
        for d in both:
            remote(x_ref(s, slot_of[d], d), x_ref(s, 2, d), x_kind(s), x_fwd.at[s], x_peer[d]).start()

    def send_sibling(s, j):
        remote(x_ref(s, j), x_ref(s, j, core=1), SIBLING, sib_recv.at[s], to_sibling).start()

    @lambda f: stepper(f, STEPS)
    def sib_own(s):
        z_got(X_STEPS[s][0])
        send_sibling(s, 0)

    @lambda f: stepper(f, STEPS)
    def sib_near(s):
        x_got(s, 0)
        x_got(s, 1)
        for slot in slot_of:
            send_sibling(s, slot)

    @lambda f: stepper(f, STEPS)
    def sib_far(s):
        far_x_got(s)
        send_sibling(s, 2)

    def sibling_got(s):
        arrived(x_ref(s, slice(None), core=1), sib_recv.at[s], "sib", s)

    def send_z_early():
        remote(b_buf.at[0, 0, 0, early_rows], b_buf.at[0, 1, 0, early_rows], Z_EARLY, z_recv.at[0], to_mirror).start()

    def send_z_pair():
        remote(b_ref.at[:, other_cols], b_buf.at[0, 2, 0], Z_KIND, z_recv.at[1], to_pair).start()

    def send_z_mirror():
        z_got(2)
        remote(b_buf.at[0, 2, 0], b_buf.at[0, 3, 0], Z_KIND, z_recv.at[2], to_mirror).start()

    def late_ref(j, k, g=1, core=0):
        return b_buf.at[j, g, core, late_rows, col_half[k]]

    def late_got(j, k):
        arrived(late_ref(j, k), z_late.at[j, k], "late", j, k)

    @lambda f: stepper(f, LATE)
    def send_late(j, k):
        if j == 2:
            far_x_got(0)
        elif j > 0:
            x_got(0, 0)
            x_got(0, 1)
        remote(late_ref(j, k, 0), late_ref(j, k), Z_LATE, z_late.at[j, k], to_mirror).start()

    @lambda f: stepper(f, LATE)
    def late_sibling(j, k):
        late_got(j, k)
        remote(late_ref(j, k), late_ref(j, k, core=1), SIBLING, sib_late.at[int(j in INNER), k], to_sibling).start()

    def late_sibling_got(slots, k):
        arrived(late_ref(pl.ds(0, 2), k, core=1), sib_late.at[int(slots == INNER), k], "sl", slots, k)

    first_rows, second_rows = pl.ds(rows, over_y), pl.ds(rows + over_y, rows - over_y)
    first_own, second_own = pl.ds(0, over_y), pl.ds(over_y, rows - over_y)

    def y_piece(slot, g, part, h):
        if (g, part) == (3, 1):
            return a_buf.at[slot, g, 1, pl.ds(rows + h * (over_y // 2), over_y // 2)]
        return a_buf.at[slot, g, h, part_rows[part]]

    def y_whole(g, part):
        return a_buf.at[1, g, 1, first_rows] if (g, part) == (3, 1) else a_buf.at[1, g, :, part_rows[part]]

    def y_kind(g, part):
        return Y_LAST if (g, part) == (3, 1) else Y_OWN + part

    def y_got(g, part, n):
        arrived(y_whole(g, part), y_recv.at[g, part, n], "y", g, part, n)

    def far_y_got(g, part):
        arrived(y_whole(g, part), y_fwd.at[g, part], "fy", g, part)

    def pair_got(g):
        arrived(a_buf.at[0, g, :, pair_rows] if g < 3 else a_buf.at[0, 3, 1, first_rows], pair_recv.at[g], "pair", g)

    @lambda f: stepper(f, [(g, part, n) for g, part in Y_STEPS for n in both])
    def send_y(g, part, n):
        if part == 1:
            pair_got(g)
        else:
            loaded(g)
        for d in both:
            h = (d + n) % 2
            remote(y_piece(0, g, part, h), y_piece(slot_of[d], g, part, h), y_kind(g, part), y_recv.at[g, part, n], y_peer[d]).start()

    @lambda f: stepper(f, Y_STEPS)
    def forward_y(g, part):
        y_got(g, part, 0)
        for d in both:
            remote(y_piece(slot_of[d], g, part, d), y_piece(2, g, part, d), y_kind(g, part), y_fwd.at[g, part], y_peer[d]).start()

    @lambda f: stepper(f, range(GROUPS))
    def send_pair(g):
        loaded((g + 2) % 4)
        if g < 3:
            remote(a_buf.at[0, (g + 2) % 4, :, own_rows], a_buf.at[0, g, :, pair_rows], PAIR_A, pair_recv.at[g], to_pair).start()
        else:
            remote(a_buf.at[0, 1, 1, first_own], a_buf.at[0, 3, 1, first_rows], PAIR_LAST, pair_recv.at[3], to_pair).start()

    @lambda f: stepper(f, (0, 1, 3, 2))
    def send_full(i):
        if i == 0:
            loaded(1)
        elif i == 2:
            far_y_got(1, 0)
        else:
            y_got(1, 0, 0)
            y_got(1, 0, 1)
        remote(a_buf.at[i, 1, 0, own_rows], a_buf.at[i, 3, 0, pair_rows], FULL, pair_full.at[0], to_pair).start()
        remote(a_buf.at[i, 1, 1, second_own], a_buf.at[i, 3, 1, second_rows], FULL_LAST, pair_full.at[1], to_pair).start()

    def full_got():
        arrived(a_buf.at[:, 3, 0, pair_rows], pair_full.at[0], "full", 0)
        arrived(a_buf.at[:, 3, 1, second_rows], pair_full.at[1], "full", 1)

    def ready(g, part, first, count, slots):
        if part == 0:
            loaded(g)
        else:
            pair_got(g)
        if (g, part) == (3, 1):
            full_got()
        if slots != FAR:
            y_got(g, part, 0)
            y_got(g, part, 1)
        if slots != NEAR:
            far_y_got(g, part)
        z_got(g)
        for s in STEPS:
            step_group, _, step_first, step_count = X_STEPS[s]
            if step_group == g and step_first < first + count and first < step_first + step_count:
                x_got(s, 0)
                x_got(s, 1)
                far_x_got(s)
                sibling_got(s)
        if g == 1:
            for j in slots:
                late_got(j, first * 2 // UNITS)
            late_sibling_got(slots, first * 2 // UNITS)

    @lambda f: stepper(f, PRODUCTS)
    def compute(g, part, first, count, slots):
        ready(g, part, first, count, slots)
        by_a = slots in (NEAR, FAR)
        last = g == 3 and slots != NEAR
        add = g > 0
        size = min(count, 2) * unit

        def body(n, carry=0):
            at = first * unit + n * size
            cols = pl.ds(at if isinstance(n, int) else pl.multiple_of(at, size), size)
            total = None
            for slot in slots:
                i, j = (slot, (y + slot - x + 4) % 4) if by_a else ((x + slot - y + 4) % 4, slot)
                for cc in both:
                    term = jnp.dot(a_buf[i, g, cc, part_rows[part], :], b_buf[j, g, cc, :, cols], preferred_element_type=jnp.float32)
                    total = term if total is None else total + term
            if add:
                total = total + acc[part_rows[part], cols]
            if not last:
                acc[part_rows[part], cols] = total
            elif part == 1:
                stage[:, cols] = total.astype(stage.dtype)
            else:
                out_ref[:, pl.ds(pl.multiple_of(side * half + at, size), size)] = total.astype(out_ref.dtype)
            return carry

        if count <= 2 or slots == FAR:
            for n in range((count + 1) // 2):
                body(n)
        else:
            lax.fori_loop(0, count // 2, body, 0)

    @lambda f: stepper(f, LAST_STEPS)
    def send_c(s):
        _, _, first, count = X_STEPS[s]
        at = pl.ds(pl.multiple_of(side * half + first * unit, unit), count * unit)
        remote(stage.at[:, pl.ds(first * unit, count * unit)], out_ref.at[:, at], C_KIND, c_recv, to_pair).start()

    b_load.wait()
    send_pair()
    send_y()
    send_x()
    send_x()
    send_z_pair()
    send_z_early()
    send_pair()
    send_y()
    send_y()
    send_late()
    send_y()
    send_pair()
    send_x()
    send_x()
    forward_x()
    send_late()
    forward_y()
    sib_own()
    send_y()
    late_sibling()
    send_y()
    sib_near()
    send_late()
    forward_y()
    send_late()
    sib_near()
    sib_own()
    send_z_mirror()
    send_x()
    forward_y()
    send_pair()
    send_y()
    send_late()
    sib_far()
    send_x()
    send_y()
    send_full()
    forward_x()
    forward_x()
    send_full()
    late_sibling()
    send_y()
    send_y()
    late_sibling()
    send_y()
    sib_own()
    send_late()
    compute()
    send_full()
    compute()
    compute()
    sib_own()
    forward_y()
    late_sibling()
    sib_own()
    send_x()
    send_x()
    send_x()
    compute()
    send_late()
    forward_y()
    send_x()
    sib_far()
    sib_far()
    send_y()
    send_y()
    sib_near()
    send_late()
    compute()
    forward_x()
    send_x()
    send_full()
    late_sibling()
    sib_near()
    compute()
    compute()
    forward_y()
    forward_x()
    send_y()
    late_sibling()
    send_y()
    compute()
    compute()
    sib_own()
    send_x()
    compute()
    send_x()
    sib_far()
    sib_near()
    forward_y()
    forward_x()
    compute()
    send_x()
    send_x()
    compute()
    send_c()
    sib_far()
    late_sibling()
    compute()
    compute()
    late_sibling()
    sib_near()
    forward_x()
    send_c()
    sib_far()
    send_y()
    send_x()
    compute()
    forward_x()
    sib_own()
    compute()
    sib_near()
    send_c()
    sib_own()
    forward_y()
    compute()
    sib_far()
    sib_near()
    compute()
    send_c()
    sib_far()
    compute()
    compute()
    send_c()
    compute()
    compute()
    compute()

    sent(b_buf.at[pl.ds(0, 3), pl.ds(0, 3), 0], X_KIND)
    sent(b_buf.at[pl.ds(0, 3), 0, 0, early_rows], X_EARLY)
    sent(a_buf.at[pl.ds(0, 3), :, :, own_rows], Y_OWN)
    sent(a_buf.at[pl.ds(0, 3), pl.ds(0, 3), :, pair_rows], Y_PAIR)
    sent(a_buf.at[pl.ds(0, 3), 3, 1, first_rows], Y_LAST)
    sent(a_buf.at[0, pl.ds(0, 3), :, own_rows], PAIR_A)
    sent(a_buf.at[0, 3, 1, first_rows], PAIR_LAST)
    sent(a_buf.at[:, 0, 0, own_rows], FULL)
    sent(a_buf.at[:, 3, 1, second_rows], FULL_LAST)
    sent(b_buf.at[0, pl.ds(0, 2), 0], Z_KIND)
    sent(b_buf.at[0, 0, 0, early_rows], Z_EARLY)
    sent(b_buf.at[:, 0, 0, late_rows], Z_LATE)
    sent(b_buf.at[:, :, 0], SIBLING)
    sent(stage, C_KIND)
    arrived(out_ref.at[:, other_cols], c_recv, "c")


def solution(mesh):
    def product(a_blk, b_blk):
        rows, width = a_blk.shape
        half = width // 2
        dma = pltpu.SemaphoreType.DMA
        return pl.pallas_call(
            kernel,
            out_shape=pltpu.VMEM((rows, width), jnp.bfloat16),
            in_specs=[pl.BlockSpec(memory_space=pltpu.HBM)] * 2,
            out_specs=pl.BlockSpec(memory_space=pltpu.VMEM),
            scratch_shapes=[
                pltpu.VMEM((4, GROUPS, 2, 2 * rows, rows), jnp.bfloat16),
                pltpu.VMEM((4, GROUPS, 2, rows, half), jnp.bfloat16),
                pltpu.VMEM((2 * rows, half), jnp.float32),
                pltpu.VMEM((rows, half), jnp.bfloat16),
                dma((GROUPS + 1,)),
                dma((GROUPS, 2, 2)),
                dma((GROUPS, 2)),
                dma((GROUPS,)),
                dma((2,)),
                dma((len(X_STEPS), 2)),
                dma((len(X_STEPS),)),
                dma((3,)),
                dma((4, 2)),
                dma((len(X_STEPS),)),
                dma((2, 2)),
                dma(()),
                dma((14,)),
            ],
            compiler_params=pltpu.CompilerParams(collective_id=0, has_side_effects=True, vmem_limit_bytes=56 * 1024 * 1024),
        )(a_blk, b_blk)

    block_spec = P(("row", "depth"), "col")
    return jax.shard_map(product, mesh=mesh, in_specs=(block_spec, block_spec), out_specs=block_spec, check_vma=False)
```

```python
import jax
import jax.numpy as jnp
from jax import lax
from jax.experimental import pallas as pl
from jax.experimental.pallas import tpu as pltpu
from jax.sharding import PartitionSpec as P

MESH = pl.DeviceIdType.MESH
GROUPS = 4
UNITS = 8
ALL, OUTER, INNER, NEAR, FAR = (0, 1, 2, 3), (0, 3), (1, 2), (0, 1, 3), (2,)
X_STEPS = ((0, False, 0, 8), (1, True, 0, 8), (2, False, 0, 8), (3, False, 0, 2), (3, False, 2, 2), (3, False, 4, 2), (3, False, 6, 1), (3, False, 7, 1))
STEPS = range(len(X_STEPS))
LAST_STEPS = [s for s in STEPS if X_STEPS[s][0] == 3]
Y_STEPS = ((0, 0), (1, 0), (0, 1), (1, 1), (2, 1), (3, 1), (2, 0), (3, 0))
LATE = ((0, 0), (0, 1), (3, 0), (3, 1), (1, 0), (2, 0), (1, 1), (2, 1))
PRODUCTS = (
    (0, 0, 4, 4, ALL),
    (0, 1, 4, 4, ALL),
    (0, 0, 0, 4, ALL),
    (0, 1, 0, 4, ALL),
    (1, 0, 0, 4, OUTER),
    (1, 0, 4, 4, OUTER),
    (1, 1, 4, 4, OUTER),
    (2, 1, 0, 4, ALL),
    (1, 1, 0, 4, OUTER),
    (1, 1, 0, 4, INNER),
    (1, 0, 0, 4, INNER),
    (3, 1, 0, 2, ALL),
    (2, 1, 4, 4, ALL),
    (3, 1, 2, 2, ALL),
    (1, 1, 4, 4, INNER),
    (3, 1, 4, 2, ALL),
    (1, 0, 4, 4, INNER),
    (3, 1, 6, 1, ALL),
    (2, 0, 4, 4, ALL),
    (3, 1, 7, 1, ALL),
    (2, 0, 0, 4, ALL),
    (3, 0, 0, 8, NEAR),
    (3, 0, 0, 8, FAR),
)
BIG, SMALL = range(2)


def stepper(function, order):
    entries = iter(order)

    def step():
        entry = next(entries)
        function(*(entry if isinstance(entry, tuple) else (entry,)))

    return step


def kernel(a_ref, b_ref, out_ref, a_buf, b_buf, acc, stage, load_sem, y_recv, y_fwd, pair_recv, pair_full, x_recv, x_fwd, z_recv, z_late, sib_recv, sib_late, c_recv, send_sem):
    z, y, r = lax.axis_index("depth"), lax.axis_index("col"), lax.axis_index("row")
    x, c = r // 2, r % 2
    rows, width = a_ref.shape
    half = width // 2
    unit = half // UNITS
    early = rows // 4
    over_y = rows * 3 // 8

    pair = z + 1 - 2 * (z % 2)
    mirror = 3 - z
    side = ((z + 1) // 2) % 2
    z_of = (z, mirror, pair, 3 - pair)

    y_peer = ({"col": (y + 1) % 4}, {"col": (y + 3) % 4})
    x_peer = ({"row": ((x + 1) % 4) * 2 + c}, {"row": ((x + 3) % 4) * 2 + c})
    to_pair, to_mirror, to_sibling = {"depth": pair}, {"depth": mirror}, {"row": x * 2 + 1 - c}
    peers = y_peer + x_peer + (to_pair, to_mirror, to_sibling)
    both = range(2)

    def remote(src, dst, kind, recv, where):
        return pltpu.make_async_remote_copy(src_ref=src, dst_ref=dst, send_sem=send_sem.at[kind], recv_sem=recv, device_id=where, device_id_type=MESH)

    waited = set()

    def arrived(ref, recv, *key):
        if key not in waited:
            waited.add(key)
            remote(ref, ref, BIG, recv, to_sibling).wait_recv()

    def sent(ref, kind):
        remote(ref, ref, kind, c_recv, to_sibling).wait_send()

    own_rows, pair_rows = part_rows = (pl.ds(0, rows), pl.ds(rows, rows))
    early_rows, late_rows = pl.ds(0, early), pl.ds(early, rows - early)
    col_half = (pl.ds(0, half // 2), pl.ds(half // 2, half // 2))
    my_cols = pl.ds(pl.multiple_of(side * half, half), half)
    other_cols = pl.ds(pl.multiple_of((1 - side) * half, half), half)
    slot_of = (3, 1)

    b_load = pltpu.make_async_copy(b_ref.at[:, my_cols], b_buf.at[0, 0, 0], load_sem.at[1])
    b_load.start()
    for g in range(GROUPS):
        for cc in both:
            start = pl.multiple_of((c + cc - 2 * c * cc) * half + z_of[g] * rows, rows)
            pltpu.make_async_copy(a_ref.at[:, pl.ds(start, rows)], a_buf.at[0, g, cc, own_rows], load_sem.at[0]).start()

    barrier = pltpu.get_barrier_semaphore()
    for where in peers:
        pl.semaphore_signal(barrier, inc=1, device_id=where, device_id_type=MESH)
    pl.semaphore_wait(barrier, len(peers))

    def loaded():
        arrived(a_buf.at[0, :, :, own_rows], load_sem.at[0], "load")

    def x_ref(s, slot, piece=None, core=0):
        g, early_only, first, count = X_STEPS[s]
        size = early if early_only else rows
        at = pl.ds(0, size) if piece is None else pl.ds(piece * (size // 2), size // 2)
        return b_buf.at[slot, g, core, at, pl.ds(first * unit, count * unit)]

    def x_kind(s):
        return SMALL if X_STEPS[s][1] else BIG

    def x_got(s, n):
        arrived(x_ref(s, 1), x_recv.at[s, n], "x", s, n)

    def far_x_got(s):
        arrived(x_ref(s, 2), x_fwd.at[s], "fx", s)

    def z_got(g):
        if g > 0:
            arrived(b_buf.at[0, g, 0, early_rows] if g == 1 else b_buf.at[0, g, 0], z_recv.at[g - 1], "z", g)

    @lambda f: stepper(f, [(s, n) for s in STEPS for n in both])
    def send_x(s, n):
        z_got(X_STEPS[s][0])
        for d in both:
            h = (d + n) % 2
            remote(x_ref(s, 0, h), x_ref(s, slot_of[d], h), x_kind(s), x_recv.at[s, n], x_peer[d]).start()

    @lambda f: stepper(f, STEPS)
    def forward_x(s):
        x_got(s, 0)
        for d in both:
            remote(x_ref(s, slot_of[d], d), x_ref(s, 2, d), x_kind(s), x_fwd.at[s], x_peer[d]).start()

    def send_sibling(s, j):
        remote(x_ref(s, j), x_ref(s, j, core=1), BIG, sib_recv.at[s], to_sibling).start()

    @lambda f: stepper(f, STEPS)
    def sib_own(s):
        z_got(X_STEPS[s][0])
        send_sibling(s, 0)

    @lambda f: stepper(f, STEPS)
    def sib_near(s):
        x_got(s, 0)
        x_got(s, 1)
        for slot in slot_of:
            send_sibling(s, slot)

    @lambda f: stepper(f, STEPS)
    def sib_far(s):
        far_x_got(s)
        send_sibling(s, 2)

    def sibling_got(s):
        arrived(x_ref(s, slice(None), core=1), sib_recv.at[s], "sib", s)

    def send_z_early():
        remote(b_buf.at[0, 0, 0, early_rows], b_buf.at[0, 1, 0, early_rows], SMALL, z_recv.at[0], to_mirror).start()

    def send_z_pair():
        remote(b_ref.at[:, other_cols], b_buf.at[0, 2, 0], BIG, z_recv.at[1], to_pair).start()

    def send_z_mirror():
        z_got(2)
        remote(b_buf.at[0, 2, 0], b_buf.at[0, 3, 0], BIG, z_recv.at[2], to_mirror).start()

    def late_ref(j, k, g=1, core=0):
        return b_buf.at[j, g, core, late_rows, col_half[k]]

    def late_got(j, k):
        arrived(late_ref(j, k), z_late.at[j, k], "late", j, k)

    @lambda f: stepper(f, LATE)
    def send_late(j, k):
        if j == 2:
            far_x_got(0)
        elif j > 0:
            x_got(0, 0)
            x_got(0, 1)
        remote(late_ref(j, k, 0), late_ref(j, k), BIG, z_late.at[j, k], to_mirror).start()

    @lambda f: stepper(f, LATE)
    def late_sibling(j, k):
        late_got(j, k)
        remote(late_ref(j, k), late_ref(j, k, core=1), BIG, sib_late.at[int(j in INNER), k], to_sibling).start()

    def late_sibling_got(slots, k):
        arrived(late_ref(pl.ds(0, 2), k, core=1), sib_late.at[int(slots == INNER), k], "sl", slots, k)

    first_rows, second_rows = pl.ds(rows, over_y), pl.ds(rows + over_y, rows - over_y)
    first_own, second_own = pl.ds(0, over_y), pl.ds(over_y, rows - over_y)

    def y_piece(slot, g, part, h):
        if (g, part) == (3, 1):
            return a_buf.at[slot, g, 1, pl.ds(rows + h * (over_y // 2), over_y // 2)]
        return a_buf.at[slot, g, h, part_rows[part]]

    def y_whole(g, part):
        return a_buf.at[1, g, 1, first_rows] if (g, part) == (3, 1) else a_buf.at[1, g, :, part_rows[part]]

    def y_got(g, part, n):
        arrived(y_whole(g, part), y_recv.at[g, part, n], "y", g, part, n)

    def far_y_got(g, part):
        arrived(y_whole(g, part), y_fwd.at[g, part], "fy", g, part)

    def pair_got(g):
        arrived(a_buf.at[0, g, :, pair_rows] if g < 3 else a_buf.at[0, 3, 1, first_rows], pair_recv.at[g], "pair", g)

    @lambda f: stepper(f, [(g, part, n) for g, part in Y_STEPS for n in both])
    def send_y(g, part, n):
        if part == 1:
            pair_got(g)
        else:
            loaded()
        for d in both:
            h = (d + n) % 2
            remote(y_piece(0, g, part, h), y_piece(slot_of[d], g, part, h), SMALL, y_recv.at[g, part, n], y_peer[d]).start()

    @lambda f: stepper(f, Y_STEPS)
    def forward_y(g, part):
        y_got(g, part, 0)
        for d in both:
            remote(y_piece(slot_of[d], g, part, d), y_piece(2, g, part, d), SMALL, y_fwd.at[g, part], y_peer[d]).start()

    @lambda f: stepper(f, range(GROUPS))
    def send_pair(g):
        loaded()
        if g < 3:
            remote(a_buf.at[0, (g + 2) % 4, :, own_rows], a_buf.at[0, g, :, pair_rows], SMALL, pair_recv.at[g], to_pair).start()
        else:
            remote(a_buf.at[0, 1, 1, first_own], a_buf.at[0, 3, 1, first_rows], SMALL, pair_recv.at[3], to_pair).start()

    @lambda f: stepper(f, (0, 1, 3, 2))
    def send_full(i):
        if i == 0:
            loaded()
        elif i == 2:
            far_y_got(1, 0)
        else:
            y_got(1, 0, 0)
            y_got(1, 0, 1)
        remote(a_buf.at[i, 1, 0, own_rows], a_buf.at[i, 3, 0, pair_rows], BIG, pair_full.at[0], to_pair).start()
        remote(a_buf.at[i, 1, 1, second_own], a_buf.at[i, 3, 1, second_rows], SMALL, pair_full.at[1], to_pair).start()

    def full_got():
        arrived(a_buf.at[:, 3, 0, pair_rows], pair_full.at[0], "full", 0)
        arrived(a_buf.at[:, 3, 1, second_rows], pair_full.at[1], "full", 1)

    def ready(g, part, first, count, slots):
        if part == 0:
            loaded()
        else:
            pair_got(g)
        if (g, part) == (3, 1):
            full_got()
        if slots != FAR:
            y_got(g, part, 0)
            y_got(g, part, 1)
        if slots != NEAR:
            far_y_got(g, part)
        z_got(g)
        for s in STEPS:
            step_group, _, step_first, step_count = X_STEPS[s]
            if step_group == g and step_first < first + count and first < step_first + step_count:
                x_got(s, 0)
                x_got(s, 1)
                far_x_got(s)
                sibling_got(s)
        if g == 1:
            for j in slots:
                late_got(j, first * 2 // UNITS)
            late_sibling_got(slots, first * 2 // UNITS)

    @lambda f: stepper(f, PRODUCTS)
    def compute(g, part, first, count, slots):
        ready(g, part, first, count, slots)
        by_a = slots in (NEAR, FAR)
        last = g == 3 and slots != NEAR
        add = g > 0
        size = min(count, 2) * unit

        def body(n, carry=0):
            at = first * unit + n * size
            cols = pl.ds(at if isinstance(n, int) else pl.multiple_of(at, size), size)
            total = None
            for slot in slots:
                i, j = (slot, (y + slot - x + 4) % 4) if by_a else ((x + slot - y + 4) % 4, slot)
                for cc in both:
                    term = jnp.dot(a_buf[i, g, cc, part_rows[part], :], b_buf[j, g, cc, :, cols], preferred_element_type=jnp.float32)
                    total = term if total is None else total + term
            if add:
                total = total + acc[part_rows[part], cols]
            if not last:
                acc[part_rows[part], cols] = total
            elif part == 1:
                stage[:, cols] = total.astype(stage.dtype)
            else:
                out_ref[:, pl.ds(pl.multiple_of(side * half + at, size), size)] = total.astype(out_ref.dtype)
            return carry

        if count <= 2 or slots == FAR:
            for n in range((count + 1) // 2):
                body(n)
        else:
            lax.fori_loop(0, count // 2, body, 0)

    @lambda f: stepper(f, LAST_STEPS)
    def send_c(s):
        _, _, first, count = X_STEPS[s]
        at = pl.ds(pl.multiple_of(side * half + first * unit, unit), count * unit)
        remote(stage.at[:, pl.ds(first * unit, count * unit)], out_ref.at[:, at], BIG, c_recv, to_pair).start()

    b_load.wait()
    send_pair()
    send_y()
    send_x()
    send_x()
    send_z_pair()
    send_z_early()
    send_pair()
    send_y()
    send_y()
    send_late()
    send_y()
    send_pair()
    send_x()
    send_x()
    forward_x()
    send_late()
    forward_y()
    sib_own()
    send_y()
    late_sibling()
    send_y()
    sib_near()
    send_late()
    forward_y()
    send_late()
    sib_near()
    sib_own()
    send_z_mirror()
    send_x()
    forward_y()
    send_pair()
    send_y()
    send_late()
    sib_far()
    send_x()
    send_y()
    send_full()
    forward_x()
    forward_x()
    send_full()
    late_sibling()
    send_y()
    send_y()
    late_sibling()
    send_y()
    sib_own()
    send_late()
    compute()
    send_full()
    compute()
    compute()
    sib_own()
    forward_y()
    late_sibling()
    sib_own()
    send_x()
    send_x()
    send_x()
    compute()
    send_late()
    forward_y()
    send_x()
    sib_far()
    sib_far()
    send_y()
    send_y()
    sib_near()
    send_late()
    compute()
    forward_x()
    send_x()
    send_full()
    late_sibling()
    sib_near()
    compute()
    compute()
    forward_y()
    forward_x()
    send_y()
    late_sibling()
    send_y()
    compute()
    compute()
    sib_own()
    send_x()
    compute()
    send_x()
    sib_far()
    sib_near()
    forward_y()
    forward_x()
    compute()
    send_x()
    send_x()
    compute()
    send_c()
    sib_far()
    late_sibling()
    compute()
    compute()
    late_sibling()
    sib_near()
    forward_x()
    send_c()
    sib_far()
    send_y()
    send_x()
    compute()
    forward_x()
    sib_own()
    compute()
    sib_near()
    send_c()
    sib_own()
    forward_y()
    compute()
    sib_far()
    sib_near()
    compute()
    send_c()
    sib_far()
    compute()
    compute()
    send_c()
    compute()
    compute()
    compute()

    sent(b_buf, BIG)
    sent(a_buf.at[:, :, :, pl.ds(0, rows + rows * 3 // 4)], SMALL)
    arrived(out_ref.at[:, other_cols], c_recv, "c")


def solution(mesh):
    def product(a_blk, b_blk):
        rows, width = a_blk.shape
        half = width // 2
        dma = pltpu.SemaphoreType.DMA
        return pl.pallas_call(
            kernel,
            out_shape=pltpu.VMEM((rows, width), jnp.bfloat16),
            in_specs=[pl.BlockSpec(memory_space=pltpu.HBM)] * 2,
            out_specs=pl.BlockSpec(memory_space=pltpu.VMEM),
            scratch_shapes=[
                pltpu.VMEM((4, GROUPS, 2, 2 * rows, rows), jnp.bfloat16),
                pltpu.VMEM((4, GROUPS, 2, rows, half), jnp.bfloat16),
                pltpu.VMEM((2 * rows, half), jnp.float32),
                pltpu.VMEM((rows, half), jnp.bfloat16),
                dma((2,)),
                dma((GROUPS, 2, 2)),
                dma((GROUPS, 2)),
                dma((GROUPS,)),
                dma((2,)),
                dma((len(X_STEPS), 2)),
                dma((len(X_STEPS),)),
                dma((3,)),
                dma((4, 2)),
                dma((len(X_STEPS),)),
                dma((2, 2)),
                dma(()),
                dma((2,)),
            ],
            compiler_params=pltpu.CompilerParams(collective_id=0, has_side_effects=True, vmem_limit_bytes=56 * 1024 * 1024),
        )(a_blk, b_blk)

    block_spec = P(("row", "depth"), "col")
    return jax.shard_map(product, mesh=mesh, in_specs=(block_spec, block_spec), out_specs=block_spec, check_vma=False)
```

```python
import jax
import jax.numpy as jnp
from jax import lax
from jax.experimental import pallas as pl
from jax.experimental.pallas import tpu as pltpu
from jax.sharding import PartitionSpec as P

MESH = pl.DeviceIdType.MESH
GROUPS = 4
UNITS = 8
ALL, OUTER, INNER, NEAR, FAR = (0, 1, 2, 3), (0, 3), (1, 2), (0, 1, 3), (2,)
X_STEPS = ((0, False, 0, 8), (1, True, 0, 8), (2, False, 0, 8), (3, False, 0, 2), (3, False, 2, 2), (3, False, 4, 2), (3, False, 6, 1), (3, False, 7, 1))
STEPS = range(len(X_STEPS))
LAST_STEPS = [s for s in STEPS if X_STEPS[s][0] == 3]
Y_STEPS = ((0, 0), (1, 0), (0, 1), (1, 1), (2, 1), (3, 1), (2, 0), (3, 0))
LATE = ((0, 0), (0, 1), (3, 0), (3, 1), (1, 0), (2, 0), (1, 1), (2, 1))
PRODUCTS = (
    (0, 0, 4, 4, ALL),
    (0, 1, 4, 4, ALL),
    (0, 0, 0, 4, ALL),
    (0, 1, 0, 4, ALL),
    (1, 0, 0, 4, OUTER),
    (1, 0, 4, 4, OUTER),
    (1, 1, 4, 4, OUTER),
    (2, 1, 0, 4, ALL),
    (1, 1, 0, 4, OUTER),
    (1, 1, 0, 4, INNER),
    (1, 0, 0, 4, INNER),
    (3, 1, 0, 2, ALL),
    (2, 1, 4, 4, ALL),
    (3, 1, 2, 2, ALL),
    (1, 1, 4, 4, INNER),
    (3, 1, 4, 2, ALL),
    (1, 0, 4, 4, INNER),
    (3, 1, 6, 1, ALL),
    (2, 0, 4, 4, ALL),
    (3, 1, 7, 1, ALL),
    (2, 0, 0, 4, ALL),
    (3, 0, 0, 8, NEAR),
    (3, 0, 0, 8, FAR),
)
BIG, SMALL = range(2)


def stepper(function, order):
    entries = iter(order)

    def step():
        entry = next(entries)
        function(*(entry if isinstance(entry, tuple) else (entry,)))

    return step


def kernel(a_ref, b_ref, out_ref, a_buf, b_buf, acc, stage, load_sem, y_recv, y_fwd, pair_recv, pair_full, x_recv, x_fwd, z_recv, z_late, sib_recv, sib_late, c_recv, send_sem, ready):
    z, y, r = lax.axis_index("depth"), lax.axis_index("col"), lax.axis_index("row")
    x, c = r // 2, r % 2
    rows, width = a_ref.shape
    half = width // 2
    unit = half // UNITS
    early = rows // 4
    over_y = rows * 3 // 8

    pair = z + 1 - 2 * (z % 2)
    mirror = 3 - z
    side = ((z + 1) // 2) % 2
    z_of = (z, mirror, pair, 3 - pair)

    y_peer = ({"col": (y + 1) % 4}, {"col": (y + 3) % 4})
    x_peer = ({"row": ((x + 1) % 4) * 2 + c}, {"row": ((x + 3) % 4) * 2 + c})
    to_pair, to_mirror, to_sibling = {"depth": pair}, {"depth": mirror}, {"row": x * 2 + 1 - c}
    peers = y_peer + x_peer + (to_pair, to_mirror, to_sibling)
    both = range(2)

    def remote(src, dst, kind, recv, where):
        return pltpu.make_async_remote_copy(src_ref=src, dst_ref=dst, send_sem=send_sem.at[kind], recv_sem=recv, device_id=where, device_id_type=MESH)

    waited = set()

    def arrived(ref, recv, *key):
        if key not in waited:
            waited.add(key)
            remote(ref, ref, BIG, recv, to_sibling).wait_recv()

    def sent(ref, kind):
        remote(ref, ref, kind, c_recv, to_sibling).wait_send()

    own_rows, pair_rows = part_rows = (pl.ds(0, rows), pl.ds(rows, rows))
    early_rows, late_rows = pl.ds(0, early), pl.ds(early, rows - early)
    col_half = (pl.ds(0, half // 2), pl.ds(half // 2, half // 2))
    my_cols = pl.ds(pl.multiple_of(side * half, half), half)
    other_cols = pl.ds(pl.multiple_of((1 - side) * half, half), half)
    slot_of = (3, 1)

    b_load = pltpu.make_async_copy(b_ref.at[:, my_cols], b_buf.at[0, 0, 0], load_sem.at[1])
    b_load.start()
    for g in range(GROUPS):
        for cc in both:
            start = pl.multiple_of((c + cc - 2 * c * cc) * half + z_of[g] * rows, rows)
            pltpu.make_async_copy(a_ref.at[:, pl.ds(start, rows)], a_buf.at[0, g, cc, own_rows], load_sem.at[0]).start()

    MIRROR = 5
    lower = ((y + 1) % 4 < y, (y + 3) % 4 < y, (x + 1) % 4 < x, (x + 3) % 4 < x, pair < z, mirror < z, c == 0)
    seen_there_as = (1, 0, 3, 2, 4, MIRROR, 6)
    barrier = pltpu.get_barrier_semaphore()
    for is_lower, where in zip(lower, peers):

        @pl.when(jnp.logical_not(is_lower))
        def _(where=where):
            pl.semaphore_signal(barrier, inc=1, device_id=where, device_id_type=MESH)

    awaited = sum(is_lower.astype(jnp.int32) for is_lower in lower)

    @pl.when(awaited > 0)
    def _():
        pl.semaphore_wait(barrier, awaited)

    for is_lower, where, index in zip(lower, peers, seen_there_as):

        @pl.when(is_lower)
        def _(where=where, index=index):
            pl.semaphore_signal(ready.at[index], inc=1, device_id=where, device_id_type=MESH)

    def met(peer):
        if ("met", peer) not in waited:
            waited.add(("met", peer))

            @pl.when(jnp.logical_not(lower[peer]))
            def _():
                pl.semaphore_wait(ready.at[peer], 1)

    def loaded():
        arrived(a_buf.at[0, :, :, own_rows], load_sem.at[0], "load")

    def x_ref(s, slot, piece=None, core=0):
        g, early_only, first, count = X_STEPS[s]
        size = early if early_only else rows
        at = pl.ds(0, size) if piece is None else pl.ds(piece * (size // 2), size // 2)
        return b_buf.at[slot, g, core, at, pl.ds(first * unit, count * unit)]

    def x_kind(s):
        return SMALL if X_STEPS[s][1] else BIG

    def x_got(s, n):
        arrived(x_ref(s, 1), x_recv.at[s, n], "x", s, n)

    def far_x_got(s):
        arrived(x_ref(s, 2), x_fwd.at[s], "fx", s)

    def z_got(g):
        if g > 0:
            arrived(b_buf.at[0, g, 0, early_rows] if g == 1 else b_buf.at[0, g, 0], z_recv.at[g - 1], "z", g)

    @lambda f: stepper(f, [(s, n) for s in STEPS for n in both])
    def send_x(s, n):
        z_got(X_STEPS[s][0])
        for d in both:
            h = (d + n) % 2
            remote(x_ref(s, 0, h), x_ref(s, slot_of[d], h), x_kind(s), x_recv.at[s, n], x_peer[d]).start()

    @lambda f: stepper(f, STEPS)
    def forward_x(s):
        x_got(s, 0)
        for d in both:
            remote(x_ref(s, slot_of[d], d), x_ref(s, 2, d), x_kind(s), x_fwd.at[s], x_peer[d]).start()

    def send_sibling(s, j):
        remote(x_ref(s, j), x_ref(s, j, core=1), BIG, sib_recv.at[s], to_sibling).start()

    @lambda f: stepper(f, STEPS)
    def sib_own(s):
        z_got(X_STEPS[s][0])
        send_sibling(s, 0)

    @lambda f: stepper(f, STEPS)
    def sib_near(s):
        x_got(s, 0)
        x_got(s, 1)
        for slot in slot_of:
            send_sibling(s, slot)

    @lambda f: stepper(f, STEPS)
    def sib_far(s):
        far_x_got(s)
        send_sibling(s, 2)

    def sibling_got(s):
        arrived(x_ref(s, slice(None), core=1), sib_recv.at[s], "sib", s)

    def send_z_early():
        met(MIRROR)
        remote(b_buf.at[0, 0, 0, early_rows], b_buf.at[0, 1, 0, early_rows], SMALL, z_recv.at[0], to_mirror).start()

    def send_z_pair():
        remote(b_ref.at[:, other_cols], b_buf.at[0, 2, 0], BIG, z_recv.at[1], to_pair).start()

    def send_z_mirror():
        z_got(2)
        remote(b_buf.at[0, 2, 0], b_buf.at[0, 3, 0], BIG, z_recv.at[2], to_mirror).start()

    def late_ref(j, k, g=1, core=0):
        return b_buf.at[j, g, core, late_rows, col_half[k]]

    def late_got(j, k):
        arrived(late_ref(j, k), z_late.at[j, k], "late", j, k)

    @lambda f: stepper(f, LATE)
    def send_late(j, k):
        if j == 2:
            far_x_got(0)
        elif j > 0:
            x_got(0, 0)
            x_got(0, 1)
        met(MIRROR)
        remote(late_ref(j, k, 0), late_ref(j, k), BIG, z_late.at[j, k], to_mirror).start()

    @lambda f: stepper(f, LATE)
    def late_sibling(j, k):
        late_got(j, k)
        remote(late_ref(j, k), late_ref(j, k, core=1), BIG, sib_late.at[int(j in INNER), k], to_sibling).start()

    def late_sibling_got(slots, k):
        arrived(late_ref(pl.ds(0, 2), k, core=1), sib_late.at[int(slots == INNER), k], "sl", slots, k)

    first_rows, second_rows = pl.ds(rows, over_y), pl.ds(rows + over_y, rows - over_y)
    first_own, second_own = pl.ds(0, over_y), pl.ds(over_y, rows - over_y)

    def y_piece(slot, g, part, h):
        if (g, part) == (3, 1):
            return a_buf.at[slot, g, 1, pl.ds(rows + h * (over_y // 2), over_y // 2)]
        return a_buf.at[slot, g, h, part_rows[part]]

    def y_whole(g, part):
        return a_buf.at[1, g, 1, first_rows] if (g, part) == (3, 1) else a_buf.at[1, g, :, part_rows[part]]

    def y_got(g, part, n):
        arrived(y_whole(g, part), y_recv.at[g, part, n], "y", g, part, n)

    def far_y_got(g, part):
        arrived(y_whole(g, part), y_fwd.at[g, part], "fy", g, part)

    def pair_got(g):
        arrived(a_buf.at[0, g, :, pair_rows] if g < 3 else a_buf.at[0, 3, 1, first_rows], pair_recv.at[g], "pair", g)

    @lambda f: stepper(f, [(g, part, n) for g, part in Y_STEPS for n in both])
    def send_y(g, part, n):
        if part == 1:
            pair_got(g)
        else:
            loaded()
        for d in both:
            h = (d + n) % 2
            remote(y_piece(0, g, part, h), y_piece(slot_of[d], g, part, h), SMALL, y_recv.at[g, part, n], y_peer[d]).start()

    @lambda f: stepper(f, Y_STEPS)
    def forward_y(g, part):
        y_got(g, part, 0)
        for d in both:
            remote(y_piece(slot_of[d], g, part, d), y_piece(2, g, part, d), SMALL, y_fwd.at[g, part], y_peer[d]).start()

    @lambda f: stepper(f, range(GROUPS))
    def send_pair(g):
        loaded()
        if g < 3:
            remote(a_buf.at[0, (g + 2) % 4, :, own_rows], a_buf.at[0, g, :, pair_rows], SMALL, pair_recv.at[g], to_pair).start()
        else:
            remote(a_buf.at[0, 1, 1, first_own], a_buf.at[0, 3, 1, first_rows], SMALL, pair_recv.at[3], to_pair).start()

    @lambda f: stepper(f, (0, 1, 3, 2))
    def send_full(i):
        if i == 0:
            loaded()
        elif i == 2:
            far_y_got(1, 0)
        else:
            y_got(1, 0, 0)
            y_got(1, 0, 1)
        remote(a_buf.at[i, 1, 0, own_rows], a_buf.at[i, 3, 0, pair_rows], BIG, pair_full.at[0], to_pair).start()
        remote(a_buf.at[i, 1, 1, second_own], a_buf.at[i, 3, 1, second_rows], SMALL, pair_full.at[1], to_pair).start()

    def full_got():
        arrived(a_buf.at[:, 3, 0, pair_rows], pair_full.at[0], "full", 0)
        arrived(a_buf.at[:, 3, 1, second_rows], pair_full.at[1], "full", 1)

    def inputs_got(g, part, first, count, slots):
        if part == 0:
            loaded()
        else:
            pair_got(g)
        if (g, part) == (3, 1):
            full_got()
        if slots != FAR:
            y_got(g, part, 0)
            y_got(g, part, 1)
        if slots != NEAR:
            far_y_got(g, part)
        z_got(g)
        for s in STEPS:
            step_group, _, step_first, step_count = X_STEPS[s]
            if step_group == g and step_first < first + count and first < step_first + step_count:
                x_got(s, 0)
                x_got(s, 1)
                far_x_got(s)
                sibling_got(s)
        if g == 1:
            for j in slots:
                late_got(j, first * 2 // UNITS)
            late_sibling_got(slots, first * 2 // UNITS)

    @lambda f: stepper(f, PRODUCTS)
    def compute(g, part, first, count, slots):
        inputs_got(g, part, first, count, slots)
        by_a = slots in (NEAR, FAR)
        last = g == 3 and slots != NEAR
        add = g > 0
        size = min(count, 2) * unit

        def body(n, carry=0):
            at = first * unit + n * size
            cols = pl.ds(at if isinstance(n, int) else pl.multiple_of(at, size), size)
            total = None
            for slot in slots:
                i, j = (slot, (y + slot - x + 4) % 4) if by_a else ((x + slot - y + 4) % 4, slot)
                for cc in both:
                    term = jnp.dot(a_buf[i, g, cc, part_rows[part], :], b_buf[j, g, cc, :, cols], preferred_element_type=jnp.float32)
                    total = term if total is None else total + term
            if add:
                total = total + acc[part_rows[part], cols]
            if not last:
                acc[part_rows[part], cols] = total
            elif part == 1:
                stage[:, cols] = total.astype(stage.dtype)
            else:
                out_ref[:, pl.ds(pl.multiple_of(side * half + at, size), size)] = total.astype(out_ref.dtype)
            return carry

        if count <= 2 or slots == FAR:
            for n in range((count + 1) // 2):
                body(n)
        else:
            lax.fori_loop(0, count // 2, body, 0)

    @lambda f: stepper(f, LAST_STEPS)
    def send_c(s):
        _, _, first, count = X_STEPS[s]
        at = pl.ds(pl.multiple_of(side * half + first * unit, unit), count * unit)
        remote(stage.at[:, pl.ds(first * unit, count * unit)], out_ref.at[:, at], BIG, c_recv, to_pair).start()

    b_load.wait()
    for peer in (6, 2, 0, 4, 3, 1):
        met(peer)
    send_pair()
    send_y()
    send_x()
    send_x()
    send_z_pair()
    send_pair()
    send_y()
    send_y()
    send_y()
    send_pair()
    send_z_early()
    send_late()
    send_x()
    send_x()
    forward_x()
    send_late()
    forward_y()
    sib_own()
    send_y()
    late_sibling()
    send_y()
    sib_near()
    send_late()
    forward_y()
    send_late()
    sib_near()
    sib_own()
    send_z_mirror()
    send_x()
    forward_y()
    send_pair()
    send_y()
    send_late()
    sib_far()
    send_x()
    send_y()
    send_full()
    forward_x()
    forward_x()
    send_full()
    late_sibling()
    send_y()
    send_y()
    late_sibling()
    send_y()
    sib_own()
    send_late()
    compute()
    send_full()
    compute()
    compute()
    sib_own()
    forward_y()
    late_sibling()
    sib_own()
    send_x()
    send_x()
    send_x()
    compute()
    send_late()
    forward_y()
    send_x()
    sib_far()
    sib_far()
    send_y()
    send_y()
    sib_near()
    send_late()
    compute()
    forward_x()
    send_x()
    send_full()
    late_sibling()
    sib_near()
    compute()
    compute()
    forward_y()
    forward_x()
    send_y()
    late_sibling()
    send_y()
    compute()
    compute()
    sib_own()
    send_x()
    compute()
    send_x()
    sib_far()
    sib_near()
    forward_y()
    forward_x()
    compute()
    send_x()
    send_x()
    compute()
    send_c()
    sib_far()
    late_sibling()
    compute()
    compute()
    late_sibling()
    sib_near()
    forward_x()
    send_c()
    sib_far()
    send_y()
    send_x()
    compute()
    forward_x()
    sib_own()
    compute()
    sib_near()
    send_c()
    sib_own()
    forward_y()
    compute()
    sib_far()
    sib_near()
    compute()
    send_c()
    sib_far()
    compute()
    compute()
    send_c()
    compute()
    compute()
    compute()

    sent(b_buf, BIG)
    sent(a_buf.at[:, :, :, pl.ds(0, rows + rows * 3 // 4)], SMALL)
    arrived(out_ref.at[:, other_cols], c_recv, "c")


def solution(mesh):
    def product(a_blk, b_blk):
        rows, width = a_blk.shape
        half = width // 2
        dma = pltpu.SemaphoreType.DMA
        return pl.pallas_call(
            kernel,
            out_shape=pltpu.VMEM((rows, width), jnp.bfloat16),
            in_specs=[pl.BlockSpec(memory_space=pltpu.HBM)] * 2,
            out_specs=pl.BlockSpec(memory_space=pltpu.VMEM),
            scratch_shapes=[
                pltpu.VMEM((4, GROUPS, 2, 2 * rows, rows), jnp.bfloat16),
                pltpu.VMEM((4, GROUPS, 2, rows, half), jnp.bfloat16),
                pltpu.VMEM((2 * rows, half), jnp.float32),
                pltpu.VMEM((rows, half), jnp.bfloat16),
                dma((2,)),
                dma((GROUPS, 2, 2)),
                dma((GROUPS, 2)),
                dma((GROUPS,)),
                dma((2,)),
                dma((len(X_STEPS), 2)),
                dma((len(X_STEPS),)),
                dma((3,)),
                dma((4, 2)),
                dma((len(X_STEPS),)),
                dma((2, 2)),
                dma(()),
                dma((2,)),
                pltpu.SemaphoreType.REGULAR((7,)),
            ],
            compiler_params=pltpu.CompilerParams(collective_id=0, has_side_effects=True, vmem_limit_bytes=56 * 1024 * 1024),
        )(a_blk, b_blk)

    block_spec = P(("row", "depth"), "col")
    return jax.shard_map(product, mesh=mesh, in_specs=(block_spec, block_spec), out_specs=block_spec, check_vma=False)
```

```python
import jax
import jax.numpy as jnp
from jax import lax
from jax.experimental import pallas as pl
from jax.experimental.pallas import tpu as pltpu
from jax.sharding import PartitionSpec as P

MESH = pl.DeviceIdType.MESH
GROUPS = 4
UNITS = 8
ALL, OUTER, INNER, NEAR, FAR = (0, 1, 2, 3), (0, 3), (1, 2), (0, 1, 3), (2,)
X_STEPS = ((0, False, 0, 8), (1, True, 0, 8), (2, False, 0, 8), (3, False, 0, 2), (3, False, 2, 2), (3, False, 4, 2), (3, False, 6, 1), (3, False, 7, 1))
STEPS = range(len(X_STEPS))
LAST_STEPS = [s for s in STEPS if X_STEPS[s][0] == 3]
Y_STEPS = ((0, 0), (1, 0), (0, 1), (1, 1), (2, 1), (3, 1), (2, 0), (3, 0))
LATE = ((0, 0), (0, 1), (3, 0), (3, 1), (1, 0), (2, 0), (1, 1), (2, 1))
PRODUCTS = (
    (0, 1, 4, 4, ALL),
    (0, 0, 0, 4, ALL),
    (0, 1, 0, 4, ALL),
    (1, 0, 0, 4, OUTER),
    (1, 1, 0, 4, OUTER),
    (1, 1, 4, 4, OUTER),
    (1, 1, 0, 4, INNER),
    (2, 1, 0, 4, ALL),
    (3, 1, 0, 2, ALL),
    (2, 1, 4, 4, ALL),
    (3, 1, 2, 2, ALL),
    (1, 0, 0, 4, INNER),
    (1, 1, 4, 4, INNER),
    (3, 1, 4, 2, ALL),
    (0, 0, 4, 4, ALL),
    (1, 0, 4, 4, INNER),
    (1, 0, 4, 4, OUTER),
    (3, 1, 6, 1, ALL),
    (2, 0, 4, 4, ALL),
    (3, 1, 7, 1, ALL),
    (3, 0, 0, 8, NEAR),
    (2, 0, 0, 4, ALL),
    (3, 0, 0, 8, FAR),
)
BIG, SMALL = range(2)


def stepper(function, order):
    entries = iter(order)

    def step():
        entry = next(entries)
        function(*(entry if isinstance(entry, tuple) else (entry,)))

    return step


def kernel(a_ref, b_ref, out_ref, a_buf, b_buf, acc, stage, load_sem, y_recv, y_fwd, pair_recv, pair_full, x_recv, x_fwd, z_recv, z_late, sib_recv, sib_late, c_recv, send_sem, ready):
    z, y, r = lax.axis_index("depth"), lax.axis_index("col"), lax.axis_index("row")
    x, c = r // 2, r % 2
    rows, width = a_ref.shape
    half = width // 2
    unit = half // UNITS
    early = rows // 4
    over_y = rows * 3 // 8

    pair = z + 1 - 2 * (z % 2)
    mirror = 3 - z
    side = ((z + 1) // 2) % 2
    z_of = (z, mirror, pair, 3 - pair)

    y_peer = ({"col": (y + 1) % 4}, {"col": (y + 3) % 4})
    x_peer = ({"row": ((x + 1) % 4) * 2 + c}, {"row": ((x + 3) % 4) * 2 + c})
    to_pair, to_mirror, to_sibling = {"depth": pair}, {"depth": mirror}, {"row": x * 2 + 1 - c}
    peers = y_peer + x_peer + (to_pair, to_mirror, to_sibling)
    both = range(2)

    def remote(src, dst, kind, recv, where):
        return pltpu.make_async_remote_copy(src_ref=src, dst_ref=dst, send_sem=send_sem.at[kind], recv_sem=recv, device_id=where, device_id_type=MESH)

    waited = set()

    def arrived(ref, recv, *key):
        if key not in waited:
            waited.add(key)
            remote(ref, ref, BIG, recv, to_sibling).wait_recv()

    def sent(ref, kind):
        remote(ref, ref, kind, c_recv, to_sibling).wait_send()

    own_rows, pair_rows = part_rows = (pl.ds(0, rows), pl.ds(rows, rows))
    early_rows, late_rows = pl.ds(0, early), pl.ds(early, rows - early)
    col_half = (pl.ds(0, half // 2), pl.ds(half // 2, half // 2))
    my_cols = pl.ds(pl.multiple_of(side * half, half), half)
    other_cols = pl.ds(pl.multiple_of((1 - side) * half, half), half)
    slot_of = (3, 1)

    b_load = pltpu.make_async_copy(b_ref.at[:, my_cols], b_buf.at[0, 0, 0], load_sem.at[1])
    b_load.start()
    for g in range(GROUPS):
        for cc in both:
            start = pl.multiple_of((c + cc - 2 * c * cc) * half + z_of[g] * rows, rows)
            pltpu.make_async_copy(a_ref.at[:, pl.ds(start, rows)], a_buf.at[0, g, cc, own_rows], load_sem.at[0]).start()

    MIRROR = 5
    lower = ((y + 1) % 4 < y, (y + 3) % 4 < y, (x + 1) % 4 < x, (x + 3) % 4 < x, pair < z, mirror < z, c == 0)
    seen_there_as = (1, 0, 3, 2, 4, MIRROR, 6)
    barrier = pltpu.get_barrier_semaphore()
    for is_lower, where in zip(lower, peers):

        @pl.when(jnp.logical_not(is_lower))
        def _(where=where):
            pl.semaphore_signal(barrier, inc=1, device_id=where, device_id_type=MESH)

    awaited = sum(is_lower.astype(jnp.int32) for is_lower in lower)

    @pl.when(awaited > 0)
    def _():
        pl.semaphore_wait(barrier, awaited)

    for is_lower, where, index in zip(lower, peers, seen_there_as):

        @pl.when(is_lower)
        def _(where=where, index=index):
            pl.semaphore_signal(ready.at[index], inc=1, device_id=where, device_id_type=MESH)

    def met(peer):
        if ("met", peer) not in waited:
            waited.add(("met", peer))

            @pl.when(jnp.logical_not(lower[peer]))
            def _():
                pl.semaphore_wait(ready.at[peer], 1)

    def loaded():
        arrived(a_buf.at[0, :, :, own_rows], load_sem.at[0], "load")

    def x_ref(s, slot, piece=None, core=0):
        g, early_only, first, count = X_STEPS[s]
        size = early if early_only else rows
        at = pl.ds(0, size) if piece is None else pl.ds(piece * (size // 2), size // 2)
        return b_buf.at[slot, g, core, at, pl.ds(first * unit, count * unit)]

    def x_kind(s):
        return SMALL if X_STEPS[s][1] else BIG

    def x_got(s, n):
        arrived(x_ref(s, 1), x_recv.at[s, n], "x", s, n)

    def far_x_got(s):
        arrived(x_ref(s, 2), x_fwd.at[s], "fx", s)

    def z_got(g):
        if g > 0:
            arrived(b_buf.at[0, g, 0, early_rows] if g == 1 else b_buf.at[0, g, 0], z_recv.at[g - 1], "z", g)

    @lambda f: stepper(f, [(s, n) for s in STEPS for n in both])
    def send_x(s, n):
        z_got(X_STEPS[s][0])
        for d in both:
            h = (d + n) % 2
            remote(x_ref(s, 0, h), x_ref(s, slot_of[d], h), x_kind(s), x_recv.at[s, n], x_peer[d]).start()

    @lambda f: stepper(f, STEPS)
    def forward_x(s):
        x_got(s, 0)
        for d in both:
            remote(x_ref(s, slot_of[d], d), x_ref(s, 2, d), x_kind(s), x_fwd.at[s], x_peer[d]).start()

    def send_sibling(s, j):
        remote(x_ref(s, j), x_ref(s, j, core=1), BIG, sib_recv.at[s], to_sibling).start()

    @lambda f: stepper(f, STEPS)
    def sib_own(s):
        z_got(X_STEPS[s][0])
        send_sibling(s, 0)

    @lambda f: stepper(f, STEPS)
    def sib_near(s):
        x_got(s, 0)
        x_got(s, 1)
        for slot in slot_of:
            send_sibling(s, slot)

    @lambda f: stepper(f, STEPS)
    def sib_far(s):
        far_x_got(s)
        send_sibling(s, 2)

    def sibling_got(s):
        arrived(x_ref(s, slice(None), core=1), sib_recv.at[s], "sib", s)

    def send_z_early():
        met(MIRROR)
        remote(b_buf.at[0, 0, 0, early_rows], b_buf.at[0, 1, 0, early_rows], SMALL, z_recv.at[0], to_mirror).start()

    def send_z_pair():
        remote(b_ref.at[:, other_cols], b_buf.at[0, 2, 0], BIG, z_recv.at[1], to_pair).start()

    def send_z_mirror():
        z_got(2)
        remote(b_buf.at[0, 2, 0], b_buf.at[0, 3, 0], BIG, z_recv.at[2], to_mirror).start()

    def late_ref(j, k, g=1, core=0):
        return b_buf.at[j, g, core, late_rows, col_half[k]]

    def late_got(j, k):
        arrived(late_ref(j, k), z_late.at[j, k], "late", j, k)

    @lambda f: stepper(f, LATE)
    def send_late(j, k):
        if j == 2:
            far_x_got(0)
        elif j > 0:
            x_got(0, 0)
            x_got(0, 1)
        met(MIRROR)
        remote(late_ref(j, k, 0), late_ref(j, k), BIG, z_late.at[j, k], to_mirror).start()

    @lambda f: stepper(f, LATE)
    def late_sibling(j, k):
        late_got(j, k)
        remote(late_ref(j, k), late_ref(j, k, core=1), BIG, sib_late.at[int(j in INNER), k], to_sibling).start()

    def late_sibling_got(slots, k):
        arrived(late_ref(pl.ds(0, 2), k, core=1), sib_late.at[int(slots == INNER), k], "sl", slots, k)

    first_rows, second_rows = pl.ds(rows, over_y), pl.ds(rows + over_y, rows - over_y)
    first_own, second_own = pl.ds(0, over_y), pl.ds(over_y, rows - over_y)

    def y_piece(slot, g, part, h):
        if (g, part) == (3, 1):
            return a_buf.at[slot, g, 1, pl.ds(rows + h * (over_y // 2), over_y // 2)]
        return a_buf.at[slot, g, h, part_rows[part]]

    def y_whole(g, part):
        return a_buf.at[1, g, 1, first_rows] if (g, part) == (3, 1) else a_buf.at[1, g, :, part_rows[part]]

    def y_got(g, part, n):
        arrived(y_whole(g, part), y_recv.at[g, part, n], "y", g, part, n)

    def far_y_got(g, part):
        arrived(y_whole(g, part), y_fwd.at[g, part], "fy", g, part)

    def pair_got(g):
        arrived(a_buf.at[0, g, :, pair_rows] if g < 3 else a_buf.at[0, 3, 1, first_rows], pair_recv.at[g], "pair", g)

    @lambda f: stepper(f, [(g, part, n) for g, part in Y_STEPS for n in both])
    def send_y(g, part, n):
        if part == 1:
            pair_got(g)
        else:
            loaded()
        for d in both:
            h = (d + n) % 2
            remote(y_piece(0, g, part, h), y_piece(slot_of[d], g, part, h), SMALL, y_recv.at[g, part, n], y_peer[d]).start()

    @lambda f: stepper(f, Y_STEPS)
    def forward_y(g, part):
        y_got(g, part, 0)
        for d in both:
            remote(y_piece(slot_of[d], g, part, d), y_piece(2, g, part, d), SMALL, y_fwd.at[g, part], y_peer[d]).start()

    @lambda f: stepper(f, range(GROUPS))
    def send_pair(g):
        loaded()
        if g < 3:
            remote(a_buf.at[0, (g + 2) % 4, :, own_rows], a_buf.at[0, g, :, pair_rows], SMALL, pair_recv.at[g], to_pair).start()
        else:
            remote(a_buf.at[0, 1, 1, first_own], a_buf.at[0, 3, 1, first_rows], SMALL, pair_recv.at[3], to_pair).start()

    @lambda f: stepper(f, (0, 1, 3, 2))
    def send_full(i):
        if i == 0:
            loaded()
        elif i == 2:
            far_y_got(1, 0)
        else:
            y_got(1, 0, 0)
            y_got(1, 0, 1)
        remote(a_buf.at[i, 1, 0, own_rows], a_buf.at[i, 3, 0, pair_rows], BIG, pair_full.at[0], to_pair).start()
        remote(a_buf.at[i, 1, 1, second_own], a_buf.at[i, 3, 1, second_rows], SMALL, pair_full.at[1], to_pair).start()

    def full_got():
        arrived(a_buf.at[:, 3, 0, pair_rows], pair_full.at[0], "full", 0)
        arrived(a_buf.at[:, 3, 1, second_rows], pair_full.at[1], "full", 1)

    def inputs_got(g, part, first, count, slots):
        if part == 0:
            loaded()
        else:
            pair_got(g)
        if (g, part) == (3, 1):
            full_got()
        if slots != FAR:
            y_got(g, part, 0)
            y_got(g, part, 1)
        if slots != NEAR:
            far_y_got(g, part)
        z_got(g)
        for s in STEPS:
            step_group, _, step_first, step_count = X_STEPS[s]
            if step_group == g and step_first < first + count and first < step_first + step_count:
                x_got(s, 0)
                x_got(s, 1)
                far_x_got(s)
                sibling_got(s)
        if g == 1:
            for j in slots:
                late_got(j, first * 2 // UNITS)
            late_sibling_got(slots, first * 2 // UNITS)

    @lambda f: stepper(f, PRODUCTS)
    def compute(g, part, first, count, slots):
        inputs_got(g, part, first, count, slots)
        by_a = slots in (NEAR, FAR)
        last = g == 3 and slots != NEAR
        add = g > 0
        size = min(count, 2) * unit

        def body(n, carry=0):
            at = first * unit + n * size
            cols = pl.ds(at if isinstance(n, int) else pl.multiple_of(at, size), size)
            total = None
            for slot in slots:
                i, j = (slot, (y + slot - x + 4) % 4) if by_a else ((x + slot - y + 4) % 4, slot)
                for cc in both:
                    term = jnp.dot(a_buf[i, g, cc, part_rows[part], :], b_buf[j, g, cc, :, cols], preferred_element_type=jnp.float32)
                    total = term if total is None else total + term
            if add:
                total = total + acc[part_rows[part], cols]
            if not last:
                acc[part_rows[part], cols] = total
            elif part == 1:
                stage[:, cols] = total.astype(stage.dtype)
            else:
                out_ref[:, pl.ds(pl.multiple_of(side * half + at, size), size)] = total.astype(out_ref.dtype)
            return carry

        if count <= 2 or slots == FAR:
            for n in range((count + 1) // 2):
                body(n)
        else:
            lax.fori_loop(0, count // 2, body, 0)

    @lambda f: stepper(f, LAST_STEPS)
    def send_c(s):
        _, _, first, count = X_STEPS[s]
        at = pl.ds(pl.multiple_of(side * half + first * unit, unit), count * unit)
        remote(stage.at[:, pl.ds(first * unit, count * unit)], out_ref.at[:, at], BIG, c_recv, to_pair).start()

    b_load.wait()
    for peer in (6, 2, 0, 4, 3, 1):
        met(peer)
    send_x()
    send_y()
    send_pair()
    send_z_pair()
    send_x()
    send_pair()
    send_y()
    send_y()
    send_y()
    send_pair()
    send_late()
    send_z_early()
    send_late()
    forward_y()
    send_y()
    send_y()
    forward_x()
    forward_y()
    send_late()
    send_x()
    sib_own()
    late_sibling()
    send_pair()
    send_x()
    send_late()
    sib_far()
    send_x()
    send_full()
    forward_y()
    late_sibling()
    send_z_mirror()
    sib_near()
    forward_x()
    send_full()
    send_x()
    late_sibling()
    send_y()
    send_y()
    send_full()
    sib_near()
    send_late()
    forward_y()
    compute()
    sib_own()
    sib_far()
    forward_x()
    send_y()
    send_y()
    sib_own()
    send_late()
    send_y()
    send_late()
    sib_near()
    sib_own()
    send_x()
    send_full()
    send_x()
    compute()
    send_x()
    send_x()
    late_sibling()
    send_y()
    forward_y()
    sib_own()
    send_y()
    sib_own()
    compute()
    forward_y()
    forward_x()
    sib_own()
    sib_far()
    late_sibling()
    send_y()
    send_x()
    compute()
    send_late()
    compute()
    late_sibling()
    send_y()
    forward_x()
    send_x()
    send_x()
    compute()
    sib_own()
    sib_near()
    compute()
    sib_far()
    send_x()
    compute()
    forward_x()
    compute()
    send_x()
    send_c()
    sib_near()
    send_x()
    late_sibling()
    forward_y()
    sib_far()
    compute()
    compute()
    send_y()
    send_c()
    forward_x()
    sib_near()
    late_sibling()
    sib_far()
    compute()
    forward_x()
    compute()
    compute()
    send_c()
    sib_near()
    forward_y()
    compute()
    sib_far()
    compute()
    sib_near()
    compute()
    compute()
    sib_far()
    send_c()
    compute()
    compute()
    send_c()
    compute()
    compute()
    compute()

    sent(b_buf, BIG)
    sent(a_buf.at[:, :, :, pl.ds(0, rows + rows * 3 // 4)], SMALL)
    arrived(out_ref.at[:, other_cols], c_recv, "c")


def solution(mesh):
    def product(a_blk, b_blk):
        rows, width = a_blk.shape
        half = width // 2
        dma = pltpu.SemaphoreType.DMA
        return pl.pallas_call(
            kernel,
            out_shape=pltpu.VMEM((rows, width), jnp.bfloat16),
            in_specs=[pl.BlockSpec(memory_space=pltpu.HBM)] * 2,
            out_specs=pl.BlockSpec(memory_space=pltpu.VMEM),
            scratch_shapes=[
                pltpu.VMEM((4, GROUPS, 2, 2 * rows, rows), jnp.bfloat16),
                pltpu.VMEM((4, GROUPS, 2, rows, half), jnp.bfloat16),
                pltpu.VMEM((2 * rows, half), jnp.float32),
                pltpu.VMEM((rows, half), jnp.bfloat16),
                dma((2,)),
                dma((GROUPS, 2, 2)),
                dma((GROUPS, 2)),
                dma((GROUPS,)),
                dma((2,)),
                dma((len(X_STEPS), 2)),
                dma((len(X_STEPS),)),
                dma((3,)),
                dma((4, 2)),
                dma((len(X_STEPS),)),
                dma((2, 2)),
                dma(()),
                dma((2,)),
                pltpu.SemaphoreType.REGULAR((7,)),
            ],
            compiler_params=pltpu.CompilerParams(collective_id=0, has_side_effects=True, vmem_limit_bytes=56 * 1024 * 1024),
        )(a_blk, b_blk)

    block_spec = P(("row", "depth"), "col")
    return jax.shard_map(product, mesh=mesh, in_specs=(block_spec, block_spec), out_specs=block_spec, check_vma=False)
```

```python
import jax
import jax.numpy as jnp
from jax import lax
from jax.experimental import pallas as pl
from jax.experimental.pallas import tpu as pltpu
from jax.sharding import PartitionSpec as P

MESH = pl.DeviceIdType.MESH
GROUPS = 4
UNITS = 8
ALL, OUTER, INNER, NEAR, FAR = (0, 1, 2, 3), (0, 3), (1, 2), (0, 1, 3), (2,)
X_STEPS = ((0, False, 0, 8), (1, True, 0, 8), (2, False, 0, 8), (3, False, 0, 2), (3, False, 2, 2), (3, False, 4, 2), (3, False, 6, 1), (3, False, 7, 1))
STEPS = range(len(X_STEPS))
LAST_STEPS = [s for s in STEPS if X_STEPS[s][0] == 3]
Y_STEPS = ((0, 0), (1, 0), (0, 1), (1, 1), (2, 1), (3, 1), (2, 0), (3, 0))
LATE = ((0, 0), (0, 1), (3, 0), (3, 1), (1, 0), (2, 0), (1, 1), (2, 1))
PRODUCTS = (
    (0, 1, 4, 4, ALL),
    (0, 0, 0, 4, ALL),
    (0, 1, 0, 4, ALL),
    (1, 0, 0, 4, OUTER),
    (1, 1, 0, 4, OUTER),
    (1, 1, 4, 4, OUTER),
    (1, 1, 0, 4, INNER),
    (2, 1, 0, 4, ALL),
    (3, 1, 0, 2, ALL),
    (2, 1, 4, 4, ALL),
    (3, 1, 2, 2, ALL),
    (1, 0, 0, 4, INNER),
    (1, 1, 4, 4, INNER),
    (3, 1, 4, 2, ALL),
    (0, 0, 4, 4, ALL),
    (1, 0, 4, 4, INNER),
    (1, 0, 4, 4, OUTER),
    (3, 1, 6, 1, ALL),
    (2, 0, 4, 4, ALL),
    (3, 1, 7, 1, ALL),
    (3, 0, 0, 8, NEAR),
    (2, 0, 0, 4, ALL),
    (3, 0, 0, 8, FAR),
)
BIG, SMALL = range(2)


def stepper(function, order):
    entries = iter(order)

    def step():
        entry = next(entries)
        function(*(entry if isinstance(entry, tuple) else (entry,)))

    return step


def kernel(a_ref, b_ref, out_ref, a_buf, b_buf, acc, stage, load_sem, y_recv, y_fwd, pair_recv, pair_full, x_recv, x_fwd, z_recv, z_late, sib_recv, sib_late, c_recv, send_sem):
    z, y, r = lax.axis_index("depth"), lax.axis_index("col"), lax.axis_index("row")
    x, c = r // 2, r % 2
    rows, width = a_ref.shape
    half = width // 2
    unit = half // UNITS
    early = rows // 4
    over_y = rows * 3 // 8

    pair = z + 1 - 2 * (z % 2)
    mirror = 3 - z
    side = ((z + 1) // 2) % 2
    z_of = (z, mirror, pair, 3 - pair)

    y_peer = ({"col": (y + 1) % 4}, {"col": (y + 3) % 4})
    x_peer = ({"row": ((x + 1) % 4) * 2 + c}, {"row": ((x + 3) % 4) * 2 + c})
    to_pair, to_mirror, to_sibling = {"depth": pair}, {"depth": mirror}, {"row": x * 2 + 1 - c}
    peers = y_peer + x_peer + (to_pair, to_mirror, to_sibling)
    both = range(2)

    def remote(src, dst, kind, recv, where):
        return pltpu.make_async_remote_copy(src_ref=src, dst_ref=dst, send_sem=send_sem.at[kind], recv_sem=recv, device_id=where, device_id_type=MESH)

    waited = set()

    def arrived(ref, recv, *key):
        if key not in waited:
            waited.add(key)
            remote(ref, ref, BIG, recv, to_sibling).wait_recv()

    def sent(ref, kind):
        remote(ref, ref, kind, c_recv, to_sibling).wait_send()

    own_rows, pair_rows = part_rows = (pl.ds(0, rows), pl.ds(rows, rows))
    early_rows, late_rows = pl.ds(0, early), pl.ds(early, rows - early)
    col_half = (pl.ds(0, half // 2), pl.ds(half // 2, half // 2))
    my_cols = pl.ds(pl.multiple_of(side * half, half), half)
    other_cols = pl.ds(pl.multiple_of((1 - side) * half, half), half)
    slot_of = (3, 1)

    b_load = pltpu.make_async_copy(b_ref.at[:, my_cols], b_buf.at[0, 0, 0], load_sem.at[1])
    b_load.start()
    for g in range(GROUPS):
        for cc in both:
            start = pl.multiple_of((c + cc - 2 * c * cc) * half + z_of[g] * rows, rows)
            pltpu.make_async_copy(a_ref.at[:, pl.ds(start, rows)], a_buf.at[0, g, cc, own_rows], load_sem.at[0]).start()

    barrier = pltpu.get_barrier_semaphore()
    for where in peers:
        pl.semaphore_signal(barrier, inc=1, device_id=where, device_id_type=MESH)
    pl.semaphore_wait(barrier, len(peers))

    def loaded():
        arrived(a_buf.at[0, :, :, own_rows], load_sem.at[0], "load")

    def x_ref(s, slot, piece=None, core=0):
        g, early_only, first, count = X_STEPS[s]
        size = early if early_only else rows
        at = pl.ds(0, size) if piece is None else pl.ds(piece * (size // 2), size // 2)
        return b_buf.at[slot, g, core, at, pl.ds(first * unit, count * unit)]

    def x_kind(s):
        return SMALL if X_STEPS[s][1] else BIG

    def x_got(s, n):
        arrived(x_ref(s, 1), x_recv.at[s, n], "x", s, n)

    def far_x_got(s):
        arrived(x_ref(s, 2), x_fwd.at[s], "fx", s)

    def z_got(g):
        if g > 0:
            arrived(b_buf.at[0, g, 0, early_rows] if g == 1 else b_buf.at[0, g, 0], z_recv.at[g - 1], "z", g)

    @lambda f: stepper(f, [(s, n) for s in STEPS for n in both])
    def send_x(s, n):
        z_got(X_STEPS[s][0])
        for d in both:
            h = (d + n) % 2
            remote(x_ref(s, 0, h), x_ref(s, slot_of[d], h), x_kind(s), x_recv.at[s, n], x_peer[d]).start()

    @lambda f: stepper(f, STEPS)
    def forward_x(s):
        x_got(s, 0)
        for d in both:
            remote(x_ref(s, slot_of[d], d), x_ref(s, 2, d), x_kind(s), x_fwd.at[s], x_peer[d]).start()

    def send_sibling(s, j):
        remote(x_ref(s, j), x_ref(s, j, core=1), BIG, sib_recv.at[s], to_sibling).start()

    @lambda f: stepper(f, STEPS)
    def sib_own(s):
        z_got(X_STEPS[s][0])
        send_sibling(s, 0)

    @lambda f: stepper(f, STEPS)
    def sib_near(s):
        x_got(s, 0)
        x_got(s, 1)
        for slot in slot_of:
            send_sibling(s, slot)

    @lambda f: stepper(f, STEPS)
    def sib_far(s):
        far_x_got(s)
        send_sibling(s, 2)

    def sibling_got(s):
        arrived(x_ref(s, slice(None), core=1), sib_recv.at[s], "sib", s)

    def send_z_early():
        remote(b_buf.at[0, 0, 0, early_rows], b_buf.at[0, 1, 0, early_rows], SMALL, z_recv.at[0], to_mirror).start()

    def send_z_pair():
        remote(b_ref.at[:, other_cols], b_buf.at[0, 2, 0], BIG, z_recv.at[1], to_pair).start()

    def send_z_mirror():
        z_got(2)
        remote(b_buf.at[0, 2, 0], b_buf.at[0, 3, 0], BIG, z_recv.at[2], to_mirror).start()

    def late_ref(j, k, g=1, core=0):
        return b_buf.at[j, g, core, late_rows, col_half[k]]

    def late_got(j, k):
        arrived(late_ref(j, k), z_late.at[j, k], "late", j, k)

    @lambda f: stepper(f, LATE)
    def send_late(j, k):
        if j == 2:
            far_x_got(0)
        elif j > 0:
            x_got(0, 0)
            x_got(0, 1)
        remote(late_ref(j, k, 0), late_ref(j, k), BIG, z_late.at[j, k], to_mirror).start()

    @lambda f: stepper(f, LATE)
    def late_sibling(j, k):
        late_got(j, k)
        remote(late_ref(j, k), late_ref(j, k, core=1), BIG, sib_late.at[int(j in INNER), k], to_sibling).start()

    def late_sibling_got(slots, k):
        arrived(late_ref(pl.ds(0, 2), k, core=1), sib_late.at[int(slots == INNER), k], "sl", slots, k)

    first_rows, second_rows = pl.ds(rows, over_y), pl.ds(rows + over_y, rows - over_y)
    first_own, second_own = pl.ds(0, over_y), pl.ds(over_y, rows - over_y)

    def y_piece(slot, g, part, h):
        if (g, part) == (3, 1):
            return a_buf.at[slot, g, 1, pl.ds(rows + h * (over_y // 2), over_y // 2)]
        return a_buf.at[slot, g, h, part_rows[part]]

    def y_whole(g, part):
        return a_buf.at[1, g, 1, first_rows] if (g, part) == (3, 1) else a_buf.at[1, g, :, part_rows[part]]

    def y_got(g, part, n):
        arrived(y_whole(g, part), y_recv.at[g, part, n], "y", g, part, n)

    def far_y_got(g, part):
        arrived(y_whole(g, part), y_fwd.at[g, part], "fy", g, part)

    def pair_got(g):
        arrived(a_buf.at[0, g, :, pair_rows] if g < 3 else a_buf.at[0, 3, 1, first_rows], pair_recv.at[g], "pair", g)

    @lambda f: stepper(f, [(g, part, n) for g, part in Y_STEPS for n in both])
    def send_y(g, part, n):
        if part == 1:
            pair_got(g)
        else:
            loaded()
        for d in both:
            h = (d + n) % 2
            remote(y_piece(0, g, part, h), y_piece(slot_of[d], g, part, h), SMALL, y_recv.at[g, part, n], y_peer[d]).start()

    @lambda f: stepper(f, Y_STEPS)
    def forward_y(g, part):
        y_got(g, part, 0)
        for d in both:
            remote(y_piece(slot_of[d], g, part, d), y_piece(2, g, part, d), SMALL, y_fwd.at[g, part], y_peer[d]).start()

    @lambda f: stepper(f, range(GROUPS))
    def send_pair(g):
        loaded()
        if g < 3:
            remote(a_buf.at[0, (g + 2) % 4, :, own_rows], a_buf.at[0, g, :, pair_rows], SMALL, pair_recv.at[g], to_pair).start()
        else:
            remote(a_buf.at[0, 1, 1, first_own], a_buf.at[0, 3, 1, first_rows], SMALL, pair_recv.at[3], to_pair).start()

    @lambda f: stepper(f, (0, 1, 3, 2))
    def send_full(i):
        if i == 0:
            loaded()
        elif i == 2:
            far_y_got(1, 0)
        else:
            y_got(1, 0, 0)
            y_got(1, 0, 1)
        remote(a_buf.at[i, 1, 0, own_rows], a_buf.at[i, 3, 0, pair_rows], BIG, pair_full.at[0], to_pair).start()
        remote(a_buf.at[i, 1, 1, second_own], a_buf.at[i, 3, 1, second_rows], SMALL, pair_full.at[1], to_pair).start()

    def full_got():
        arrived(a_buf.at[:, 3, 0, pair_rows], pair_full.at[0], "full", 0)
        arrived(a_buf.at[:, 3, 1, second_rows], pair_full.at[1], "full", 1)

    def ready(g, part, first, count, slots):
        if part == 0:
            loaded()
        else:
            pair_got(g)
        if (g, part) == (3, 1):
            full_got()
        if slots != FAR:
            y_got(g, part, 0)
            y_got(g, part, 1)
        if slots != NEAR:
            far_y_got(g, part)
        z_got(g)
        for s in STEPS:
            step_group, _, step_first, step_count = X_STEPS[s]
            if step_group == g and step_first < first + count and first < step_first + step_count:
                x_got(s, 0)
                x_got(s, 1)
                far_x_got(s)
                sibling_got(s)
        if g == 1:
            for j in slots:
                late_got(j, first * 2 // UNITS)
            late_sibling_got(slots, first * 2 // UNITS)

    @lambda f: stepper(f, PRODUCTS)
    def compute(g, part, first, count, slots):
        ready(g, part, first, count, slots)
        by_a = slots in (NEAR, FAR)
        last = g == 3 and slots != NEAR
        add = g > 0
        size = min(count, 2) * unit

        def body(n, carry=0):
            at = first * unit + n * size
            cols = pl.ds(at if isinstance(n, int) else pl.multiple_of(at, size), size)
            total = None
            for slot in slots:
                i, j = (slot, (y + slot - x + 4) % 4) if by_a else ((x + slot - y + 4) % 4, slot)
                for cc in both:
                    term = jnp.dot(a_buf[i, g, cc, part_rows[part], :], b_buf[j, g, cc, :, cols], preferred_element_type=jnp.float32)
                    total = term if total is None else total + term
            if add:
                total = total + acc[part_rows[part], cols]
            if not last:
                acc[part_rows[part], cols] = total
            elif part == 1:
                stage[:, cols] = total.astype(stage.dtype)
            else:
                out_ref[:, pl.ds(pl.multiple_of(side * half + at, size), size)] = total.astype(out_ref.dtype)
            return carry

        if count <= 2 or slots == FAR:
            for n in range((count + 1) // 2):
                body(n)
        else:
            lax.fori_loop(0, count // 2, body, 0)

    @lambda f: stepper(f, LAST_STEPS)
    def send_c(s):
        _, _, first, count = X_STEPS[s]
        at = pl.ds(pl.multiple_of(side * half + first * unit, unit), count * unit)
        remote(stage.at[:, pl.ds(first * unit, count * unit)], out_ref.at[:, at], BIG, c_recv, to_pair).start()

    b_load.wait()
    send_x()
    send_y()
    send_pair()
    send_late()
    send_z_pair()
    send_x()
    send_pair()
    send_z_early()
    send_late()
    send_y()
    send_y()
    send_y()
    send_pair()
    forward_y()
    send_y()
    send_y()
    forward_x()
    forward_y()
    send_late()
    send_x()
    sib_own()
    late_sibling()
    send_pair()
    send_x()
    send_late()
    sib_far()
    send_x()
    send_full()
    forward_y()
    late_sibling()
    send_z_mirror()
    sib_near()
    forward_x()
    send_full()
    send_x()
    late_sibling()
    send_y()
    send_y()
    send_full()
    sib_near()
    send_late()
    forward_y()
    compute()
    sib_own()
    sib_far()
    forward_x()
    send_y()
    send_y()
    sib_own()
    send_late()
    send_y()
    send_late()
    sib_near()
    sib_own()
    send_x()
    send_full()
    send_x()
    compute()
    send_x()
    send_x()
    late_sibling()
    send_y()
    forward_y()
    sib_own()
    send_y()
    sib_own()
    compute()
    forward_y()
    forward_x()
    sib_own()
    sib_far()
    late_sibling()
    send_y()
    send_x()
    compute()
    send_late()
    compute()
    late_sibling()
    send_y()
    forward_x()
    send_x()
    send_x()
    compute()
    sib_own()
    sib_near()
    compute()
    sib_far()
    send_x()
    compute()
    forward_x()
    compute()
    send_x()
    send_c()
    sib_near()
    send_x()
    late_sibling()
    forward_y()
    sib_far()
    compute()
    compute()
    send_y()
    send_c()
    forward_x()
    sib_near()
    late_sibling()
    sib_far()
    compute()
    forward_x()
    compute()
    compute()
    send_c()
    sib_near()
    forward_y()
    compute()
    sib_far()
    compute()
    sib_near()
    compute()
    compute()
    sib_far()
    send_c()
    compute()
    compute()
    send_c()
    compute()
    compute()
    compute()

    sent(b_buf, BIG)
    sent(a_buf.at[:, :, :, pl.ds(0, rows + rows * 3 // 4)], SMALL)
    arrived(out_ref.at[:, other_cols], c_recv, "c")


def solution(mesh):
    def product(a_blk, b_blk):
        rows, width = a_blk.shape
        half = width // 2
        dma = pltpu.SemaphoreType.DMA
        return pl.pallas_call(
            kernel,
            out_shape=pltpu.VMEM((rows, width), jnp.bfloat16),
            in_specs=[pl.BlockSpec(memory_space=pltpu.HBM)] * 2,
            out_specs=pl.BlockSpec(memory_space=pltpu.VMEM),
            scratch_shapes=[
                pltpu.VMEM((4, GROUPS, 2, 2 * rows, rows), jnp.bfloat16),
                pltpu.VMEM((4, GROUPS, 2, rows, half), jnp.bfloat16),
                pltpu.VMEM((2 * rows, half), jnp.float32),
                pltpu.VMEM((rows, half), jnp.bfloat16),
                dma((2,)),
                dma((GROUPS, 2, 2)),
                dma((GROUPS, 2)),
                dma((GROUPS,)),
                dma((2,)),
                dma((len(X_STEPS), 2)),
                dma((len(X_STEPS),)),
                dma((3,)),
                dma((4, 2)),
                dma((len(X_STEPS),)),
                dma((2, 2)),
                dma(()),
                dma((2,)),
            ],
            compiler_params=pltpu.CompilerParams(collective_id=0, has_side_effects=True, vmem_limit_bytes=56 * 1024 * 1024),
        )(a_blk, b_blk)

    block_spec = P(("row", "depth"), "col")
    return jax.shard_map(product, mesh=mesh, in_specs=(block_spec, block_spec), out_specs=block_spec, check_vma=False)
```

```python
import jax
import jax.numpy as jnp
from jax import lax
from jax.experimental import pallas as pl
from jax.experimental.pallas import tpu as pltpu
from jax.sharding import PartitionSpec as P

MESH = pl.DeviceIdType.MESH
GROUPS = 4
UNITS = 8
ALL, OUTER, INNER, NEAR, FAR = (0, 1, 2, 3), (0, 3), (1, 2), (0, 1, 3), (2,)
X_STEPS = ((0, False, 0, 8), (1, True, 0, 8), (2, False, 0, 8), (3, False, 0, 2), (3, False, 2, 2), (3, False, 4, 2), (3, False, 6, 1), (3, False, 7, 1))
STEPS = range(len(X_STEPS))
LAST_STEPS = [s for s in STEPS if X_STEPS[s][0] == 3]
Y_STEPS = ((0, 0), (1, 0), (0, 1), (1, 1), (2, 1), (3, 1), (2, 0), (3, 0))
LATE = ((0, 0), (0, 1), (3, 0), (3, 1), (1, 0), (2, 0), (1, 1), (2, 1))
PRODUCTS = (
    (0, 0, 0, 4, ALL),
    (0, 1, 0, 4, ALL),
    (0, 1, 4, 4, ALL),
    (0, 0, 4, 4, ALL),
    (1, 1, 0, 4, OUTER),
    (1, 1, 4, 4, OUTER),
    (2, 1, 0, 4, ALL),
    (1, 1, 0, 4, INNER),
    (1, 0, 4, 4, OUTER),
    (3, 1, 0, 2, ALL),
    (1, 0, 0, 4, OUTER),
    (2, 1, 4, 4, ALL),
    (3, 1, 2, 2, ALL),
    (1, 0, 0, 4, INNER),
    (1, 1, 4, 4, INNER),
    (3, 1, 4, 2, ALL),
    (1, 0, 4, 4, INNER),
    (3, 1, 6, 1, ALL),
    (2, 0, 4, 4, ALL),
    (3, 1, 7, 1, ALL),
    (3, 0, 0, 8, NEAR),
    (2, 0, 0, 4, ALL),
    (3, 0, 0, 8, FAR),
)
BIG, SMALL = range(2)


def stepper(function, order):
    entries = iter(order)

    def step():
        entry = next(entries)
        function(*(entry if isinstance(entry, tuple) else (entry,)))

    return step


def kernel(a_ref, b_ref, out_ref, a_buf, b_buf, acc, stage, load_sem, y_recv, y_fwd, pair_recv, pair_full, x_recv, x_fwd, z_recv, z_late, sib_recv, sib_late, c_recv, send_sem):
    z, y, r = lax.axis_index("depth"), lax.axis_index("col"), lax.axis_index("row")
    x, c = r // 2, r % 2
    rows, width = a_ref.shape
    half = width // 2
    unit = half // UNITS
    early = rows // 4
    over_y = rows * 3 // 8

    pair = z + 1 - 2 * (z % 2)
    mirror = 3 - z
    side = ((z + 1) // 2) % 2
    z_of = (z, mirror, pair, 3 - pair)

    y_peer = ({"col": (y + 1) % 4}, {"col": (y + 3) % 4})
    x_peer = ({"row": ((x + 1) % 4) * 2 + c}, {"row": ((x + 3) % 4) * 2 + c})
    to_pair, to_mirror, to_sibling = {"depth": pair}, {"depth": mirror}, {"row": x * 2 + 1 - c}
    peers = y_peer + x_peer + (to_pair, to_mirror, to_sibling)
    both = range(2)

    def remote(src, dst, kind, recv, where):
        return pltpu.make_async_remote_copy(src_ref=src, dst_ref=dst, send_sem=send_sem.at[kind], recv_sem=recv, device_id=where, device_id_type=MESH)

    waited = set()

    def arrived(ref, recv, *key):
        if key not in waited:
            waited.add(key)
            remote(ref, ref, BIG, recv, to_sibling).wait_recv()

    def sent(ref, kind):
        remote(ref, ref, kind, c_recv, to_sibling).wait_send()

    own_rows, pair_rows = part_rows = (pl.ds(0, rows), pl.ds(rows, rows))
    early_rows, late_rows = pl.ds(0, early), pl.ds(early, rows - early)
    col_half = (pl.ds(0, half // 2), pl.ds(half // 2, half // 2))
    my_cols = pl.ds(pl.multiple_of(side * half, half), half)
    other_cols = pl.ds(pl.multiple_of((1 - side) * half, half), half)
    slot_of = (3, 1)

    b_load = pltpu.make_async_copy(b_ref.at[:, my_cols], b_buf.at[0, 0, 0], load_sem.at[1])
    b_load.start()
    for g in range(GROUPS):
        for cc in both:
            start = pl.multiple_of((c + cc - 2 * c * cc) * half + z_of[g] * rows, rows)
            pltpu.make_async_copy(a_ref.at[:, pl.ds(start, rows)], a_buf.at[0, g, cc, own_rows], load_sem.at[0]).start()

    barrier = pltpu.get_barrier_semaphore()
    for where in peers:
        pl.semaphore_signal(barrier, inc=1, device_id=where, device_id_type=MESH)
    pl.semaphore_wait(barrier, len(peers))

    def loaded():
        arrived(a_buf.at[0, :, :, own_rows], load_sem.at[0], "load")

    def x_ref(s, slot, piece=None, core=0):
        g, early_only, first, count = X_STEPS[s]
        size = early if early_only else rows
        at = pl.ds(0, size) if piece is None else pl.ds(piece * (size // 2), size // 2)
        return b_buf.at[slot, g, core, at, pl.ds(first * unit, count * unit)]

    def x_kind(s):
        return SMALL if X_STEPS[s][1] else BIG

    def x_got(s, n):
        arrived(x_ref(s, 1), x_recv.at[s, n], "x", s, n)

    def far_x_got(s):
        arrived(x_ref(s, 2), x_fwd.at[s], "fx", s)

    def z_got(g):
        if g > 0:
            arrived(b_buf.at[0, g, 0, early_rows] if g == 1 else b_buf.at[0, g, 0], z_recv.at[g - 1], "z", g)

    @lambda f: stepper(f, [(s, n) for s in STEPS for n in both])
    def send_x(s, n):
        z_got(X_STEPS[s][0])
        for d in both:
            h = (d + n) % 2
            remote(x_ref(s, 0, h), x_ref(s, slot_of[d], h), x_kind(s), x_recv.at[s, n], x_peer[d]).start()

    @lambda f: stepper(f, STEPS)
    def forward_x(s):
        x_got(s, 0)
        for d in both:
            remote(x_ref(s, slot_of[d], d), x_ref(s, 2, d), x_kind(s), x_fwd.at[s], x_peer[d]).start()

    def send_sibling(s, j):
        remote(x_ref(s, j), x_ref(s, j, core=1), BIG, sib_recv.at[s], to_sibling).start()

    @lambda f: stepper(f, STEPS)
    def sib_own(s):
        z_got(X_STEPS[s][0])
        send_sibling(s, 0)

    @lambda f: stepper(f, STEPS)
    def sib_near(s):
        x_got(s, 0)
        x_got(s, 1)
        for slot in slot_of:
            send_sibling(s, slot)

    @lambda f: stepper(f, STEPS)
    def sib_far(s):
        far_x_got(s)
        send_sibling(s, 2)

    def sibling_got(s):
        arrived(x_ref(s, slice(None), core=1), sib_recv.at[s], "sib", s)

    def send_z_early():
        remote(b_buf.at[0, 0, 0, early_rows], b_buf.at[0, 1, 0, early_rows], SMALL, z_recv.at[0], to_mirror).start()

    def send_z_pair():
        remote(b_ref.at[:, other_cols], b_buf.at[0, 2, 0], BIG, z_recv.at[1], to_pair).start()

    def send_z_mirror():
        z_got(2)
        remote(b_buf.at[0, 2, 0], b_buf.at[0, 3, 0], BIG, z_recv.at[2], to_mirror).start()

    def late_ref(j, k, g=1, core=0):
        return b_buf.at[j, g, core, late_rows, col_half[k]]

    def late_got(j, k):
        arrived(late_ref(j, k), z_late.at[j, k], "late", j, k)

    @lambda f: stepper(f, LATE)
    def send_late(j, k):
        if j == 2:
            far_x_got(0)
        elif j > 0:
            x_got(0, 0)
            x_got(0, 1)
        remote(late_ref(j, k, 0), late_ref(j, k), BIG, z_late.at[j, k], to_mirror).start()

    @lambda f: stepper(f, LATE)
    def late_sibling(j, k):
        late_got(j, k)
        remote(late_ref(j, k), late_ref(j, k, core=1), BIG, sib_late.at[int(j in INNER), k], to_sibling).start()

    def late_sibling_got(slots, k):
        arrived(late_ref(pl.ds(0, 2), k, core=1), sib_late.at[int(slots == INNER), k], "sl", slots, k)

    first_rows, second_rows = pl.ds(rows, over_y), pl.ds(rows + over_y, rows - over_y)
    first_own, second_own = pl.ds(0, over_y), pl.ds(over_y, rows - over_y)

    def y_piece(slot, g, part, h):
        if (g, part) == (3, 1):
            return a_buf.at[slot, g, 1, pl.ds(rows + h * (over_y // 2), over_y // 2)]
        return a_buf.at[slot, g, h, part_rows[part]]

    def y_whole(g, part):
        return a_buf.at[1, g, 1, first_rows] if (g, part) == (3, 1) else a_buf.at[1, g, :, part_rows[part]]

    def y_got(g, part, n):
        arrived(y_whole(g, part), y_recv.at[g, part, n], "y", g, part, n)

    def far_y_got(g, part):
        arrived(y_whole(g, part), y_fwd.at[g, part], "fy", g, part)

    def pair_got(g):
        arrived(a_buf.at[0, g, :, pair_rows] if g < 3 else a_buf.at[0, 3, 1, first_rows], pair_recv.at[g], "pair", g)

    @lambda f: stepper(f, [(g, part, n) for g, part in Y_STEPS for n in both])
    def send_y(g, part, n):
        if part == 1:
            pair_got(g)
        else:
            loaded()
        for d in both:
            h = (d + n) % 2
            remote(y_piece(0, g, part, h), y_piece(slot_of[d], g, part, h), SMALL, y_recv.at[g, part, n], y_peer[d]).start()

    @lambda f: stepper(f, Y_STEPS)
    def forward_y(g, part):
        y_got(g, part, 0)
        for d in both:
            remote(y_piece(slot_of[d], g, part, d), y_piece(2, g, part, d), SMALL, y_fwd.at[g, part], y_peer[d]).start()

    @lambda f: stepper(f, range(GROUPS))
    def send_pair(g):
        loaded()
        if g < 3:
            remote(a_buf.at[0, (g + 2) % 4, :, own_rows], a_buf.at[0, g, :, pair_rows], SMALL, pair_recv.at[g], to_pair).start()
        else:
            remote(a_buf.at[0, 1, 1, first_own], a_buf.at[0, 3, 1, first_rows], SMALL, pair_recv.at[3], to_pair).start()

    @lambda f: stepper(f, (0, 1, 3, 2))
    def send_full(i):
        if i == 0:
            loaded()
        elif i == 2:
            far_y_got(1, 0)
        else:
            y_got(1, 0, 0)
            y_got(1, 0, 1)
        remote(a_buf.at[i, 1, 0, own_rows], a_buf.at[i, 3, 0, pair_rows], BIG, pair_full.at[0], to_pair).start()
        remote(a_buf.at[i, 1, 1, second_own], a_buf.at[i, 3, 1, second_rows], SMALL, pair_full.at[1], to_pair).start()

    def full_got():
        arrived(a_buf.at[:, 3, 0, pair_rows], pair_full.at[0], "full", 0)
        arrived(a_buf.at[:, 3, 1, second_rows], pair_full.at[1], "full", 1)

    def ready(g, part, first, count, slots):
        if part == 0:
            loaded()
        else:
            pair_got(g)
        if (g, part) == (3, 1):
            full_got()
        if slots != FAR:
            y_got(g, part, 0)
            y_got(g, part, 1)
        if slots != NEAR:
            far_y_got(g, part)
        z_got(g)
        for s in STEPS:
            step_group, _, step_first, step_count = X_STEPS[s]
            if step_group == g and step_first < first + count and first < step_first + step_count:
                x_got(s, 0)
                x_got(s, 1)
                far_x_got(s)
                sibling_got(s)
        if g == 1:
            for j in slots:
                late_got(j, first * 2 // UNITS)
            late_sibling_got(slots, first * 2 // UNITS)

    @lambda f: stepper(f, PRODUCTS)
    def compute(g, part, first, count, slots):
        ready(g, part, first, count, slots)
        by_a = slots in (NEAR, FAR)
        last = g == 3 and slots != NEAR
        add = g > 0
        size = min(count, 2) * unit

        def body(n, carry=0):
            at = first * unit + n * size
            cols = pl.ds(at if isinstance(n, int) else pl.multiple_of(at, size), size)
            total = None
            for slot in slots:
                i, j = (slot, (y + slot - x + 4) % 4) if by_a else ((x + slot - y + 4) % 4, slot)
                for cc in both:
                    term = jnp.dot(a_buf[i, g, cc, part_rows[part], :], b_buf[j, g, cc, :, cols], preferred_element_type=jnp.float32)
                    total = term if total is None else total + term
            if add:
                total = total + acc[part_rows[part], cols]
            if not last:
                acc[part_rows[part], cols] = total
            elif part == 1:
                stage[:, cols] = total.astype(stage.dtype)
            else:
                out_ref[:, pl.ds(pl.multiple_of(side * half + at, size), size)] = total.astype(out_ref.dtype)
            return carry

        if count <= 2 or slots == FAR:
            for n in range((count + 1) // 2):
                body(n)
        else:
            lax.fori_loop(0, count // 2, body, 0)

    @lambda f: stepper(f, LAST_STEPS)
    def send_c(s):
        _, _, first, count = X_STEPS[s]
        at = pl.ds(pl.multiple_of(side * half + first * unit, unit), count * unit)
        remote(stage.at[:, pl.ds(first * unit, count * unit)], out_ref.at[:, at], BIG, c_recv, to_pair).start()

    b_load.wait()
    send_pair()
    send_x()
    send_y()
    send_y()
    send_z_pair()
    send_x()
    send_z_early()
    send_y()
    send_late()
    send_late()
    send_x()
    send_pair()
    send_y()
    send_x()
    send_y()
    forward_x()
    send_pair()
    send_late()
    sib_own()
    send_full()
    send_y()
    send_late()
    forward_y()
    late_sibling()
    send_x()
    forward_y()
    sib_near()
    forward_y()
    send_z_mirror()
    send_x()
    sib_far()
    send_pair()
    forward_x()
    send_y()
    send_late()
    send_late()
    sib_own()
    send_full()
    compute()
    send_y()
    sib_near()
    late_sibling()
    forward_y()
    sib_own()
    forward_x()
    compute()
    compute()
    send_late()
    send_y()
    send_y()
    compute()
    send_x()
    send_full()
    sib_far()
    sib_own()
    send_late()
    send_y()
    late_sibling()
    send_x()
    sib_far()
    forward_y()
    sib_near()
    send_x()
    send_y()
    late_sibling()
    forward_x()
    send_x()
    send_x()
    late_sibling()
    send_y()
    send_full()
    compute()
    sib_near()
    forward_y()
    compute()
    forward_x()
    send_y()
    sib_far()
    late_sibling()
    send_x()
    compute()
    compute()
    send_x()
    send_y()
    compute()
    forward_x()
    sib_near()
    send_x()
    send_x()
    sib_own()
    compute()
    send_c()
    compute()
    sib_far()
    forward_y()
    compute()
    sib_near()
    forward_x()
    sib_own()
    compute()
    late_sibling()
    sib_own()
    send_c()
    send_y()
    send_x()
    late_sibling()
    compute()
    sib_far()
    sib_own()
    forward_x()
    compute()
    compute()
    send_c()
    sib_near()
    sib_far()
    sib_near()
    compute()
    forward_y()
    compute()
    send_c()
    sib_far()
    compute()
    compute()
    send_c()
    compute()
    compute()
    compute()

    sent(b_buf, BIG)
    sent(a_buf.at[:, :, :, pl.ds(0, rows + rows * 3 // 4)], SMALL)
    arrived(out_ref.at[:, other_cols], c_recv, "c")


def solution(mesh):
    def product(a_blk, b_blk):
        rows, width = a_blk.shape
        half = width // 2
        dma = pltpu.SemaphoreType.DMA
        return pl.pallas_call(
            kernel,
            out_shape=pltpu.VMEM((rows, width), jnp.bfloat16),
            in_specs=[pl.BlockSpec(memory_space=pltpu.HBM)] * 2,
            out_specs=pl.BlockSpec(memory_space=pltpu.VMEM),
            scratch_shapes=[
                pltpu.VMEM((4, GROUPS, 2, 2 * rows, rows), jnp.bfloat16),
                pltpu.VMEM((4, GROUPS, 2, rows, half), jnp.bfloat16),
                pltpu.VMEM((2 * rows, half), jnp.float32),
                pltpu.VMEM((rows, half), jnp.bfloat16),
                dma((2,)),
                dma((GROUPS, 2, 2)),
                dma((GROUPS, 2)),
                dma((GROUPS,)),
                dma((2,)),
                dma((len(X_STEPS), 2)),
                dma((len(X_STEPS),)),
                dma((3,)),
                dma((4, 2)),
                dma((len(X_STEPS),)),
                dma((2, 2)),
                dma(()),
                dma((2,)),
            ],
            compiler_params=pltpu.CompilerParams(collective_id=0, has_side_effects=True, vmem_limit_bytes=56 * 1024 * 1024),
        )(a_blk, b_blk)

    block_spec = P(("row", "depth"), "col")
    return jax.shard_map(product, mesh=mesh, in_specs=(block_spec, block_spec), out_specs=block_spec, check_vma=False)
```

```python
import jax
import jax.numpy as jnp
from jax import lax
from jax.experimental import pallas as pl
from jax.experimental.pallas import tpu as pltpu
from jax.sharding import PartitionSpec as P

MESH = pl.DeviceIdType.MESH
GROUPS = 4
UNITS = 8
ALL, OUTER, INNER, NEAR, FAR = (0, 1, 2, 3), (0, 3), (1, 2), (0, 1, 3), (2,)
X_STEPS = ((0, False, 0, 8), (1, True, 0, 8), (2, False, 0, 8), (3, False, 0, 2), (3, False, 2, 2), (3, False, 4, 2), (3, False, 6, 1), (3, False, 7, 1))
STEPS = range(len(X_STEPS))
LAST_STEPS = [s for s in STEPS if X_STEPS[s][0] == 3]
Y_STEPS = ((0, 0), (1, 0), (0, 1), (1, 1), (2, 1), (3, 1), (2, 0), (3, 0))
LATE = ((0, 0), (0, 1), (3, 0), (3, 1), (1, 0), (2, 0), (1, 1), (2, 1))
PRODUCTS = (
    (0, 1, 0, 4, ALL),
    (0, 0, 4, 4, ALL),
    (0, 1, 4, 4, ALL),
    (1, 1, 0, 4, OUTER),
    (1, 1, 4, 4, OUTER),
    (0, 0, 0, 4, ALL),
    (1, 0, 4, 4, OUTER),
    (2, 1, 4, 4, ALL),
    (2, 1, 0, 4, ALL),
    (1, 1, 0, 4, INNER),
    (3, 1, 0, 2, ALL),
    (1, 0, 0, 4, INNER),
    (1, 0, 0, 4, OUTER),
    (3, 1, 2, 2, ALL),
    (1, 1, 4, 4, INNER),
    (3, 1, 4, 2, ALL),
    (1, 0, 4, 4, INNER),
    (3, 1, 6, 1, ALL),
    (2, 0, 4, 4, ALL),
    (3, 1, 7, 1, ALL),
    (2, 0, 0, 4, ALL),
    (3, 0, 0, 8, NEAR),
    (3, 0, 0, 8, FAR),
)
BIG, SMALL = range(2)


def stepper(function, order):
    entries = iter(order)

    def step():
        entry = next(entries)
        function(*(entry if isinstance(entry, tuple) else (entry,)))

    return step


def kernel(a_ref, b_ref, out_ref, a_buf, b_buf, acc, stage, load_sem, y_recv, y_fwd, pair_recv, pair_full, x_recv, x_fwd, z_recv, z_late, sib_recv, sib_late, c_recv, send_sem):
    z, y, r = lax.axis_index("depth"), lax.axis_index("col"), lax.axis_index("row")
    x, c = r // 2, r % 2
    rows, width = a_ref.shape
    half = width // 2
    unit = half // UNITS
    early = rows // 4
    over_y = rows * 3 // 8

    pair = z + 1 - 2 * (z % 2)
    mirror = 3 - z
    side = ((z + 1) // 2) % 2
    z_of = (z, mirror, pair, 3 - pair)

    y_peer = ({"col": (y + 1) % 4}, {"col": (y + 3) % 4})
    x_peer = ({"row": ((x + 1) % 4) * 2 + c}, {"row": ((x + 3) % 4) * 2 + c})
    to_pair, to_mirror, to_sibling = {"depth": pair}, {"depth": mirror}, {"row": x * 2 + 1 - c}
    peers = y_peer + x_peer + (to_pair, to_mirror, to_sibling)
    both = range(2)

    def remote(src, dst, kind, recv, where):
        return pltpu.make_async_remote_copy(src_ref=src, dst_ref=dst, send_sem=send_sem.at[kind], recv_sem=recv, device_id=where, device_id_type=MESH)

    waited = set()

    def arrived(ref, recv, *key):
        if key not in waited:
            waited.add(key)
            remote(ref, ref, BIG, recv, to_sibling).wait_recv()

    def sent(ref, kind):
        remote(ref, ref, kind, c_recv, to_sibling).wait_send()

    own_rows, pair_rows = part_rows = (pl.ds(0, rows), pl.ds(rows, rows))
    early_rows, late_rows = pl.ds(0, early), pl.ds(early, rows - early)
    col_half = (pl.ds(0, half // 2), pl.ds(half // 2, half // 2))
    my_cols = pl.ds(pl.multiple_of(side * half, half), half)
    other_cols = pl.ds(pl.multiple_of((1 - side) * half, half), half)
    slot_of = (3, 1)

    b_load = pltpu.make_async_copy(b_ref.at[:, my_cols], b_buf.at[0, 0, 0], load_sem.at[1])
    b_load.start()
    for g in range(GROUPS):
        for cc in both:
            start = pl.multiple_of((c + cc - 2 * c * cc) * half + z_of[g] * rows, rows)
            pltpu.make_async_copy(a_ref.at[:, pl.ds(start, rows)], a_buf.at[0, g, cc, own_rows], load_sem.at[0]).start()

    barrier = pltpu.get_barrier_semaphore()
    for where in peers:
        pl.semaphore_signal(barrier, inc=1, device_id=where, device_id_type=MESH)
    pl.semaphore_wait(barrier, len(peers))

    def loaded():
        arrived(a_buf.at[0, :, :, own_rows], load_sem.at[0], "load")

    def x_ref(s, slot, piece=None, core=0):
        g, early_only, first, count = X_STEPS[s]
        size = early if early_only else rows
        at = pl.ds(0, size) if piece is None else pl.ds(piece * (size // 2), size // 2)
        return b_buf.at[slot, g, core, at, pl.ds(first * unit, count * unit)]

    def x_kind(s):
        return SMALL if X_STEPS[s][1] else BIG

    def x_got(s, n):
        arrived(x_ref(s, 1), x_recv.at[s, n], "x", s, n)

    def far_x_got(s):
        arrived(x_ref(s, 2), x_fwd.at[s], "fx", s)

    def z_got(g):
        if g > 0:
            arrived(b_buf.at[0, g, 0, early_rows] if g == 1 else b_buf.at[0, g, 0], z_recv.at[g - 1], "z", g)

    @lambda f: stepper(f, [(s, n) for s in STEPS for n in both])
    def send_x(s, n):
        z_got(X_STEPS[s][0])
        for d in both:
            h = (d + n) % 2
            remote(x_ref(s, 0, h), x_ref(s, slot_of[d], h), x_kind(s), x_recv.at[s, n], x_peer[d]).start()

    @lambda f: stepper(f, STEPS)
    def forward_x(s):
        x_got(s, 0)
        for d in both:
            remote(x_ref(s, slot_of[d], d), x_ref(s, 2, d), x_kind(s), x_fwd.at[s], x_peer[d]).start()

    def send_sibling(s, j):
        remote(x_ref(s, j), x_ref(s, j, core=1), BIG, sib_recv.at[s], to_sibling).start()

    @lambda f: stepper(f, STEPS)
    def sib_own(s):
        z_got(X_STEPS[s][0])
        send_sibling(s, 0)

    @lambda f: stepper(f, STEPS)
    def sib_near(s):
        x_got(s, 0)
        x_got(s, 1)
        for slot in slot_of:
            send_sibling(s, slot)

    @lambda f: stepper(f, STEPS)
    def sib_far(s):
        far_x_got(s)
        send_sibling(s, 2)

    def sibling_got(s):
        arrived(x_ref(s, slice(None), core=1), sib_recv.at[s], "sib", s)

    def send_z_early():
        remote(b_buf.at[0, 0, 0, early_rows], b_buf.at[0, 1, 0, early_rows], SMALL, z_recv.at[0], to_mirror).start()

    def send_z_pair():
        remote(b_ref.at[:, other_cols], b_buf.at[0, 2, 0], BIG, z_recv.at[1], to_pair).start()

    def send_z_mirror():
        z_got(2)
        remote(b_buf.at[0, 2, 0], b_buf.at[0, 3, 0], BIG, z_recv.at[2], to_mirror).start()

    def late_ref(j, k, g=1, core=0):
        return b_buf.at[j, g, core, late_rows, col_half[k]]

    def late_got(j, k):
        arrived(late_ref(j, k), z_late.at[j, k], "late", j, k)

    @lambda f: stepper(f, LATE)
    def send_late(j, k):
        if j == 2:
            far_x_got(0)
        elif j > 0:
            x_got(0, 0)
            x_got(0, 1)
        remote(late_ref(j, k, 0), late_ref(j, k), BIG, z_late.at[j, k], to_mirror).start()

    @lambda f: stepper(f, LATE)
    def late_sibling(j, k):
        late_got(j, k)
        remote(late_ref(j, k), late_ref(j, k, core=1), BIG, sib_late.at[int(j in INNER), k], to_sibling).start()

    def late_sibling_got(slots, k):
        arrived(late_ref(pl.ds(0, 2), k, core=1), sib_late.at[int(slots == INNER), k], "sl", slots, k)

    first_rows, second_rows = pl.ds(rows, over_y), pl.ds(rows + over_y, rows - over_y)
    first_own, second_own = pl.ds(0, over_y), pl.ds(over_y, rows - over_y)

    def y_piece(slot, g, part, h):
        if (g, part) == (3, 1):
            return a_buf.at[slot, g, 1, pl.ds(rows + h * (over_y // 2), over_y // 2)]
        return a_buf.at[slot, g, h, part_rows[part]]

    def y_whole(g, part):
        return a_buf.at[1, g, 1, first_rows] if (g, part) == (3, 1) else a_buf.at[1, g, :, part_rows[part]]

    def y_got(g, part, n):
        arrived(y_whole(g, part), y_recv.at[g, part, n], "y", g, part, n)

    def far_y_got(g, part):
        arrived(y_whole(g, part), y_fwd.at[g, part], "fy", g, part)

    def pair_got(g):
        arrived(a_buf.at[0, g, :, pair_rows] if g < 3 else a_buf.at[0, 3, 1, first_rows], pair_recv.at[g], "pair", g)

    @lambda f: stepper(f, [(g, part, n) for g, part in Y_STEPS for n in both])
    def send_y(g, part, n):
        if part == 1:
            pair_got(g)
        else:
            loaded()
        for d in both:
            h = (d + n) % 2
            remote(y_piece(0, g, part, h), y_piece(slot_of[d], g, part, h), SMALL, y_recv.at[g, part, n], y_peer[d]).start()

    @lambda f: stepper(f, Y_STEPS)
    def forward_y(g, part):
        y_got(g, part, 0)
        for d in both:
            remote(y_piece(slot_of[d], g, part, d), y_piece(2, g, part, d), SMALL, y_fwd.at[g, part], y_peer[d]).start()

    @lambda f: stepper(f, range(GROUPS))
    def send_pair(g):
        loaded()
        if g < 3:
            remote(a_buf.at[0, (g + 2) % 4, :, own_rows], a_buf.at[0, g, :, pair_rows], SMALL, pair_recv.at[g], to_pair).start()
        else:
            remote(a_buf.at[0, 1, 1, first_own], a_buf.at[0, 3, 1, first_rows], SMALL, pair_recv.at[3], to_pair).start()

    @lambda f: stepper(f, (0, 1, 3, 2))
    def send_full(i):
        if i == 0:
            loaded()
        elif i == 2:
            far_y_got(1, 0)
        else:
            y_got(1, 0, 0)
            y_got(1, 0, 1)
        remote(a_buf.at[i, 1, 0, own_rows], a_buf.at[i, 3, 0, pair_rows], BIG, pair_full.at[0], to_pair).start()
        remote(a_buf.at[i, 1, 1, second_own], a_buf.at[i, 3, 1, second_rows], SMALL, pair_full.at[1], to_pair).start()

    def full_got():
        arrived(a_buf.at[:, 3, 0, pair_rows], pair_full.at[0], "full", 0)
        arrived(a_buf.at[:, 3, 1, second_rows], pair_full.at[1], "full", 1)

    def ready(g, part, first, count, slots):
        if part == 0:
            loaded()
        else:
            pair_got(g)
        if (g, part) == (3, 1):
            full_got()
        if slots != FAR:
            y_got(g, part, 0)
            y_got(g, part, 1)
        if slots != NEAR:
            far_y_got(g, part)
        z_got(g)
        for s in STEPS:
            step_group, _, step_first, step_count = X_STEPS[s]
            if step_group == g and step_first < first + count and first < step_first + step_count:
                x_got(s, 0)
                x_got(s, 1)
                far_x_got(s)
                sibling_got(s)
        if g == 1:
            for j in slots:
                late_got(j, first * 2 // UNITS)
            late_sibling_got(slots, first * 2 // UNITS)

    @lambda f: stepper(f, PRODUCTS)
    def compute(g, part, first, count, slots):
        ready(g, part, first, count, slots)
        by_a = slots in (NEAR, FAR)
        last = g == 3 and slots != NEAR
        add = g > 0
        size = min(count, 2) * unit

        def body(n, carry=0):
            at = first * unit + n * size
            cols = pl.ds(at if isinstance(n, int) else pl.multiple_of(at, size), size)
            total = None
            for slot in slots:
                i, j = (slot, (y + slot - x + 4) % 4) if by_a else ((x + slot - y + 4) % 4, slot)
                for cc in both:
                    term = jnp.dot(a_buf[i, g, cc, part_rows[part], :], b_buf[j, g, cc, :, cols], preferred_element_type=jnp.float32)
                    total = term if total is None else total + term
            if add:
                total = total + acc[part_rows[part], cols]
            if not last:
                acc[part_rows[part], cols] = total
            elif part == 1:
                stage[:, cols] = total.astype(stage.dtype)
            else:
                out_ref[:, pl.ds(pl.multiple_of(side * half + at, size), size)] = total.astype(out_ref.dtype)
            return carry

        if count <= 2 or slots == FAR:
            for n in range((count + 1) // 2):
                body(n)
        else:
            lax.fori_loop(0, count // 2, body, 0)

    @lambda f: stepper(f, LAST_STEPS)
    def send_c(s):
        _, _, first, count = X_STEPS[s]
        at = pl.ds(pl.multiple_of(side * half + first * unit, unit), count * unit)
        remote(stage.at[:, pl.ds(first * unit, count * unit)], out_ref.at[:, at], BIG, c_recv, to_pair).start()

    b_load.wait()
    send_y()
    send_y()
    send_pair()
    send_x()
    send_z_early()
    sib_own()
    send_x()
    send_y()
    send_z_pair()
    send_y()
    send_x()
    sib_own()
    send_pair()
    send_late()
    send_y()
    send_late()
    forward_x()
    send_pair()
    send_y()
    late_sibling()
    forward_y()
    send_pair()
    send_late()
    forward_y()
    sib_near()
    late_sibling()
    forward_x()
    send_full()
    send_late()
    send_x()
    send_z_mirror()
    forward_y()
    send_x()
    sib_near()
    send_late()
    send_y()
    send_full()
    send_x()
    send_late()
    late_sibling()
    send_y()
    send_y()
    sib_far()
    sib_own()
    forward_y()
    send_y()
    sib_far()
    send_y()
    send_y()
    forward_x()
    compute()
    compute()
    send_late()
    sib_near()
    send_full()
    send_x()
    send_x()
    compute()
    late_sibling()
    send_x()
    forward_y()
    compute()
    send_x()
    send_full()
    sib_own()
    compute()
    compute()
    forward_x()
    send_y()
    send_x()
    compute()
    forward_y()
    late_sibling()
    sib_far()
    forward_x()
    send_y()
    send_x()
    send_y()
    sib_near()
    send_late()
    compute()
    sib_own()
    send_x()
    late_sibling()
    sib_far()
    sib_own()
    compute()
    sib_own()
    compute()
    forward_x()
    compute()
    send_c()
    sib_far()
    send_x()
    send_x()
    sib_near()
    compute()
    forward_y()
    compute()
    late_sibling()
    sib_near()
    forward_x()
    compute()
    send_c()
    late_sibling()
    send_x()
    send_y()
    sib_far()
    sib_near()
    compute()
    forward_x()
    compute()
    send_c()
    sib_far()
    forward_y()
    sib_own()
    compute()
    sib_near()
    compute()
    send_c()
    sib_far()
    compute()
    compute()
    send_c()
    compute()
    compute()
    compute()

    sent(b_buf, BIG)
    sent(a_buf.at[:, :, :, pl.ds(0, rows + rows * 3 // 4)], SMALL)
    arrived(out_ref.at[:, other_cols], c_recv, "c")


def solution(mesh):
    def product(a_blk, b_blk):
        rows, width = a_blk.shape
        half = width // 2
        dma = pltpu.SemaphoreType.DMA
        return pl.pallas_call(
            kernel,
            out_shape=pltpu.VMEM((rows, width), jnp.bfloat16),
            in_specs=[pl.BlockSpec(memory_space=pltpu.HBM)] * 2,
            out_specs=pl.BlockSpec(memory_space=pltpu.VMEM),
            scratch_shapes=[
                pltpu.VMEM((4, GROUPS, 2, 2 * rows, rows), jnp.bfloat16),
                pltpu.VMEM((4, GROUPS, 2, rows, half), jnp.bfloat16),
                pltpu.VMEM((2 * rows, half), jnp.float32),
                pltpu.VMEM((rows, half), jnp.bfloat16),
                dma((2,)),
                dma((GROUPS, 2, 2)),
                dma((GROUPS, 2)),
                dma((GROUPS,)),
                dma((2,)),
                dma((len(X_STEPS), 2)),
                dma((len(X_STEPS),)),
                dma((3,)),
                dma((4, 2)),
                dma((len(X_STEPS),)),
                dma((2, 2)),
                dma(()),
                dma((2,)),
            ],
            compiler_params=pltpu.CompilerParams(collective_id=0, has_side_effects=True, vmem_limit_bytes=56 * 1024 * 1024),
        )(a_blk, b_blk)

    block_spec = P(("row", "depth"), "col")
    return jax.shard_map(product, mesh=mesh, in_specs=(block_spec, block_spec), out_specs=block_spec, check_vma=False)
```

```python
import jax
import jax.numpy as jnp
from jax import lax
from jax.experimental import pallas as pl
from jax.experimental.pallas import tpu as pltpu
from jax.sharding import PartitionSpec as P

MESH = pl.DeviceIdType.MESH
GROUPS = 4
UNITS = 8
ALL, OUTER, INNER, NEAR, FAR = (0, 1, 2, 3), (0, 3), (1, 2), (0, 1, 3), (2,)
X_STEPS = ((0, False, 0, 8), (1, True, 0, 8), (2, False, 0, 8), (3, False, 0, 2), (3, False, 2, 2), (3, False, 4, 2), (3, False, 6, 1), (3, False, 7, 1))
STEPS = range(len(X_STEPS))
LAST_STEPS = [s for s in STEPS if X_STEPS[s][0] == 3]
Y_STEPS = ((0, 0), (1, 0), (0, 1), (1, 1), (2, 1), (3, 1), (2, 0), (3, 0))
LATE = ((0, 0), (0, 1), (3, 0), (3, 1), (1, 0), (2, 0), (1, 1), (2, 1))
PRODUCTS = (
    (0, 0, 4, 4, ALL),
    (0, 1, 4, 4, ALL),
    (0, 0, 0, 4, ALL),
    (1, 1, 4, 4, OUTER),
    (1, 0, 0, 4, OUTER),
    (1, 0, 4, 4, OUTER),
    (0, 1, 0, 4, ALL),
    (1, 1, 0, 4, OUTER),
    (2, 1, 0, 4, ALL),
    (1, 1, 0, 4, INNER),
    (3, 1, 0, 2, ALL),
    (2, 1, 4, 4, ALL),
    (3, 1, 2, 2, ALL),
    (1, 0, 0, 4, INNER),
    (1, 1, 4, 4, INNER),
    (3, 1, 4, 2, ALL),
    (1, 0, 4, 4, INNER),
    (3, 1, 6, 1, ALL),
    (2, 0, 0, 4, ALL),
    (3, 1, 7, 1, ALL),
    (2, 0, 4, 4, ALL),
    (3, 0, 0, 8, NEAR),
    (3, 0, 0, 8, FAR),
)
BIG, SMALL = range(2)


def stepper(function, order):
    entries = iter(order)

    def step():
        entry = next(entries)
        function(*(entry if isinstance(entry, tuple) else (entry,)))

    return step


def kernel(a_ref, b_ref, out_ref, a_buf, b_buf, acc, stage, load_sem, y_recv, y_fwd, pair_recv, pair_full, x_recv, x_fwd, z_recv, z_late, sib_recv, sib_late, c_recv, send_sem):
    z, y, r = lax.axis_index("depth"), lax.axis_index("col"), lax.axis_index("row")
    x, c = r // 2, r % 2
    rows, width = a_ref.shape
    half = width // 2
    unit = half // UNITS
    early = rows // 4
    over_y = rows * 3 // 8

    pair = z + 1 - 2 * (z % 2)
    mirror = 3 - z
    side = ((z + 1) // 2) % 2
    z_of = (z, mirror, pair, 3 - pair)

    y_peer = ({"col": (y + 1) % 4}, {"col": (y + 3) % 4})
    x_peer = ({"row": ((x + 1) % 4) * 2 + c}, {"row": ((x + 3) % 4) * 2 + c})
    to_pair, to_mirror, to_sibling = {"depth": pair}, {"depth": mirror}, {"row": x * 2 + 1 - c}
    peers = y_peer + x_peer + (to_pair, to_mirror, to_sibling)
    both = range(2)

    def remote(src, dst, kind, recv, where):
        return pltpu.make_async_remote_copy(src_ref=src, dst_ref=dst, send_sem=send_sem.at[kind], recv_sem=recv, device_id=where, device_id_type=MESH)

    waited = set()

    def arrived(ref, recv, *key):
        if key not in waited:
            waited.add(key)
            remote(ref, ref, BIG, recv, to_sibling).wait_recv()

    def sent(ref, kind):
        remote(ref, ref, kind, c_recv, to_sibling).wait_send()

    own_rows, pair_rows = part_rows = (pl.ds(0, rows), pl.ds(rows, rows))
    early_rows, late_rows = pl.ds(0, early), pl.ds(early, rows - early)
    col_half = (pl.ds(0, half // 2), pl.ds(half // 2, half // 2))
    my_cols = pl.ds(pl.multiple_of(side * half, half), half)
    other_cols = pl.ds(pl.multiple_of((1 - side) * half, half), half)
    slot_of = (3, 1)

    b_load = pltpu.make_async_copy(b_ref.at[:, my_cols], b_buf.at[0, 0, 0], load_sem.at[1])
    b_load.start()
    for g in range(GROUPS):
        for cc in both:
            start = pl.multiple_of((c + cc - 2 * c * cc) * half + z_of[g] * rows, rows)
            pltpu.make_async_copy(a_ref.at[:, pl.ds(start, rows)], a_buf.at[0, g, cc, own_rows], load_sem.at[0]).start()

    barrier = pltpu.get_barrier_semaphore()
    for where in peers:
        pl.semaphore_signal(barrier, inc=1, device_id=where, device_id_type=MESH)
    pl.semaphore_wait(barrier, len(peers))

    def loaded():
        arrived(a_buf.at[0, :, :, own_rows], load_sem.at[0], "load")

    def x_ref(s, slot, piece=None, core=0):
        g, early_only, first, count = X_STEPS[s]
        size = early if early_only else rows
        at = pl.ds(0, size) if piece is None else pl.ds(piece * (size // 2), size // 2)
        return b_buf.at[slot, g, core, at, pl.ds(first * unit, count * unit)]

    def x_kind(s):
        return SMALL if X_STEPS[s][1] else BIG

    def x_got(s, n):
        arrived(x_ref(s, 1), x_recv.at[s, n], "x", s, n)

    def far_x_got(s):
        arrived(x_ref(s, 2), x_fwd.at[s], "fx", s)

    def z_got(g):
        if g > 0:
            arrived(b_buf.at[0, g, 0, early_rows] if g == 1 else b_buf.at[0, g, 0], z_recv.at[g - 1], "z", g)

    @lambda f: stepper(f, [(s, n) for s in STEPS for n in both])
    def send_x(s, n):
        z_got(X_STEPS[s][0])
        for d in both:
            h = (d + n) % 2
            remote(x_ref(s, 0, h), x_ref(s, slot_of[d], h), x_kind(s), x_recv.at[s, n], x_peer[d]).start()

    @lambda f: stepper(f, STEPS)
    def forward_x(s):
        x_got(s, 0)
        for d in both:
            remote(x_ref(s, slot_of[d], d), x_ref(s, 2, d), x_kind(s), x_fwd.at[s], x_peer[d]).start()

    def send_sibling(s, j):
        remote(x_ref(s, j), x_ref(s, j, core=1), BIG, sib_recv.at[s], to_sibling).start()

    @lambda f: stepper(f, STEPS)
    def sib_own(s):
        z_got(X_STEPS[s][0])
        send_sibling(s, 0)

    @lambda f: stepper(f, STEPS)
    def sib_near(s):
        x_got(s, 0)
        x_got(s, 1)
        for slot in slot_of:
            send_sibling(s, slot)

    @lambda f: stepper(f, STEPS)
    def sib_far(s):
        far_x_got(s)
        send_sibling(s, 2)

    def sibling_got(s):
        arrived(x_ref(s, slice(None), core=1), sib_recv.at[s], "sib", s)

    def send_z_early():
        remote(b_buf.at[0, 0, 0, early_rows], b_buf.at[0, 1, 0, early_rows], SMALL, z_recv.at[0], to_mirror).start()

    def send_z_pair():
        remote(b_ref.at[:, other_cols], b_buf.at[0, 2, 0], BIG, z_recv.at[1], to_pair).start()

    def send_z_mirror():
        z_got(2)
        remote(b_buf.at[0, 2, 0], b_buf.at[0, 3, 0], BIG, z_recv.at[2], to_mirror).start()

    def late_ref(j, k, g=1, core=0):
        return b_buf.at[j, g, core, late_rows, col_half[k]]

    def late_got(j, k):
        arrived(late_ref(j, k), z_late.at[j, k], "late", j, k)

    @lambda f: stepper(f, LATE)
    def send_late(j, k):
        if j == 2:
            far_x_got(0)
        elif j > 0:
            x_got(0, 0)
            x_got(0, 1)
        remote(late_ref(j, k, 0), late_ref(j, k), BIG, z_late.at[j, k], to_mirror).start()

    @lambda f: stepper(f, LATE)
    def late_sibling(j, k):
        late_got(j, k)
        remote(late_ref(j, k), late_ref(j, k, core=1), BIG, sib_late.at[int(j in INNER), k], to_sibling).start()

    def late_sibling_got(slots, k):
        arrived(late_ref(pl.ds(0, 2), k, core=1), sib_late.at[int(slots == INNER), k], "sl", slots, k)

    first_rows, second_rows = pl.ds(rows, over_y), pl.ds(rows + over_y, rows - over_y)
    first_own, second_own = pl.ds(0, over_y), pl.ds(over_y, rows - over_y)

    def y_piece(slot, g, part, h):
        if (g, part) == (3, 1):
            return a_buf.at[slot, g, 1, pl.ds(rows + h * (over_y // 2), over_y // 2)]
        return a_buf.at[slot, g, h, part_rows[part]]

    def y_whole(g, part):
        return a_buf.at[1, g, 1, first_rows] if (g, part) == (3, 1) else a_buf.at[1, g, :, part_rows[part]]

    def y_got(g, part, n):
        arrived(y_whole(g, part), y_recv.at[g, part, n], "y", g, part, n)

    def far_y_got(g, part):
        arrived(y_whole(g, part), y_fwd.at[g, part], "fy", g, part)

    def pair_got(g):
        arrived(a_buf.at[0, g, :, pair_rows] if g < 3 else a_buf.at[0, 3, 1, first_rows], pair_recv.at[g], "pair", g)

    @lambda f: stepper(f, [(g, part, n) for g, part in Y_STEPS for n in both])
    def send_y(g, part, n):
        if part == 1:
            pair_got(g)
        else:
            loaded()
        for d in both:
            h = (d + n) % 2
            remote(y_piece(0, g, part, h), y_piece(slot_of[d], g, part, h), SMALL, y_recv.at[g, part, n], y_peer[d]).start()

    @lambda f: stepper(f, Y_STEPS)
    def forward_y(g, part):
        y_got(g, part, 0)
        for d in both:
            remote(y_piece(slot_of[d], g, part, d), y_piece(2, g, part, d), SMALL, y_fwd.at[g, part], y_peer[d]).start()

    @lambda f: stepper(f, range(GROUPS))
    def send_pair(g):
        loaded()
        if g < 3:
            remote(a_buf.at[0, (g + 2) % 4, :, own_rows], a_buf.at[0, g, :, pair_rows], SMALL, pair_recv.at[g], to_pair).start()
        else:
            remote(a_buf.at[0, 1, 1, first_own], a_buf.at[0, 3, 1, first_rows], SMALL, pair_recv.at[3], to_pair).start()

    @lambda f: stepper(f, (0, 1, 3, 2))
    def send_full(i):
        if i == 0:
            loaded()
        elif i == 2:
            far_y_got(1, 0)
        else:
            y_got(1, 0, 0)
            y_got(1, 0, 1)
        remote(a_buf.at[i, 1, 0, own_rows], a_buf.at[i, 3, 0, pair_rows], BIG, pair_full.at[0], to_pair).start()
        remote(a_buf.at[i, 1, 1, second_own], a_buf.at[i, 3, 1, second_rows], SMALL, pair_full.at[1], to_pair).start()

    def full_got():
        arrived(a_buf.at[:, 3, 0, pair_rows], pair_full.at[0], "full", 0)
        arrived(a_buf.at[:, 3, 1, second_rows], pair_full.at[1], "full", 1)

    def ready(g, part, first, count, slots):
        if part == 0:
            loaded()
        else:
            pair_got(g)
        if (g, part) == (3, 1):
            full_got()
        if slots != FAR:
            y_got(g, part, 0)
            y_got(g, part, 1)
        if slots != NEAR:
            far_y_got(g, part)
        z_got(g)
        for s in STEPS:
            step_group, _, step_first, step_count = X_STEPS[s]
            if step_group == g and step_first < first + count and first < step_first + step_count:
                x_got(s, 0)
                x_got(s, 1)
                far_x_got(s)
                sibling_got(s)
        if g == 1:
            for j in slots:
                late_got(j, first * 2 // UNITS)
            late_sibling_got(slots, first * 2 // UNITS)

    @lambda f: stepper(f, PRODUCTS)
    def compute(g, part, first, count, slots):
        ready(g, part, first, count, slots)
        by_a = slots in (NEAR, FAR)
        last = g == 3 and slots != NEAR
        add = g > 0
        size = min(count, 2) * unit

        def body(n, carry=0):
            at = first * unit + n * size
            cols = pl.ds(at if isinstance(n, int) else pl.multiple_of(at, size), size)
            total = None
            for slot in slots:
                i, j = (slot, (y + slot - x + 4) % 4) if by_a else ((x + slot - y + 4) % 4, slot)
                for cc in both:
                    term = jnp.dot(a_buf[i, g, cc, part_rows[part], :], b_buf[j, g, cc, :, cols], preferred_element_type=jnp.float32)
                    total = term if total is None else total + term
            if add:
                total = total + acc[part_rows[part], cols]
            if not last:
                acc[part_rows[part], cols] = total
            elif part == 1:
                stage[:, cols] = total.astype(stage.dtype)
            else:
                out_ref[:, pl.ds(pl.multiple_of(side * half + at, size), size)] = total.astype(out_ref.dtype)
            return carry

        if count <= 2 or slots == FAR:
            for n in range((count + 1) // 2):
                body(n)
        else:
            lax.fori_loop(0, count // 2, body, 0)

    @lambda f: stepper(f, LAST_STEPS)
    def send_c(s):
        _, _, first, count = X_STEPS[s]
        at = pl.ds(pl.multiple_of(side * half + first * unit, unit), count * unit)
        remote(stage.at[:, pl.ds(first * unit, count * unit)], out_ref.at[:, at], BIG, c_recv, to_pair).start()

    b_load.wait()
    send_y()
    send_x()
    send_x()
    send_y()
    send_y()
    send_z_early()
    send_pair()
    send_z_pair()
    sib_own()
    send_late()
    send_y()
    send_y()
    send_pair()
    send_y()
    send_x()
    send_late()
    send_pair()
    sib_own()
    forward_x()
    forward_y()
    send_late()
    send_late()
    forward_x()
    forward_y()
    forward_y()
    send_pair()
    send_x()
    send_z_mirror()
    send_x()
    late_sibling()
    send_y()
    send_y()
    sib_far()
    sib_near()
    late_sibling()
    send_full()
    send_x()
    send_y()
    forward_x()
    send_full()
    forward_y()
    sib_near()
    send_late()
    compute()
    send_y()
    send_x()
    send_late()
    send_y()
    late_sibling()
    send_x()
    compute()
    sib_near()
    send_full()
    send_full()
    late_sibling()
    send_x()
    compute()
    forward_y()
    sib_own()
    send_x()
    send_late()
    send_y()
    forward_x()
    sib_far()
    sib_own()
    send_y()
    compute()
    sib_own()
    forward_y()
    send_late()
    sib_near()
    send_x()
    sib_own()
    send_y()
    compute()
    sib_far()
    late_sibling()
    compute()
    sib_own()
    compute()
    sib_own()
    forward_x()
    send_x()
    sib_near()
    late_sibling()
    send_y()
    send_x()
    compute()
    compute()
    sib_far()
    compute()
    forward_x()
    compute()
    send_x()
    send_x()
    send_c()
    sib_far()
    late_sibling()
    forward_y()
    compute()
    compute()
    send_c()
    send_y()
    forward_x()
    send_x()
    sib_near()
    late_sibling()
    sib_far()
    compute()
    compute()
    forward_x()
    compute()
    send_c()
    sib_far()
    sib_near()
    forward_y()
    sib_near()
    compute()
    compute()
    sib_far()
    send_c()
    compute()
    compute()
    send_c()
    compute()
    compute()
    compute()

    sent(b_buf, BIG)
    sent(a_buf.at[:, :, :, pl.ds(0, rows + rows * 3 // 4)], SMALL)
    arrived(out_ref.at[:, other_cols], c_recv, "c")


def solution(mesh):
    def product(a_blk, b_blk):
        rows, width = a_blk.shape
        half = width // 2
        dma = pltpu.SemaphoreType.DMA
        return pl.pallas_call(
            kernel,
            out_shape=pltpu.VMEM((rows, width), jnp.bfloat16),
            in_specs=[pl.BlockSpec(memory_space=pltpu.HBM)] * 2,
            out_specs=pl.BlockSpec(memory_space=pltpu.VMEM),
            scratch_shapes=[
                pltpu.VMEM((4, GROUPS, 2, 2 * rows, rows), jnp.bfloat16),
                pltpu.VMEM((4, GROUPS, 2, rows, half), jnp.bfloat16),
                pltpu.VMEM((2 * rows, half), jnp.float32),
                pltpu.VMEM((rows, half), jnp.bfloat16),
                dma((2,)),
                dma((GROUPS, 2, 2)),
                dma((GROUPS, 2)),
                dma((GROUPS,)),
                dma((2,)),
                dma((len(X_STEPS), 2)),
                dma((len(X_STEPS),)),
                dma((3,)),
                dma((4, 2)),
                dma((len(X_STEPS),)),
                dma((2, 2)),
                dma(()),
                dma((2,)),
            ],
            compiler_params=pltpu.CompilerParams(collective_id=0, has_side_effects=True, vmem_limit_bytes=56 * 1024 * 1024),
        )(a_blk, b_blk)

    block_spec = P(("row", "depth"), "col")
    return jax.shard_map(product, mesh=mesh, in_specs=(block_spec, block_spec), out_specs=block_spec, check_vma=False)
```

```python
import jax
import jax.numpy as jnp
from jax import lax
from jax.experimental import pallas as pl
from jax.experimental.pallas import tpu as pltpu
from jax.sharding import PartitionSpec as P

MESH = pl.DeviceIdType.MESH
GROUPS = 4
UNITS = 8
ALL, OUTER, INNER, NEAR, FAR = (0, 1, 2, 3), (0, 3), (1, 2), (0, 1, 3), (2,)
X_STEPS = ((0, False, 0, 8), (1, True, 0, 8), (2, False, 0, 8), (3, False, 0, 2), (3, False, 2, 2), (3, False, 4, 2), (3, False, 6, 1), (3, False, 7, 1))
STEPS = range(len(X_STEPS))
LAST_STEPS = [s for s in STEPS if X_STEPS[s][0] == 3]
Y_STEPS = ((0, 0), (1, 0), (0, 1), (1, 1), (2, 1), (3, 1), (2, 0), (3, 0))
LATE = ((0, 0), (0, 1), (3, 0), (3, 1), (1, 0), (2, 0), (1, 1), (2, 1))
PRODUCTS = (
    (0, 1, 4, 4, ALL),
    (0, 0, 0, 4, ALL),
    (0, 1, 0, 4, ALL),
    (1, 1, 4, 4, OUTER),
    (0, 0, 4, 4, ALL),
    (1, 1, 0, 4, OUTER),
    (2, 1, 0, 4, ALL),
    (1, 0, 4, 4, OUTER),
    (1, 0, 0, 4, OUTER),
    (1, 1, 0, 4, INNER),
    (3, 1, 0, 2, ALL),
    (1, 0, 0, 4, INNER),
    (2, 1, 4, 4, ALL),
    (3, 1, 2, 2, ALL),
    (1, 1, 4, 4, INNER),
    (3, 1, 4, 2, ALL),
    (1, 0, 4, 4, INNER),
    (3, 1, 6, 1, ALL),
    (2, 0, 4, 4, ALL),
    (3, 1, 7, 1, ALL),
    (3, 0, 0, 8, NEAR),
    (2, 0, 0, 4, ALL),
    (3, 0, 0, 8, FAR),
)
BIG, SMALL = range(2)


def stepper(function, order):
    entries = iter(order)

    def step():
        entry = next(entries)
        function(*(entry if isinstance(entry, tuple) else (entry,)))

    return step


def kernel(a_ref, b_ref, out_ref, a_buf, b_buf, acc, stage, load_sem, y_recv, y_fwd, pair_recv, pair_full, x_recv, x_fwd, z_recv, z_late, sib_recv, sib_late, c_recv, send_sem):
    z, y, r = lax.axis_index("depth"), lax.axis_index("col"), lax.axis_index("row")
    x, c = r // 2, r % 2
    rows, width = a_ref.shape
    half = width // 2
    unit = half // UNITS
    early = rows // 4
    over_y = rows * 3 // 8

    pair = z + 1 - 2 * (z % 2)
    mirror = 3 - z
    side = ((z + 1) // 2) % 2
    z_of = (z, mirror, pair, 3 - pair)

    y_peer = ({"col": (y + 1) % 4}, {"col": (y + 3) % 4})
    x_peer = ({"row": ((x + 1) % 4) * 2 + c}, {"row": ((x + 3) % 4) * 2 + c})
    to_pair, to_mirror, to_sibling = {"depth": pair}, {"depth": mirror}, {"row": x * 2 + 1 - c}
    peers = y_peer + x_peer + (to_pair, to_mirror, to_sibling)
    both = range(2)

    def remote(src, dst, kind, recv, where):
        return pltpu.make_async_remote_copy(src_ref=src, dst_ref=dst, send_sem=send_sem.at[kind], recv_sem=recv, device_id=where, device_id_type=MESH)

    waited = set()

    def arrived(ref, recv, *key):
        if key not in waited:
            waited.add(key)
            remote(ref, ref, BIG, recv, to_sibling).wait_recv()

    def sent(ref, kind):
        remote(ref, ref, kind, c_recv, to_sibling).wait_send()

    own_rows, pair_rows = part_rows = (pl.ds(0, rows), pl.ds(rows, rows))
    early_rows, late_rows = pl.ds(0, early), pl.ds(early, rows - early)
    col_half = (pl.ds(0, half // 2), pl.ds(half // 2, half // 2))
    my_cols = pl.ds(pl.multiple_of(side * half, half), half)
    other_cols = pl.ds(pl.multiple_of((1 - side) * half, half), half)
    slot_of = (3, 1)

    b_load = pltpu.make_async_copy(b_ref.at[:, my_cols], b_buf.at[0, 0, 0], load_sem.at[1])
    b_load.start()
    for g in range(GROUPS):
        for cc in both:
            start = pl.multiple_of((c + cc - 2 * c * cc) * half + z_of[g] * rows, rows)
            pltpu.make_async_copy(a_ref.at[:, pl.ds(start, rows)], a_buf.at[0, g, cc, own_rows], load_sem.at[0]).start()

    barrier = pltpu.get_barrier_semaphore()
    for where in peers:
        pl.semaphore_signal(barrier, inc=1, device_id=where, device_id_type=MESH)
    pl.semaphore_wait(barrier, len(peers))

    def loaded():
        arrived(a_buf.at[0, :, :, own_rows], load_sem.at[0], "load")

    def x_ref(s, slot, piece=None, core=0):
        g, early_only, first, count = X_STEPS[s]
        size = early if early_only else rows
        at = pl.ds(0, size) if piece is None else pl.ds(piece * (size // 2), size // 2)
        return b_buf.at[slot, g, core, at, pl.ds(first * unit, count * unit)]

    def x_kind(s):
        return SMALL if X_STEPS[s][1] else BIG

    def x_got(s, n):
        arrived(x_ref(s, 1), x_recv.at[s, n], "x", s, n)

    def far_x_got(s):
        arrived(x_ref(s, 2), x_fwd.at[s], "fx", s)

    def z_got(g):
        if g > 0:
            arrived(b_buf.at[0, g, 0, early_rows] if g == 1 else b_buf.at[0, g, 0], z_recv.at[g - 1], "z", g)

    @lambda f: stepper(f, [(s, n) for s in STEPS for n in both])
    def send_x(s, n):
        z_got(X_STEPS[s][0])
        for d in both:
            h = (d + n) % 2
            remote(x_ref(s, 0, h), x_ref(s, slot_of[d], h), x_kind(s), x_recv.at[s, n], x_peer[d]).start()

    @lambda f: stepper(f, STEPS)
    def forward_x(s):
        x_got(s, 0)
        for d in both:
            remote(x_ref(s, slot_of[d], d), x_ref(s, 2, d), x_kind(s), x_fwd.at[s], x_peer[d]).start()

    def send_sibling(s, j):
        remote(x_ref(s, j), x_ref(s, j, core=1), BIG, sib_recv.at[s], to_sibling).start()

    @lambda f: stepper(f, STEPS)
    def sib_own(s):
        z_got(X_STEPS[s][0])
        send_sibling(s, 0)

    @lambda f: stepper(f, STEPS)
    def sib_near(s):
        x_got(s, 0)
        x_got(s, 1)
        for slot in slot_of:
            send_sibling(s, slot)

    @lambda f: stepper(f, STEPS)
    def sib_far(s):
        far_x_got(s)
        send_sibling(s, 2)

    def sibling_got(s):
        arrived(x_ref(s, slice(None), core=1), sib_recv.at[s], "sib", s)

    def send_z_early():
        remote(b_buf.at[0, 0, 0, early_rows], b_buf.at[0, 1, 0, early_rows], SMALL, z_recv.at[0], to_mirror).start()

    def send_z_pair():
        remote(b_ref.at[:, other_cols], b_buf.at[0, 2, 0], BIG, z_recv.at[1], to_pair).start()

    def send_z_mirror():
        z_got(2)
        remote(b_buf.at[0, 2, 0], b_buf.at[0, 3, 0], BIG, z_recv.at[2], to_mirror).start()

    def late_ref(j, k, g=1, core=0):
        return b_buf.at[j, g, core, late_rows, col_half[k]]

    def late_got(j, k):
        arrived(late_ref(j, k), z_late.at[j, k], "late", j, k)

    @lambda f: stepper(f, LATE)
    def send_late(j, k):
        if j == 2:
            far_x_got(0)
        elif j > 0:
            x_got(0, 0)
            x_got(0, 1)
        remote(late_ref(j, k, 0), late_ref(j, k), BIG, z_late.at[j, k], to_mirror).start()

    @lambda f: stepper(f, LATE)
    def late_sibling(j, k):
        late_got(j, k)
        remote(late_ref(j, k), late_ref(j, k, core=1), BIG, sib_late.at[int(j in INNER), k], to_sibling).start()

    def late_sibling_got(slots, k):
        arrived(late_ref(pl.ds(0, 2), k, core=1), sib_late.at[int(slots == INNER), k], "sl", slots, k)

    first_rows, second_rows = pl.ds(rows, over_y), pl.ds(rows + over_y, rows - over_y)
    first_own, second_own = pl.ds(0, over_y), pl.ds(over_y, rows - over_y)

    def y_piece(slot, g, part, h):
        if (g, part) == (3, 1):
            return a_buf.at[slot, g, 1, pl.ds(rows + h * (over_y // 2), over_y // 2)]
        return a_buf.at[slot, g, h, part_rows[part]]

    def y_whole(g, part):
        return a_buf.at[1, g, 1, first_rows] if (g, part) == (3, 1) else a_buf.at[1, g, :, part_rows[part]]

    def y_got(g, part, n):
        arrived(y_whole(g, part), y_recv.at[g, part, n], "y", g, part, n)

    def far_y_got(g, part):
        arrived(y_whole(g, part), y_fwd.at[g, part], "fy", g, part)

    def pair_got(g):
        arrived(a_buf.at[0, g, :, pair_rows] if g < 3 else a_buf.at[0, 3, 1, first_rows], pair_recv.at[g], "pair", g)

    @lambda f: stepper(f, [(g, part, n) for g, part in Y_STEPS for n in both])
    def send_y(g, part, n):
        if part == 1:
            pair_got(g)
        else:
            loaded()
        for d in both:
            h = (d + n) % 2
            remote(y_piece(0, g, part, h), y_piece(slot_of[d], g, part, h), SMALL, y_recv.at[g, part, n], y_peer[d]).start()

    @lambda f: stepper(f, Y_STEPS)
    def forward_y(g, part):
        y_got(g, part, 0)
        for d in both:
            remote(y_piece(slot_of[d], g, part, d), y_piece(2, g, part, d), SMALL, y_fwd.at[g, part], y_peer[d]).start()

    @lambda f: stepper(f, range(GROUPS))
    def send_pair(g):
        loaded()
        if g < 3:
            remote(a_buf.at[0, (g + 2) % 4, :, own_rows], a_buf.at[0, g, :, pair_rows], SMALL, pair_recv.at[g], to_pair).start()
        else:
            remote(a_buf.at[0, 1, 1, first_own], a_buf.at[0, 3, 1, first_rows], SMALL, pair_recv.at[3], to_pair).start()

    @lambda f: stepper(f, (0, 1, 3, 2))
    def send_full(i):
        if i == 0:
            loaded()
        elif i == 2:
            far_y_got(1, 0)
        else:
            y_got(1, 0, 0)
            y_got(1, 0, 1)
        remote(a_buf.at[i, 1, 0, own_rows], a_buf.at[i, 3, 0, pair_rows], BIG, pair_full.at[0], to_pair).start()
        remote(a_buf.at[i, 1, 1, second_own], a_buf.at[i, 3, 1, second_rows], SMALL, pair_full.at[1], to_pair).start()

    def full_got():
        arrived(a_buf.at[:, 3, 0, pair_rows], pair_full.at[0], "full", 0)
        arrived(a_buf.at[:, 3, 1, second_rows], pair_full.at[1], "full", 1)

    def ready(g, part, first, count, slots):
        if part == 0:
            loaded()
        else:
            pair_got(g)
        if (g, part) == (3, 1):
            full_got()
        if slots != FAR:
            y_got(g, part, 0)
            y_got(g, part, 1)
        if slots != NEAR:
            far_y_got(g, part)
        z_got(g)
        for s in STEPS:
            step_group, _, step_first, step_count = X_STEPS[s]
            if step_group == g and step_first < first + count and first < step_first + step_count:
                x_got(s, 0)
                x_got(s, 1)
                far_x_got(s)
                sibling_got(s)
        if g == 1:
            for j in slots:
                late_got(j, first * 2 // UNITS)
            late_sibling_got(slots, first * 2 // UNITS)

    @lambda f: stepper(f, PRODUCTS)
    def compute(g, part, first, count, slots):
        ready(g, part, first, count, slots)
        by_a = slots in (NEAR, FAR)
        last = g == 3 and slots != NEAR
        add = g > 0
        size = min(count, 2) * unit

        def body(n, carry=0):
            at = first * unit + n * size
            cols = pl.ds(at if isinstance(n, int) else pl.multiple_of(at, size), size)
            total = None
            for slot in slots:
                i, j = (slot, (y + slot - x + 4) % 4) if by_a else ((x + slot - y + 4) % 4, slot)
                for cc in both:
                    term = jnp.dot(a_buf[i, g, cc, part_rows[part], :], b_buf[j, g, cc, :, cols], preferred_element_type=jnp.float32)
                    total = term if total is None else total + term
            if add:
                total = total + acc[part_rows[part], cols]
            if not last:
                acc[part_rows[part], cols] = total
            elif part == 1:
                stage[:, cols] = total.astype(stage.dtype)
            else:
                out_ref[:, pl.ds(pl.multiple_of(side * half + at, size), size)] = total.astype(out_ref.dtype)
            return carry

        if count <= 2 or slots == FAR:
            for n in range((count + 1) // 2):
                body(n)
        else:
            lax.fori_loop(0, count // 2, body, 0)

    @lambda f: stepper(f, LAST_STEPS)
    def send_c(s):
        _, _, first, count = X_STEPS[s]
        at = pl.ds(pl.multiple_of(side * half + first * unit, unit), count * unit)
        remote(stage.at[:, pl.ds(first * unit, count * unit)], out_ref.at[:, at], BIG, c_recv, to_pair).start()

    b_load.wait()
    send_y()
    send_x()
    send_pair()
    send_x()
    send_y()
    send_y()
    send_z_early()
    send_late()
    send_z_pair()
    send_pair()
    send_x()
    send_late()
    send_y()
    forward_x()
    send_pair()
    send_y()
    forward_y()
    late_sibling()
    forward_y()
    late_sibling()
    send_y()
    send_late()
    send_x()
    send_late()
    forward_x()
    send_x()
    send_z_mirror()
    send_late()
    sib_near()
    sib_own()
    send_full()
    forward_y()
    sib_far()
    send_pair()
    sib_near()
    late_sibling()
    send_full()
    send_x()
    send_late()
    send_y()
    send_y()
    send_y()
    send_full()
    forward_x()
    sib_own()
    forward_y()
    compute()
    sib_far()
    compute()
    send_y()
    send_x()
    send_y()
    send_x()
    send_y()
    sib_near()
    send_late()
    compute()
    send_x()
    late_sibling()
    forward_y()
    send_full()
    sib_own()
    send_x()
    forward_x()
    sib_far()
    send_late()
    forward_y()
    compute()
    send_y()
    send_y()
    send_x()
    sib_own()
    forward_x()
    compute()
    sib_near()
    late_sibling()
    sib_own()
    late_sibling()
    compute()
    send_x()
    send_x()
    sib_near()
    compute()
    compute()
    send_y()
    sib_far()
    compute()
    forward_x()
    compute()
    compute()
    send_c()
    late_sibling()
    send_x()
    sib_own()
    sib_far()
    forward_y()
    send_x()
    compute()
    compute()
    compute()
    send_c()
    late_sibling()
    send_y()
    sib_near()
    forward_x()
    send_x()
    sib_far()
    sib_near()
    compute()
    forward_x()
    compute()
    send_c()
    forward_y()
    sib_own()
    sib_far()
    compute()
    sib_own()
    sib_near()
    compute()
    send_c()
    sib_far()
    compute()
    compute()
    send_c()
    compute()
    compute()
    compute()

    sent(b_buf, BIG)
    sent(a_buf.at[:, :, :, pl.ds(0, rows + rows * 3 // 4)], SMALL)
    arrived(out_ref.at[:, other_cols], c_recv, "c")


def solution(mesh):
    def product(a_blk, b_blk):
        rows, width = a_blk.shape
        half = width // 2
        dma = pltpu.SemaphoreType.DMA
        return pl.pallas_call(
            kernel,
            out_shape=pltpu.VMEM((rows, width), jnp.bfloat16),
            in_specs=[pl.BlockSpec(memory_space=pltpu.HBM)] * 2,
            out_specs=pl.BlockSpec(memory_space=pltpu.VMEM),
            scratch_shapes=[
                pltpu.VMEM((4, GROUPS, 2, 2 * rows, rows), jnp.bfloat16),
                pltpu.VMEM((4, GROUPS, 2, rows, half), jnp.bfloat16),
                pltpu.VMEM((2 * rows, half), jnp.float32),
                pltpu.VMEM((rows, half), jnp.bfloat16),
                dma((2,)),
                dma((GROUPS, 2, 2)),
                dma((GROUPS, 2)),
                dma((GROUPS,)),
                dma((2,)),
                dma((len(X_STEPS), 2)),
                dma((len(X_STEPS),)),
                dma((3,)),
                dma((4, 2)),
                dma((len(X_STEPS),)),
                dma((2, 2)),
                dma(()),
                dma((2,)),
            ],
            compiler_params=pltpu.CompilerParams(collective_id=0, has_side_effects=True, vmem_limit_bytes=56 * 1024 * 1024),
        )(a_blk, b_blk)

    block_spec = P(("row", "depth"), "col")
    return jax.shard_map(product, mesh=mesh, in_specs=(block_spec, block_spec), out_specs=block_spec, check_vma=False)
```

```python
import jax
import jax.numpy as jnp
from jax import lax
from jax.experimental import pallas as pl
from jax.experimental.pallas import tpu as pltpu
from jax.sharding import PartitionSpec as P

MESH = pl.DeviceIdType.MESH
GROUPS = 4
UNITS = 8
ALL, OUTER, INNER, NEAR, FAR = (0, 1, 2, 3), (0, 3), (1, 2), (0, 1, 3), (2,)
X_STEPS = ((0, False, 0, 8), (1, True, 0, 8), (2, False, 0, 8), (3, False, 0, 2), (3, False, 2, 2), (3, False, 4, 2), (3, False, 6, 1), (3, False, 7, 1))
STEPS = range(len(X_STEPS))
LAST_STEPS = [s for s in STEPS if X_STEPS[s][0] == 3]
Y_STEPS = ((0, 0), (1, 0), (0, 1), (1, 1), (2, 1), (3, 1), (2, 0), (3, 0))
LATE = ((0, 0), (0, 1), (3, 0), (3, 1), (1, 0), (2, 0), (1, 1), (2, 1))
PRODUCTS = (
    (0, 0, 0, 4, ALL),
    (0, 1, 0, 4, ALL),
    (0, 0, 4, 4, ALL),
    (1, 0, 4, 4, OUTER),
    (0, 1, 4, 4, ALL),
    (1, 0, 0, 4, OUTER),
    (1, 1, 0, 4, OUTER),
    (2, 1, 0, 4, ALL),
    (1, 1, 0, 4, INNER),
    (1, 0, 0, 4, INNER),
    (3, 1, 0, 2, ALL),
    (2, 1, 4, 4, ALL),
    (1, 1, 4, 4, OUTER),
    (3, 1, 2, 2, ALL),
    (1, 1, 4, 4, INNER),
    (3, 1, 4, 2, ALL),
    (1, 0, 4, 4, INNER),
    (3, 1, 6, 1, ALL),
    (2, 0, 4, 4, ALL),
    (3, 1, 7, 1, ALL),
    (2, 0, 0, 4, ALL),
    (3, 0, 0, 8, NEAR),
    (3, 0, 0, 8, FAR),
)
BIG, SMALL = range(2)


def stepper(function, order):
    entries = iter(order)

    def step():
        entry = next(entries)
        function(*(entry if isinstance(entry, tuple) else (entry,)))

    return step


def kernel(a_ref, b_ref, out_ref, a_buf, b_buf, acc, stage, load_sem, y_recv, y_fwd, pair_recv, pair_full, x_recv, x_fwd, z_recv, z_late, sib_recv, sib_late, c_recv, send_sem):
    z, y, r = lax.axis_index("depth"), lax.axis_index("col"), lax.axis_index("row")
    x, c = r // 2, r % 2
    rows, width = a_ref.shape
    half = width // 2
    unit = half // UNITS
    early = rows // 4
    over_y = rows * 3 // 8

    pair = z + 1 - 2 * (z % 2)
    mirror = 3 - z
    side = ((z + 1) // 2) % 2
    z_of = (z, mirror, pair, 3 - pair)

    y_peer = ({"col": (y + 1) % 4}, {"col": (y + 3) % 4})
    x_peer = ({"row": ((x + 1) % 4) * 2 + c}, {"row": ((x + 3) % 4) * 2 + c})
    to_pair, to_mirror, to_sibling = {"depth": pair}, {"depth": mirror}, {"row": x * 2 + 1 - c}
    peers = y_peer + x_peer + (to_pair, to_mirror, to_sibling)
    both = range(2)

    def remote(src, dst, kind, recv, where):
        return pltpu.make_async_remote_copy(src_ref=src, dst_ref=dst, send_sem=send_sem.at[kind], recv_sem=recv, device_id=where, device_id_type=MESH)

    waited = set()

    def arrived(ref, recv, *key):
        if key not in waited:
            waited.add(key)
            remote(ref, ref, BIG, recv, to_sibling).wait_recv()

    def sent(ref, kind):
        remote(ref, ref, kind, c_recv, to_sibling).wait_send()

    own_rows, pair_rows = part_rows = (pl.ds(0, rows), pl.ds(rows, rows))
    early_rows, late_rows = pl.ds(0, early), pl.ds(early, rows - early)
    col_half = (pl.ds(0, half // 2), pl.ds(half // 2, half // 2))
    my_cols = pl.ds(pl.multiple_of(side * half, half), half)
    other_cols = pl.ds(pl.multiple_of((1 - side) * half, half), half)
    slot_of = (3, 1)

    b_load = pltpu.make_async_copy(b_ref.at[:, my_cols], b_buf.at[0, 0, 0], load_sem.at[1])
    b_load.start()
    for g in range(GROUPS):
        for cc in both:
            start = pl.multiple_of((c + cc - 2 * c * cc) * half + z_of[g] * rows, rows)
            pltpu.make_async_copy(a_ref.at[:, pl.ds(start, rows)], a_buf.at[0, g, cc, own_rows], load_sem.at[0]).start()

    barrier = pltpu.get_barrier_semaphore()
    for where in peers:
        pl.semaphore_signal(barrier, inc=1, device_id=where, device_id_type=MESH)
    pl.semaphore_wait(barrier, len(peers))

    def loaded():
        arrived(a_buf.at[0, :, :, own_rows], load_sem.at[0], "load")

    def x_ref(s, slot, piece=None, core=0):
        g, early_only, first, count = X_STEPS[s]
        size = early if early_only else rows
        at = pl.ds(0, size) if piece is None else pl.ds(piece * (size // 2), size // 2)
        return b_buf.at[slot, g, core, at, pl.ds(first * unit, count * unit)]

    def x_kind(s):
        return SMALL if X_STEPS[s][1] else BIG

    def x_got(s, n):
        arrived(x_ref(s, 1), x_recv.at[s, n], "x", s, n)

    def far_x_got(s):
        arrived(x_ref(s, 2), x_fwd.at[s], "fx", s)

    def z_got(g):
        if g > 0:
            arrived(b_buf.at[0, g, 0, early_rows] if g == 1 else b_buf.at[0, g, 0], z_recv.at[g - 1], "z", g)

    @lambda f: stepper(f, [(s, n) for s in STEPS for n in both])
    def send_x(s, n):
        z_got(X_STEPS[s][0])
        for d in both:
            h = (d + n) % 2
            remote(x_ref(s, 0, h), x_ref(s, slot_of[d], h), x_kind(s), x_recv.at[s, n], x_peer[d]).start()

    @lambda f: stepper(f, STEPS)
    def forward_x(s):
        x_got(s, 0)
        for d in both:
            remote(x_ref(s, slot_of[d], d), x_ref(s, 2, d), x_kind(s), x_fwd.at[s], x_peer[d]).start()

    def send_sibling(s, j):
        remote(x_ref(s, j), x_ref(s, j, core=1), BIG, sib_recv.at[s], to_sibling).start()

    @lambda f: stepper(f, STEPS)
    def sib_own(s):
        z_got(X_STEPS[s][0])
        send_sibling(s, 0)

    @lambda f: stepper(f, STEPS)
    def sib_near(s):
        x_got(s, 0)
        x_got(s, 1)
        for slot in slot_of:
            send_sibling(s, slot)

    @lambda f: stepper(f, STEPS)
    def sib_far(s):
        far_x_got(s)
        send_sibling(s, 2)

    def sibling_got(s):
        arrived(x_ref(s, slice(None), core=1), sib_recv.at[s], "sib", s)

    def send_z_early():
        remote(b_buf.at[0, 0, 0, early_rows], b_buf.at[0, 1, 0, early_rows], SMALL, z_recv.at[0], to_mirror).start()

    def send_z_pair():
        remote(b_ref.at[:, other_cols], b_buf.at[0, 2, 0], BIG, z_recv.at[1], to_pair).start()

    def send_z_mirror():
        z_got(2)
        remote(b_buf.at[0, 2, 0], b_buf.at[0, 3, 0], BIG, z_recv.at[2], to_mirror).start()

    def late_ref(j, k, g=1, core=0):
        return b_buf.at[j, g, core, late_rows, col_half[k]]

    def late_got(j, k):
        arrived(late_ref(j, k), z_late.at[j, k], "late", j, k)

    @lambda f: stepper(f, LATE)
    def send_late(j, k):
        if j == 2:
            far_x_got(0)
        elif j > 0:
            x_got(0, 0)
            x_got(0, 1)
        remote(late_ref(j, k, 0), late_ref(j, k), BIG, z_late.at[j, k], to_mirror).start()

    @lambda f: stepper(f, LATE)
    def late_sibling(j, k):
        late_got(j, k)
        remote(late_ref(j, k), late_ref(j, k, core=1), BIG, sib_late.at[int(j in INNER), k], to_sibling).start()

    def late_sibling_got(slots, k):
        arrived(late_ref(pl.ds(0, 2), k, core=1), sib_late.at[int(slots == INNER), k], "sl", slots, k)

    first_rows, second_rows = pl.ds(rows, over_y), pl.ds(rows + over_y, rows - over_y)
    first_own, second_own = pl.ds(0, over_y), pl.ds(over_y, rows - over_y)

    def y_piece(slot, g, part, h):
        if (g, part) == (3, 1):
            return a_buf.at[slot, g, 1, pl.ds(rows + h * (over_y // 2), over_y // 2)]
        return a_buf.at[slot, g, h, part_rows[part]]

    def y_whole(g, part):
        return a_buf.at[1, g, 1, first_rows] if (g, part) == (3, 1) else a_buf.at[1, g, :, part_rows[part]]

    def y_got(g, part, n):
        arrived(y_whole(g, part), y_recv.at[g, part, n], "y", g, part, n)

    def far_y_got(g, part):
        arrived(y_whole(g, part), y_fwd.at[g, part], "fy", g, part)

    def pair_got(g):
        arrived(a_buf.at[0, g, :, pair_rows] if g < 3 else a_buf.at[0, 3, 1, first_rows], pair_recv.at[g], "pair", g)

    @lambda f: stepper(f, [(g, part, n) for g, part in Y_STEPS for n in both])
    def send_y(g, part, n):
        if part == 1:
            pair_got(g)
        else:
            loaded()
        for d in both:
            h = (d + n) % 2
            remote(y_piece(0, g, part, h), y_piece(slot_of[d], g, part, h), SMALL, y_recv.at[g, part, n], y_peer[d]).start()

    @lambda f: stepper(f, Y_STEPS)
    def forward_y(g, part):
        y_got(g, part, 0)
        for d in both:
            remote(y_piece(slot_of[d], g, part, d), y_piece(2, g, part, d), SMALL, y_fwd.at[g, part], y_peer[d]).start()

    @lambda f: stepper(f, range(GROUPS))
    def send_pair(g):
        loaded()
        if g < 3:
            remote(a_buf.at[0, (g + 2) % 4, :, own_rows], a_buf.at[0, g, :, pair_rows], SMALL, pair_recv.at[g], to_pair).start()
        else:
            remote(a_buf.at[0, 1, 1, first_own], a_buf.at[0, 3, 1, first_rows], SMALL, pair_recv.at[3], to_pair).start()

    @lambda f: stepper(f, (0, 1, 3, 2))
    def send_full(i):
        if i == 0:
            loaded()
        elif i == 2:
            far_y_got(1, 0)
        else:
            y_got(1, 0, 0)
            y_got(1, 0, 1)
        remote(a_buf.at[i, 1, 0, own_rows], a_buf.at[i, 3, 0, pair_rows], BIG, pair_full.at[0], to_pair).start()
        remote(a_buf.at[i, 1, 1, second_own], a_buf.at[i, 3, 1, second_rows], SMALL, pair_full.at[1], to_pair).start()

    def full_got():
        arrived(a_buf.at[:, 3, 0, pair_rows], pair_full.at[0], "full", 0)
        arrived(a_buf.at[:, 3, 1, second_rows], pair_full.at[1], "full", 1)

    def ready(g, part, first, count, slots):
        if part == 0:
            loaded()
        else:
            pair_got(g)
        if (g, part) == (3, 1):
            full_got()
        if slots != FAR:
            y_got(g, part, 0)
            y_got(g, part, 1)
        if slots != NEAR:
            far_y_got(g, part)
        z_got(g)
        for s in STEPS:
            step_group, _, step_first, step_count = X_STEPS[s]
            if step_group == g and step_first < first + count and first < step_first + step_count:
                x_got(s, 0)
                x_got(s, 1)
                far_x_got(s)
                sibling_got(s)
        if g == 1:
            for j in slots:
                late_got(j, first * 2 // UNITS)
            late_sibling_got(slots, first * 2 // UNITS)

    @lambda f: stepper(f, PRODUCTS)
    def compute(g, part, first, count, slots):
        ready(g, part, first, count, slots)
        by_a = slots in (NEAR, FAR)
        last = g == 3 and slots != NEAR
        add = g > 0
        size = min(count, 2) * unit

        def body(n, carry=0):
            at = first * unit + n * size
            cols = pl.ds(at if isinstance(n, int) else pl.multiple_of(at, size), size)
            total = None
            for slot in slots:
                i, j = (slot, (y + slot - x + 4) % 4) if by_a else ((x + slot - y + 4) % 4, slot)
                for cc in both:
                    term = jnp.dot(a_buf[i, g, cc, part_rows[part], :], b_buf[j, g, cc, :, cols], preferred_element_type=jnp.float32)
                    total = term if total is None else total + term
            if add:
                total = total + acc[part_rows[part], cols]
            if not last:
                acc[part_rows[part], cols] = total
            elif part == 1:
                stage[:, cols] = total.astype(stage.dtype)
            else:
                out_ref[:, pl.ds(pl.multiple_of(side * half + at, size), size)] = total.astype(out_ref.dtype)
            return carry

        if count <= 2 or slots == FAR:
            for n in range((count + 1) // 2):
                body(n)
        else:
            lax.fori_loop(0, count // 2, body, 0)

    @lambda f: stepper(f, LAST_STEPS)
    def send_c(s):
        _, _, first, count = X_STEPS[s]
        at = pl.ds(pl.multiple_of(side * half + first * unit, unit), count * unit)
        remote(stage.at[:, pl.ds(first * unit, count * unit)], out_ref.at[:, at], BIG, c_recv, to_pair).start()

    b_load.wait()
    send_y()
    send_x()
    send_pair()
    send_z_pair()
    send_y()
    send_y()
    send_pair()
    send_x()
    send_pair()
    send_late()
    send_z_early()
    send_y()
    send_late()
    late_sibling()
    send_y()
    send_x()
    forward_x()
    forward_y()
    send_late()
    sib_own()
    send_late()
    send_full()
    send_y()
    forward_x()
    sib_own()
    send_pair()
    forward_y()
    send_x()
    send_x()
    sib_near()
    send_z_mirror()
    late_sibling()
    forward_y()
    send_y()
    sib_far()
    send_full()
    send_x()
    compute()
    send_y()
    send_full()
    send_late()
    forward_x()
    send_y()
    send_y()
    compute()
    send_late()
    late_sibling()
    forward_y()
    send_x()
    send_late()
    send_y()
    sib_own()
    forward_y()
    send_late()
    sib_near()
    send_y()
    sib_own()
    compute()
    send_x()
    send_x()
    sib_far()
    late_sibling()
    send_x()
    compute()
    send_full()
    send_y()
    compute()
    late_sibling()
    compute()
    forward_x()
    sib_near()
    forward_y()
    send_x()
    send_y()
    sib_far()
    forward_x()
    send_x()
    send_y()
    compute()
    late_sibling()
    send_x()
    compute()
    sib_near()
    sib_own()
    sib_far()
    sib_own()
    sib_near()
    compute()
    compute()
    forward_x()
    compute()
    send_c()
    sib_far()
    sib_own()
    forward_y()
    send_x()
    send_x()
    compute()
    sib_own()
    late_sibling()
    compute()
    send_y()
    compute()
    sib_near()
    send_c()
    forward_x()
    send_x()
    late_sibling()
    sib_far()
    sib_near()
    compute()
    forward_x()
    compute()
    send_c()
    forward_y()
    sib_far()
    sib_near()
    compute()
    compute()
    send_c()
    sib_far()
    compute()
    compute()
    send_c()
    compute()
    compute()
    compute()

    sent(b_buf, BIG)
    sent(a_buf.at[:, :, :, pl.ds(0, rows + rows * 3 // 4)], SMALL)
    arrived(out_ref.at[:, other_cols], c_recv, "c")


def solution(mesh):
    def product(a_blk, b_blk):
        rows, width = a_blk.shape
        half = width // 2
        dma = pltpu.SemaphoreType.DMA
        return pl.pallas_call(
            kernel,
            out_shape=pltpu.VMEM((rows, width), jnp.bfloat16),
            in_specs=[pl.BlockSpec(memory_space=pltpu.HBM)] * 2,
            out_specs=pl.BlockSpec(memory_space=pltpu.VMEM),
            scratch_shapes=[
                pltpu.VMEM((4, GROUPS, 2, 2 * rows, rows), jnp.bfloat16),
                pltpu.VMEM((4, GROUPS, 2, rows, half), jnp.bfloat16),
                pltpu.VMEM((2 * rows, half), jnp.float32),
                pltpu.VMEM((rows, half), jnp.bfloat16),
                dma((2,)),
                dma((GROUPS, 2, 2)),
                dma((GROUPS, 2)),
                dma((GROUPS,)),
                dma((2,)),
                dma((len(X_STEPS), 2)),
                dma((len(X_STEPS),)),
                dma((3,)),
                dma((4, 2)),
                dma((len(X_STEPS),)),
                dma((2, 2)),
                dma(()),
                dma((2,)),
            ],
            compiler_params=pltpu.CompilerParams(collective_id=0, has_side_effects=True, vmem_limit_bytes=56 * 1024 * 1024),
        )(a_blk, b_blk)

    block_spec = P(("row", "depth"), "col")
    return jax.shard_map(product, mesh=mesh, in_specs=(block_spec, block_spec), out_specs=block_spec, check_vma=False)
```

```python
import jax
import jax.numpy as jnp
from jax import lax
from jax.experimental import pallas as pl
from jax.experimental.pallas import tpu as pltpu
from jax.sharding import PartitionSpec as P

MESH = pl.DeviceIdType.MESH
GROUPS = 4
UNITS = 8
ALL, OUTER, INNER, NEAR, FAR = (0, 1, 2, 3), (0, 3), (1, 2), (0, 1, 3), (2,)
X_STEPS = ((0, False, 0, 8), (1, True, 0, 8), (2, False, 0, 8), (3, False, 0, 2), (3, False, 2, 2), (3, False, 4, 2), (3, False, 6, 1), (3, False, 7, 1))
STEPS = range(len(X_STEPS))
LAST_STEPS = [s for s in STEPS if X_STEPS[s][0] == 3]
Y_STEPS = ((0, 0), (1, 0), (0, 1), (1, 1), (2, 1), (3, 1), (2, 0), (3, 0))
LATE = ((0, 0), (0, 1), (3, 0), (3, 1), (1, 0), (2, 0), (1, 1), (2, 1))
PRODUCTS = (
    (0, 1, 4, 4, ALL),
    (0, 1, 0, 4, ALL),
    (0, 0, 0, 4, ALL),
    (1, 1, 0, 4, OUTER),
    (1, 1, 4, 4, OUTER),
    (0, 0, 4, 4, ALL),
    (2, 1, 4, 4, ALL),
    (2, 1, 0, 4, ALL),
    (1, 1, 0, 4, INNER),
    (3, 1, 0, 2, ALL),
    (1, 0, 0, 4, OUTER),
    (1, 0, 4, 4, OUTER),
    (3, 1, 2, 2, ALL),
    (1, 1, 4, 4, INNER),
    (3, 1, 4, 2, ALL),
    (1, 0, 0, 4, INNER),
    (1, 0, 4, 4, INNER),
    (3, 1, 6, 1, ALL),
    (2, 0, 0, 4, ALL),
    (3, 1, 7, 1, ALL),
    (2, 0, 4, 4, ALL),
    (3, 0, 0, 8, NEAR),
    (3, 0, 0, 8, FAR),
)
BIG, SMALL = range(2)


def stepper(function, order):
    entries = iter(order)

    def step():
        entry = next(entries)
        function(*(entry if isinstance(entry, tuple) else (entry,)))

    return step


def kernel(a_ref, b_ref, out_ref, a_buf, b_buf, acc, stage, load_sem, y_recv, y_fwd, pair_recv, pair_full, x_recv, x_fwd, z_recv, z_late, sib_recv, sib_late, c_recv, send_sem):
    z, y, r = lax.axis_index("depth"), lax.axis_index("col"), lax.axis_index("row")
    x, c = r // 2, r % 2
    rows, width = a_ref.shape
    half = width // 2
    unit = half // UNITS
    early = rows // 4
    over_y = rows * 3 // 8

    pair = z + 1 - 2 * (z % 2)
    mirror = 3 - z
    side = ((z + 1) // 2) % 2
    z_of = (z, mirror, pair, 3 - pair)

    y_peer = ({"col": (y + 1) % 4}, {"col": (y + 3) % 4})
    x_peer = ({"row": ((x + 1) % 4) * 2 + c}, {"row": ((x + 3) % 4) * 2 + c})
    to_pair, to_mirror, to_sibling = {"depth": pair}, {"depth": mirror}, {"row": x * 2 + 1 - c}
    peers = y_peer + x_peer + (to_pair, to_mirror, to_sibling)
    both = range(2)

    def remote(src, dst, kind, recv, where):
        return pltpu.make_async_remote_copy(src_ref=src, dst_ref=dst, send_sem=send_sem.at[kind], recv_sem=recv, device_id=where, device_id_type=MESH)

    waited = set()

    def arrived(ref, recv, *key):
        if key not in waited:
            waited.add(key)
            remote(ref, ref, BIG, recv, to_sibling).wait_recv()

    def sent(ref, kind):
        remote(ref, ref, kind, c_recv, to_sibling).wait_send()

    own_rows, pair_rows = part_rows = (pl.ds(0, rows), pl.ds(rows, rows))
    early_rows, late_rows = pl.ds(0, early), pl.ds(early, rows - early)
    col_half = (pl.ds(0, half // 2), pl.ds(half // 2, half // 2))
    my_cols = pl.ds(pl.multiple_of(side * half, half), half)
    other_cols = pl.ds(pl.multiple_of((1 - side) * half, half), half)
    slot_of = (3, 1)

    b_load = pltpu.make_async_copy(b_ref.at[:, my_cols], b_buf.at[0, 0, 0], load_sem.at[1])
    b_load.start()
    for g in range(GROUPS):
        for cc in both:
            start = pl.multiple_of((c + cc - 2 * c * cc) * half + z_of[g] * rows, rows)
            pltpu.make_async_copy(a_ref.at[:, pl.ds(start, rows)], a_buf.at[0, g, cc, own_rows], load_sem.at[0]).start()

    barrier = pltpu.get_barrier_semaphore()
    for where in peers:
        pl.semaphore_signal(barrier, inc=1, device_id=where, device_id_type=MESH)
    pl.semaphore_wait(barrier, len(peers))

    def loaded():
        arrived(a_buf.at[0, :, :, own_rows], load_sem.at[0], "load")

    def x_ref(s, slot, piece=None, core=0):
        g, early_only, first, count = X_STEPS[s]
        size = early if early_only else rows
        at = pl.ds(0, size) if piece is None else pl.ds(piece * (size // 2), size // 2)
        return b_buf.at[slot, g, core, at, pl.ds(first * unit, count * unit)]

    def x_kind(s):
        return SMALL if X_STEPS[s][1] else BIG

    def x_got(s, n):
        arrived(x_ref(s, 1), x_recv.at[s, n], "x", s, n)

    def far_x_got(s):
        arrived(x_ref(s, 2), x_fwd.at[s], "fx", s)

    def z_got(g):
        if g > 0:
            arrived(b_buf.at[0, g, 0, early_rows] if g == 1 else b_buf.at[0, g, 0], z_recv.at[g - 1], "z", g)

    @lambda f: stepper(f, [(s, n) for s in STEPS for n in both])
    def send_x(s, n):
        z_got(X_STEPS[s][0])
        for d in both:
            h = (d + n) % 2
            remote(x_ref(s, 0, h), x_ref(s, slot_of[d], h), x_kind(s), x_recv.at[s, n], x_peer[d]).start()

    @lambda f: stepper(f, STEPS)
    def forward_x(s):
        x_got(s, 0)
        for d in both:
            remote(x_ref(s, slot_of[d], d), x_ref(s, 2, d), x_kind(s), x_fwd.at[s], x_peer[d]).start()

    def send_sibling(s, j):
        remote(x_ref(s, j), x_ref(s, j, core=1), BIG, sib_recv.at[s], to_sibling).start()

    @lambda f: stepper(f, STEPS)
    def sib_own(s):
        z_got(X_STEPS[s][0])
        send_sibling(s, 0)

    @lambda f: stepper(f, STEPS)
    def sib_near(s):
        x_got(s, 0)
        x_got(s, 1)
        for slot in slot_of:
            send_sibling(s, slot)

    @lambda f: stepper(f, STEPS)
    def sib_far(s):
        far_x_got(s)
        send_sibling(s, 2)

    def sibling_got(s):
        arrived(x_ref(s, slice(None), core=1), sib_recv.at[s], "sib", s)

    def send_z_early():
        remote(b_buf.at[0, 0, 0, early_rows], b_buf.at[0, 1, 0, early_rows], SMALL, z_recv.at[0], to_mirror).start()

    def send_z_pair():
        remote(b_ref.at[:, other_cols], b_buf.at[0, 2, 0], BIG, z_recv.at[1], to_pair).start()

    def send_z_mirror():
        z_got(2)
        remote(b_buf.at[0, 2, 0], b_buf.at[0, 3, 0], BIG, z_recv.at[2], to_mirror).start()

    def late_ref(j, k, g=1, core=0):
        return b_buf.at[j, g, core, late_rows, col_half[k]]

    def late_got(j, k):
        arrived(late_ref(j, k), z_late.at[j, k], "late", j, k)

    @lambda f: stepper(f, LATE)
    def send_late(j, k):
        if j == 2:
            far_x_got(0)
        elif j > 0:
            x_got(0, 0)
            x_got(0, 1)
        remote(late_ref(j, k, 0), late_ref(j, k), BIG, z_late.at[j, k], to_mirror).start()

    @lambda f: stepper(f, LATE)
    def late_sibling(j, k):
        late_got(j, k)
        remote(late_ref(j, k), late_ref(j, k, core=1), BIG, sib_late.at[int(j in INNER), k], to_sibling).start()

    def late_sibling_got(slots, k):
        arrived(late_ref(pl.ds(0, 2), k, core=1), sib_late.at[int(slots == INNER), k], "sl", slots, k)

    first_rows, second_rows = pl.ds(rows, over_y), pl.ds(rows + over_y, rows - over_y)
    first_own, second_own = pl.ds(0, over_y), pl.ds(over_y, rows - over_y)

    def y_piece(slot, g, part, h):
        if (g, part) == (3, 1):
            return a_buf.at[slot, g, 1, pl.ds(rows + h * (over_y // 2), over_y // 2)]
        return a_buf.at[slot, g, h, part_rows[part]]

    def y_whole(g, part):
        return a_buf.at[1, g, 1, first_rows] if (g, part) == (3, 1) else a_buf.at[1, g, :, part_rows[part]]

    def y_got(g, part, n):
        arrived(y_whole(g, part), y_recv.at[g, part, n], "y", g, part, n)

    def far_y_got(g, part):
        arrived(y_whole(g, part), y_fwd.at[g, part], "fy", g, part)

    def pair_got(g):
        arrived(a_buf.at[0, g, :, pair_rows] if g < 3 else a_buf.at[0, 3, 1, first_rows], pair_recv.at[g], "pair", g)

    @lambda f: stepper(f, [(g, part, n) for g, part in Y_STEPS for n in both])
    def send_y(g, part, n):
        if part == 1:
            pair_got(g)
        else:
            loaded()
        for d in both:
            h = (d + n) % 2
            remote(y_piece(0, g, part, h), y_piece(slot_of[d], g, part, h), SMALL, y_recv.at[g, part, n], y_peer[d]).start()

    @lambda f: stepper(f, Y_STEPS)
    def forward_y(g, part):
        y_got(g, part, 0)
        for d in both:
            remote(y_piece(slot_of[d], g, part, d), y_piece(2, g, part, d), SMALL, y_fwd.at[g, part], y_peer[d]).start()

    @lambda f: stepper(f, range(GROUPS))
    def send_pair(g):
        loaded()
        if g < 3:
            remote(a_buf.at[0, (g + 2) % 4, :, own_rows], a_buf.at[0, g, :, pair_rows], SMALL, pair_recv.at[g], to_pair).start()
        else:
            remote(a_buf.at[0, 1, 1, first_own], a_buf.at[0, 3, 1, first_rows], SMALL, pair_recv.at[3], to_pair).start()

    @lambda f: stepper(f, (0, 1, 3, 2))
    def send_full(i):
        if i == 0:
            loaded()
        elif i == 2:
            far_y_got(1, 0)
        else:
            y_got(1, 0, 0)
            y_got(1, 0, 1)
        remote(a_buf.at[i, 1, 0, own_rows], a_buf.at[i, 3, 0, pair_rows], BIG, pair_full.at[0], to_pair).start()
        remote(a_buf.at[i, 1, 1, second_own], a_buf.at[i, 3, 1, second_rows], SMALL, pair_full.at[1], to_pair).start()

    def full_got():
        arrived(a_buf.at[:, 3, 0, pair_rows], pair_full.at[0], "full", 0)
        arrived(a_buf.at[:, 3, 1, second_rows], pair_full.at[1], "full", 1)

    def ready(g, part, first, count, slots):
        if part == 0:
            loaded()
        else:
            pair_got(g)
        if (g, part) == (3, 1):
            full_got()
        if slots != FAR:
            y_got(g, part, 0)
            y_got(g, part, 1)
        if slots != NEAR:
            far_y_got(g, part)
        z_got(g)
        for s in STEPS:
            step_group, _, step_first, step_count = X_STEPS[s]
            if step_group == g and step_first < first + count and first < step_first + step_count:
                x_got(s, 0)
                x_got(s, 1)
                far_x_got(s)
                sibling_got(s)
        if g == 1:
            for j in slots:
                late_got(j, first * 2 // UNITS)
            late_sibling_got(slots, first * 2 // UNITS)

    @lambda f: stepper(f, PRODUCTS)
    def compute(g, part, first, count, slots):
        ready(g, part, first, count, slots)
        by_a = slots in (NEAR, FAR)
        last = g == 3 and slots != NEAR
        add = g > 0
        size = min(count, 2) * unit

        def body(n, carry=0):
            at = first * unit + n * size
            cols = pl.ds(at if isinstance(n, int) else pl.multiple_of(at, size), size)
            total = None
            for slot in slots:
                i, j = (slot, (y + slot - x + 4) % 4) if by_a else ((x + slot - y + 4) % 4, slot)
                for cc in both:
                    term = jnp.dot(a_buf[i, g, cc, part_rows[part], :], b_buf[j, g, cc, :, cols], preferred_element_type=jnp.float32)
                    total = term if total is None else total + term
            if add:
                total = total + acc[part_rows[part], cols]
            if not last:
                acc[part_rows[part], cols] = total
            elif part == 1:
                stage[:, cols] = total.astype(stage.dtype)
            else:
                out_ref[:, pl.ds(pl.multiple_of(side * half + at, size), size)] = total.astype(out_ref.dtype)
            return carry

        if count <= 2 or slots == FAR:
            for n in range((count + 1) // 2):
                body(n)
        else:
            lax.fori_loop(0, count // 2, body, 0)

    @lambda f: stepper(f, LAST_STEPS)
    def send_c(s):
        _, _, first, count = X_STEPS[s]
        at = pl.ds(pl.multiple_of(side * half + first * unit, unit), count * unit)
        remote(stage.at[:, pl.ds(first * unit, count * unit)], out_ref.at[:, at], BIG, c_recv, to_pair).start()

    b_load.wait()
    send_y()
    send_x()
    send_y()
    send_pair()
    send_x()
    send_z_pair()
    send_z_early()
    send_y()
    send_late()
    forward_y()
    late_sibling()
    send_late()
    forward_x()
    send_pair()
    send_y()
    send_y()
    send_y()
    send_late()
    send_x()
    send_late()
    send_x()
    send_pair()
    send_full()
    send_x()
    sib_own()
    forward_y()
    send_pair()
    send_z_mirror()
    send_late()
    sib_far()
    send_x()
    forward_y()
    late_sibling()
    send_y()
    late_sibling()
    forward_x()
    send_y()
    send_full()
    send_y()
    forward_x()
    sib_near()
    send_y()
    send_late()
    send_full()
    send_y()
    send_y()
    forward_y()
    send_late()
    send_x()
    sib_own()
    sib_own()
    forward_y()
    sib_near()
    compute()
    sib_far()
    send_late()
    send_full()
    send_x()
    late_sibling()
    send_x()
    forward_y()
    compute()
    send_x()
    compute()
    sib_own()
    late_sibling()
    sib_far()
    send_y()
    forward_x()
    sib_near()
    send_x()
    compute()
    forward_x()
    send_y()
    sib_near()
    compute()
    compute()
    send_y()
    send_x()
    late_sibling()
    sib_near()
    sib_own()
    compute()
    sib_far()
    send_x()
    compute()
    compute()
    forward_x()
    compute()
    forward_y()
    send_c()
    send_x()
    compute()
    sib_far()
    send_y()
    compute()
    send_x()
    sib_near()
    forward_x()
    late_sibling()
    sib_own()
    compute()
    send_c()
    sib_own()
    send_x()
    late_sibling()
    sib_far()
    compute()
    forward_x()
    forward_y()
    compute()
    sib_near()
    send_c()
    sib_far()
    sib_own()
    compute()
    sib_near()
    compute()
    compute()
    send_c()
    sib_far()
    compute()
    compute()
    send_c()
    compute()
    compute()
    compute()

    sent(b_buf, BIG)
    sent(a_buf.at[:, :, :, pl.ds(0, rows + rows * 3 // 4)], SMALL)
    arrived(out_ref.at[:, other_cols], c_recv, "c")


def solution(mesh):
    def product(a_blk, b_blk):
        rows, width = a_blk.shape
        half = width // 2
        dma = pltpu.SemaphoreType.DMA
        return pl.pallas_call(
            kernel,
            out_shape=pltpu.VMEM((rows, width), jnp.bfloat16),
            in_specs=[pl.BlockSpec(memory_space=pltpu.HBM)] * 2,
            out_specs=pl.BlockSpec(memory_space=pltpu.VMEM),
            scratch_shapes=[
                pltpu.VMEM((4, GROUPS, 2, 2 * rows, rows), jnp.bfloat16),
                pltpu.VMEM((4, GROUPS, 2, rows, half), jnp.bfloat16),
                pltpu.VMEM((2 * rows, half), jnp.float32),
                pltpu.VMEM((rows, half), jnp.bfloat16),
                dma((2,)),
                dma((GROUPS, 2, 2)),
                dma((GROUPS, 2)),
                dma((GROUPS,)),
                dma((2,)),
                dma((len(X_STEPS), 2)),
                dma((len(X_STEPS),)),
                dma((3,)),
                dma((4, 2)),
                dma((len(X_STEPS),)),
                dma((2, 2)),
                dma(()),
                dma((2,)),
            ],
            compiler_params=pltpu.CompilerParams(collective_id=0, has_side_effects=True, vmem_limit_bytes=56 * 1024 * 1024),
        )(a_blk, b_blk)

    block_spec = P(("row", "depth"), "col")
    return jax.shard_map(product, mesh=mesh, in_specs=(block_spec, block_spec), out_specs=block_spec, check_vma=False)
```

```python
import jax
import jax.numpy as jnp
from jax import lax
from jax.experimental import pallas as pl
from jax.experimental.pallas import tpu as pltpu
from jax.sharding import PartitionSpec as P

MESH = pl.DeviceIdType.MESH
GROUPS = 4
UNITS = 8
ALL, OUTER, INNER, NEAR, FAR = (0, 1, 2, 3), (0, 3), (1, 2), (0, 1, 3), (2,)
X_STEPS = ((0, False, 0, 8), (1, True, 0, 8), (2, False, 0, 8), (3, False, 0, 2), (3, False, 2, 2), (3, False, 4, 2), (3, False, 6, 1), (3, False, 7, 1))
STEPS = range(len(X_STEPS))
LAST_STEPS = [s for s in STEPS if X_STEPS[s][0] == 3]
Y_STEPS = ((0, 0), (1, 0), (0, 1), (1, 1), (2, 1), (3, 1), (2, 0), (3, 0))
LATE = ((0, 0), (0, 1), (3, 0), (3, 1), (1, 0), (2, 0), (1, 1), (2, 1))
PRODUCTS = (
    (0, 1, 4, 4, ALL),
    (0, 0, 0, 4, ALL),
    (0, 0, 4, 4, ALL),
    (0, 1, 0, 4, ALL),
    (1, 0, 0, 4, OUTER),
    (1, 0, 4, 4, OUTER),
    (1, 1, 0, 4, OUTER),
    (2, 1, 0, 4, ALL),
    (1, 1, 4, 4, OUTER),
    (1, 1, 0, 4, INNER),
    (3, 1, 0, 2, ALL),
    (1, 0, 0, 4, INNER),
    (2, 1, 4, 4, ALL),
    (3, 1, 2, 2, ALL),
    (1, 1, 4, 4, INNER),
    (3, 1, 4, 2, ALL),
    (1, 0, 4, 4, INNER),
    (3, 1, 6, 1, ALL),
    (2, 0, 4, 4, ALL),
    (3, 1, 7, 1, ALL),
    (3, 0, 0, 8, NEAR),
    (2, 0, 0, 4, ALL),
    (3, 0, 0, 8, FAR),
)
BIG, SMALL = range(2)


def stepper(function, order):
    entries = iter(order)

    def step():
        entry = next(entries)
        function(*(entry if isinstance(entry, tuple) else (entry,)))

    return step


def kernel(a_ref, b_ref, out_ref, a_buf, b_buf, acc, stage, load_sem, y_recv, y_fwd, pair_recv, pair_full, x_recv, x_fwd, z_recv, z_late, sib_recv, sib_late, c_recv, send_sem):
    z, y, r = lax.axis_index("depth"), lax.axis_index("col"), lax.axis_index("row")
    x, c = r // 2, r % 2
    rows, width = a_ref.shape
    half = width // 2
    unit = half // UNITS
    early = rows // 4
    over_y = rows * 3 // 8

    pair = z + 1 - 2 * (z % 2)
    mirror = 3 - z
    side = ((z + 1) // 2) % 2
    z_of = (z, mirror, pair, 3 - pair)

    y_peer = ({"col": (y + 1) % 4}, {"col": (y + 3) % 4})
    x_peer = ({"row": ((x + 1) % 4) * 2 + c}, {"row": ((x + 3) % 4) * 2 + c})
    to_pair, to_mirror, to_sibling = {"depth": pair}, {"depth": mirror}, {"row": x * 2 + 1 - c}
    peers = y_peer + x_peer + (to_pair, to_mirror, to_sibling)
    both = range(2)

    def remote(src, dst, kind, recv, where):
        return pltpu.make_async_remote_copy(src_ref=src, dst_ref=dst, send_sem=send_sem.at[kind], recv_sem=recv, device_id=where, device_id_type=MESH)

    waited = set()

    def arrived(ref, recv, *key):
        if key not in waited:
            waited.add(key)
            remote(ref, ref, BIG, recv, to_sibling).wait_recv()

    def sent(ref, kind):
        remote(ref, ref, kind, c_recv, to_sibling).wait_send()

    own_rows, pair_rows = part_rows = (pl.ds(0, rows), pl.ds(rows, rows))
    early_rows, late_rows = pl.ds(0, early), pl.ds(early, rows - early)
    col_half = (pl.ds(0, half // 2), pl.ds(half // 2, half // 2))
    my_cols = pl.ds(pl.multiple_of(side * half, half), half)
    other_cols = pl.ds(pl.multiple_of((1 - side) * half, half), half)
    slot_of = (3, 1)

    b_load = pltpu.make_async_copy(b_ref.at[:, my_cols], b_buf.at[0, 0, 0], load_sem.at[1])
    b_load.start()
    for g in range(GROUPS):
        for cc in both:
            start = pl.multiple_of((c + cc - 2 * c * cc) * half + z_of[g] * rows, rows)
            pltpu.make_async_copy(a_ref.at[:, pl.ds(start, rows)], a_buf.at[0, g, cc, own_rows], load_sem.at[0]).start()

    barrier = pltpu.get_barrier_semaphore()
    for where in peers:
        pl.semaphore_signal(barrier, inc=1, device_id=where, device_id_type=MESH)
    pl.semaphore_wait(barrier, len(peers))

    def loaded():
        arrived(a_buf.at[0, :, :, own_rows], load_sem.at[0], "load")

    def x_ref(s, slot, piece=None, core=0):
        g, early_only, first, count = X_STEPS[s]
        size = early if early_only else rows
        at = pl.ds(0, size) if piece is None else pl.ds(piece * (size // 2), size // 2)
        return b_buf.at[slot, g, core, at, pl.ds(first * unit, count * unit)]

    def x_kind(s):
        return SMALL if X_STEPS[s][1] else BIG

    def x_got(s, n):
        arrived(x_ref(s, 1), x_recv.at[s, n], "x", s, n)

    def far_x_got(s):
        arrived(x_ref(s, 2), x_fwd.at[s], "fx", s)

    def z_got(g):
        if g > 0:
            arrived(b_buf.at[0, g, 0, early_rows] if g == 1 else b_buf.at[0, g, 0], z_recv.at[g - 1], "z", g)

    @lambda f: stepper(f, [(s, n) for s in STEPS for n in both])
    def send_x(s, n):
        z_got(X_STEPS[s][0])
        for d in both:
            h = (d + n) % 2
            remote(x_ref(s, 0, h), x_ref(s, slot_of[d], h), x_kind(s), x_recv.at[s, n], x_peer[d]).start()

    @lambda f: stepper(f, STEPS)
    def forward_x(s):
        x_got(s, 0)
        for d in both:
            remote(x_ref(s, slot_of[d], d), x_ref(s, 2, d), x_kind(s), x_fwd.at[s], x_peer[d]).start()

    def send_sibling(s, j):
        remote(x_ref(s, j), x_ref(s, j, core=1), BIG, sib_recv.at[s], to_sibling).start()

    @lambda f: stepper(f, STEPS)
    def sib_own(s):
        z_got(X_STEPS[s][0])
        send_sibling(s, 0)

    @lambda f: stepper(f, STEPS)
    def sib_near(s):
        x_got(s, 0)
        x_got(s, 1)
        for slot in slot_of:
            send_sibling(s, slot)

    @lambda f: stepper(f, STEPS)
    def sib_far(s):
        far_x_got(s)
        send_sibling(s, 2)

    def sibling_got(s):
        arrived(x_ref(s, slice(None), core=1), sib_recv.at[s], "sib", s)

    def send_z_early():
        remote(b_buf.at[0, 0, 0, early_rows], b_buf.at[0, 1, 0, early_rows], SMALL, z_recv.at[0], to_mirror).start()

    def send_z_pair():
        remote(b_ref.at[:, other_cols], b_buf.at[0, 2, 0], BIG, z_recv.at[1], to_pair).start()

    def send_z_mirror():
        z_got(2)
        remote(b_buf.at[0, 2, 0], b_buf.at[0, 3, 0], BIG, z_recv.at[2], to_mirror).start()

    def late_ref(j, k, g=1, core=0):
        return b_buf.at[j, g, core, late_rows, col_half[k]]

    def late_got(j, k):
        arrived(late_ref(j, k), z_late.at[j, k], "late", j, k)

    @lambda f: stepper(f, LATE)
    def send_late(j, k):
        if j == 2:
            far_x_got(0)
        elif j > 0:
            x_got(0, 0)
            x_got(0, 1)
        remote(late_ref(j, k, 0), late_ref(j, k), BIG, z_late.at[j, k], to_mirror).start()

    @lambda f: stepper(f, LATE)
    def late_sibling(j, k):
        late_got(j, k)
        remote(late_ref(j, k), late_ref(j, k, core=1), BIG, sib_late.at[int(j in INNER), k], to_sibling).start()

    def late_sibling_got(slots, k):
        arrived(late_ref(pl.ds(0, 2), k, core=1), sib_late.at[int(slots == INNER), k], "sl", slots, k)

    first_rows, second_rows = pl.ds(rows, over_y), pl.ds(rows + over_y, rows - over_y)
    first_own, second_own = pl.ds(0, over_y), pl.ds(over_y, rows - over_y)

    def y_piece(slot, g, part, h):
        if (g, part) == (3, 1):
            return a_buf.at[slot, g, 1, pl.ds(rows + h * (over_y // 2), over_y // 2)]
        return a_buf.at[slot, g, h, part_rows[part]]

    def y_whole(g, part):
        return a_buf.at[1, g, 1, first_rows] if (g, part) == (3, 1) else a_buf.at[1, g, :, part_rows[part]]

    def y_got(g, part, n):
        arrived(y_whole(g, part), y_recv.at[g, part, n], "y", g, part, n)

    def far_y_got(g, part):
        arrived(y_whole(g, part), y_fwd.at[g, part], "fy", g, part)

    def pair_got(g):
        arrived(a_buf.at[0, g, :, pair_rows] if g < 3 else a_buf.at[0, 3, 1, first_rows], pair_recv.at[g], "pair", g)

    @lambda f: stepper(f, [(g, part, n) for g, part in Y_STEPS for n in both])
    def send_y(g, part, n):
        if part == 1:
            pair_got(g)
        else:
            loaded()
        for d in both:
            h = (d + n) % 2
            remote(y_piece(0, g, part, h), y_piece(slot_of[d], g, part, h), SMALL, y_recv.at[g, part, n], y_peer[d]).start()

    @lambda f: stepper(f, Y_STEPS)
    def forward_y(g, part):
        y_got(g, part, 0)
        for d in both:
            remote(y_piece(slot_of[d], g, part, d), y_piece(2, g, part, d), SMALL, y_fwd.at[g, part], y_peer[d]).start()

    @lambda f: stepper(f, range(GROUPS))
    def send_pair(g):
        loaded()
        if g < 3:
            remote(a_buf.at[0, (g + 2) % 4, :, own_rows], a_buf.at[0, g, :, pair_rows], SMALL, pair_recv.at[g], to_pair).start()
        else:
            remote(a_buf.at[0, 1, 1, first_own], a_buf.at[0, 3, 1, first_rows], SMALL, pair_recv.at[3], to_pair).start()

    @lambda f: stepper(f, (0, 1, 3, 2))
    def send_full(i):
        if i == 0:
            loaded()
        elif i == 2:
            far_y_got(1, 0)
        else:
            y_got(1, 0, 0)
            y_got(1, 0, 1)
        remote(a_buf.at[i, 1, 0, own_rows], a_buf.at[i, 3, 0, pair_rows], BIG, pair_full.at[0], to_pair).start()
        remote(a_buf.at[i, 1, 1, second_own], a_buf.at[i, 3, 1, second_rows], SMALL, pair_full.at[1], to_pair).start()

    def full_got():
        arrived(a_buf.at[:, 3, 0, pair_rows], pair_full.at[0], "full", 0)
        arrived(a_buf.at[:, 3, 1, second_rows], pair_full.at[1], "full", 1)

    def ready(g, part, first, count, slots):
        if part == 0:
            loaded()
        else:
            pair_got(g)
        if (g, part) == (3, 1):
            full_got()
        if slots != FAR:
            y_got(g, part, 0)
            y_got(g, part, 1)
        if slots != NEAR:
            far_y_got(g, part)
        z_got(g)
        for s in STEPS:
            step_group, _, step_first, step_count = X_STEPS[s]
            if step_group == g and step_first < first + count and first < step_first + step_count:
                x_got(s, 0)
                x_got(s, 1)
                far_x_got(s)
                sibling_got(s)
        if g == 1:
            for j in slots:
                late_got(j, first * 2 // UNITS)
            late_sibling_got(slots, first * 2 // UNITS)

    @lambda f: stepper(f, PRODUCTS)
    def compute(g, part, first, count, slots):
        ready(g, part, first, count, slots)
        by_a = slots in (NEAR, FAR)
        last = g == 3 and slots != NEAR
        add = g > 0
        size = min(count, 2) * unit

        def body(n, carry=0):
            at = first * unit + n * size
            cols = pl.ds(at if isinstance(n, int) else pl.multiple_of(at, size), size)
            total = None
            for slot in slots:
                i, j = (slot, (y + slot - x + 4) % 4) if by_a else ((x + slot - y + 4) % 4, slot)
                for cc in both:
                    term = jnp.dot(a_buf[i, g, cc, part_rows[part], :], b_buf[j, g, cc, :, cols], preferred_element_type=jnp.float32)
                    total = term if total is None else total + term
            if add:
                total = total + acc[part_rows[part], cols]
            if not last:
                acc[part_rows[part], cols] = total
            elif part == 1:
                stage[:, cols] = total.astype(stage.dtype)
            else:
                out_ref[:, pl.ds(pl.multiple_of(side * half + at, size), size)] = total.astype(out_ref.dtype)
            return carry

        if count <= 2 or slots == FAR:
            for n in range((count + 1) // 2):
                body(n)
        else:
            lax.fori_loop(0, count // 2, body, 0)

    @lambda f: stepper(f, LAST_STEPS)
    def send_c(s):
        _, _, first, count = X_STEPS[s]
        at = pl.ds(pl.multiple_of(side * half + first * unit, unit), count * unit)
        remote(stage.at[:, pl.ds(first * unit, count * unit)], out_ref.at[:, at], BIG, c_recv, to_pair).start()

    b_load.wait()
    send_y()
    send_x()
    sib_own()
    send_y()
    send_late()
    send_pair()
    send_x()
    send_y()
    send_z_pair()
    send_y()
    send_z_early()
    send_x()
    forward_y()
    send_x()
    send_y()
    send_late()
    forward_x()
    send_late()
    forward_x()
    sib_own()
    send_pair()
    forward_y()
    late_sibling()
    send_late()
    send_y()
    send_pair()
    forward_y()
    send_x()
    send_pair()
    send_z_mirror()
    send_y()
    send_full()
    send_y()
    send_full()
    sib_near()
    send_x()
    send_y()
    forward_x()
    send_y()
    late_sibling()
    sib_far()
    late_sibling()
    send_late()
    compute()
    compute()
    send_full()
    send_late()
    sib_far()
    forward_y()
    send_y()
    send_x()
    send_full()
    sib_near()
    forward_y()
    compute()
    send_x()
    compute()
    send_late()
    sib_own()
    send_x()
    sib_near()
    send_y()
    sib_own()
    send_x()
    compute()
    forward_x()
    sib_own()
    send_x()
    forward_y()
    send_y()
    sib_far()
    late_sibling()
    send_y()
    sib_own()
    send_late()
    compute()
    forward_x()
    compute()
    send_x()
    sib_near()
    sib_own()
    late_sibling()
    send_y()
    compute()
    late_sibling()
    compute()
    sib_far()
    send_x()
    forward_x()
    compute()
    compute()
    send_x()
    send_c()
    sib_near()
    sib_far()
    send_x()
    compute()
    forward_y()
    compute()
    compute()
    send_y()
    late_sibling()
    forward_x()
    send_x()
    send_c()
    sib_own()
    late_sibling()
    sib_near()
    sib_far()
    sib_near()
    compute()
    forward_x()
    compute()
    send_c()
    sib_far()
    forward_y()
    sib_near()
    compute()
    compute()
    send_c()
    sib_far()
    compute()
    compute()
    send_c()
    compute()
    compute()
    compute()

    sent(b_buf, BIG)
    sent(a_buf.at[:, :, :, pl.ds(0, rows + rows * 3 // 4)], SMALL)
    arrived(out_ref.at[:, other_cols], c_recv, "c")


def solution(mesh):
    def product(a_blk, b_blk):
        rows, width = a_blk.shape
        half = width // 2
        dma = pltpu.SemaphoreType.DMA
        return pl.pallas_call(
            kernel,
            out_shape=pltpu.VMEM((rows, width), jnp.bfloat16),
            in_specs=[pl.BlockSpec(memory_space=pltpu.HBM)] * 2,
            out_specs=pl.BlockSpec(memory_space=pltpu.VMEM),
            scratch_shapes=[
                pltpu.VMEM((4, GROUPS, 2, 2 * rows, rows), jnp.bfloat16),
                pltpu.VMEM((4, GROUPS, 2, rows, half), jnp.bfloat16),
                pltpu.VMEM((2 * rows, half), jnp.float32),
                pltpu.VMEM((rows, half), jnp.bfloat16),
                dma((2,)),
                dma((GROUPS, 2, 2)),
                dma((GROUPS, 2)),
                dma((GROUPS,)),
                dma((2,)),
                dma((len(X_STEPS), 2)),
                dma((len(X_STEPS),)),
                dma((3,)),
                dma((4, 2)),
                dma((len(X_STEPS),)),
                dma((2, 2)),
                dma(()),
                dma((2,)),
            ],
            compiler_params=pltpu.CompilerParams(collective_id=0, has_side_effects=True, vmem_limit_bytes=56 * 1024 * 1024),
        )(a_blk, b_blk)

    block_spec = P(("row", "depth"), "col")
    return jax.shard_map(product, mesh=mesh, in_specs=(block_spec, block_spec), out_specs=block_spec, check_vma=False)
```
